32 devices in a mesh: grp: 4 (over y, core), seq: 8 (over z, x).
Axes of the slice: x: 2, y: 2, z: 4, core: 2. Of those that a mesh axis runs over, the one named last changes fastest.
Arguments:
- layer_input: bfloat16 [8192, 2048], P(('grp', 'seq')), may hold values from -6 to 6
- entry_gain: float32 [2048], replicated, may hold values from 0.1 to 1.9
- entry_shift: float32 [2048], replicated, may hold values from -1.75 to 1.75
- joint_weight: bfloat16 [2048, 6144], P(('grp', 'seq')), may hold values from -0.125 to 0.125
- query_offset: float32 [2048], replicated, may hold values from -3 to 3
- value_offset: float32 [2048], replicated, may hold values from -0.3125 to 0.3125
- mixing_weight: bfloat16 [2048, 2048], P(('grp', 'seq')), may hold values from -1 to 1
- attention_offset: float32 [2048], replicated, may hold values from -3 to 3
- middle_gain: float32 [2048], replicated, may hold values from 0.1 to 1.9
- middle_shift: float32 [2048], replicated, may hold values from -1.75 to 1.75
- expand_weight: bfloat16 [2048, 8192], P(('grp', 'seq')), may hold values from -0.125 to 0.125
- expand_offset: float32 [8192], replicated, may hold values from -3 to 3
- shrink_weight: bfloat16 [2048, 8192], P(('grp', 'seq')), may hold values from -0.0625 to 0.0625
- shrink_offset: float32 [2048], replicated, may hold values from -3 to 3
- placement: int32 [4, 2048], P('grp'), may hold values from 0 to 2047, each once within a row
- slot_lengths: int32 [4, 4], P('grp'), may hold values from 1 to 256, 832 in all within a row
- cotangent: bfloat16 [8192, 2048], P(('grp', 'seq')), may hold values from -6 to 6
Outputs:
- layer_output: bfloat16 [8192, 2048], P(('grp', 'seq'))
- input_gradient: bfloat16 [8192, 2048], P(('grp', 'seq'))
- entry_gain_gradient: float32 [2048], replicated
- entry_shift_gradient: float32 [2048], replicated
- joint_gradient: float32 [2048, 6144], P(('grp', 'seq'))
- query_gradient: float32 [2048], replicated
- value_gradient: float32 [2048], replicated
- mixing_gradient: float32 [2048, 2048], P(('grp', 'seq'))
- attention_offset_gradient: float32 [2048], replicated
- middle_gain_gradient: float32 [2048], replicated
- middle_shift_gradient: float32 [2048], replicated
- expand_gradient: float32 [2048, 8192], P(('grp', 'seq'))
- expand_offset_gradient: float32 [8192], replicated
- shrink_gradient: float32 [2048, 8192], P(('grp', 'seq'))
- shrink_offset_gradient: float32 [2048], replicated
The draws below stay inside these ranges and needn't reach their ends.
Inputs may be any that keep to these rules, and one draw needn't show every extreme that they name: `placement`: each row holds every position of its group once. `slot_lengths`: the real tokens of each slot of 256 positions; the rest of a slot is padding; some slot of every group is full.
All inputs are finite; a program needn't handle non-finite values.
Results may differ from the reference program's by a relative error of at most 0.013.
Values may be sent and summed in bfloat16 or wider, within the bound.
A program may use at most 704 MiB of HBM per device.

```python
import math
import jax
import jax.numpy as jnp
import numpy as np
from jax import lax

D = 2048
HEADS = 16
HEAD = 128
FF = 8192
CONT = 256
QBLOCK = 512
GROUPS = 4
GROUP_TOK = 2048
PROMPT = 1024
NCONT = 4
TOKENS = 8192


def level_of(stream_key, extent, cuts, smallest, top_value):
    factor_of, own = 1.0, jax.random.fold_in(stream_key, 6)
    for dim, shards_of in cuts:
        draws = jnp.exp(jax.random.uniform(jax.random.fold_in(own, dim), (shards_of,), jnp.float32, smallest / len(cuts), top_value / len(cuts)))
        factor_of = factor_of * jnp.repeat(draws, extent[dim] // shards_of).reshape([-1 if axis == dim else 1 for axis in range(len(extent))])
    return factor_of


def length_profile(number_of, total, most, lean):
    weights = [(1 << 20) // math.isqrt(grade ** lean) + 1 for grade in range(2, number_of + 1)]
    surplus, holding = total - most - (number_of - 1), [1] * (number_of - 1)
    while surplus > 0:
        candidates = [i for i in range(number_of - 1) if holding[i] < most]
        mass, left = sum([weights[i] for i in candidates]), surplus
        for i in candidates:
            extra = min(most - holding[i], max(1, left * weights[i] // mass), surplus)
            holding[i] = holding[i] + extra
            surplus = surplus - extra
    return np.array([most] + holding)


def ragged(rng, count, total, bound, lean):
    if count == 2:
        one = jax.random.randint(rng, (), max(1, total - bound), min(bound, total - 1) + 1)
        return jnp.stack([one, total - one])
    sizes = jnp.asarray(length_profile(count, total, bound, lean), jnp.int32)
    couples = (count - 1) // 2
    source_of, sink = sizes[1:1 + 2 * couples:2], sizes[2:2 + 2 * couples:2]
    slack = jnp.minimum(source_of - 1, bound - sink)
    passed = jax.random.randint(jax.random.fold_in(rng, 1), (couples,), 0, 1 << 20) % (slack + 1)
    sizes = sizes.at[1:1 + 2 * couples:2].set(source_of - passed).at[2:2 + 2 * couples:2].set(sink + passed)
    return sizes[jax.random.permutation(jax.random.fold_in(rng, 2), count)]


def normal_values(stream_key, dims, scale, reach, split=(), kind=jnp.bfloat16):
    level = level_of(stream_key, dims, split, -0.22, 0.18) if split else 1.0
    values = jax.random.normal(stream_key, dims, jnp.float32) * scale * level
    return jnp.minimum(jnp.maximum(values, -reach), reach).astype(kind)


def setup_inputs(seed: int = 0) -> dict:
    keys = jax.random.split(jax.random.key(seed), 18)
    layer_input = normal_values(keys[0], (TOKENS, D), 1.0, 6.0, ((0, 32),))
    entry_gain = jnp.clip(1.0 + 0.18 * jax.random.normal(keys[1], (D,), jnp.float32), 0.1, 1.9)
    entry_shift = normal_values(keys[2], (D,), 0.3, 1.75, (), jnp.float32)
    joint_weight = normal_values(keys[3], (D, 3 * D), D ** -0.5, 0.125, ((0, 32),))
    query_offset = normal_values(keys[4], (D,), 0.5, 3.0, (), jnp.float32)
    value_offset = normal_values(keys[5], (D,), 0.05, 0.3125, (), jnp.float32)
    mixing_weight = normal_values(keys[6], (D, D), (D // 64) ** -0.5, 1.0, ((0, 32),))
    attention_offset = normal_values(keys[7], (D,), 0.5, 3.0, (), jnp.float32)
    middle_gain = jnp.clip(1.0 + 0.18 * jax.random.normal(keys[8], (D,), jnp.float32), 0.1, 1.9)
    middle_shift = normal_values(keys[9], (D,), 0.3, 1.75, (), jnp.float32)
    expand_weight = normal_values(keys[10], (D, FF), D ** -0.5, 0.125, ((0, 32),))
    expand_offset = normal_values(keys[11], (FF,), 0.5, 3.0, (), jnp.float32)
    shrink_weight = normal_values(keys[12], (D, FF), FF ** -0.5, 0.0625, ((0, 32),))
    shrink_offset = normal_values(keys[13], (D,), 0.5, 3.0, (), jnp.float32)
    placement = jax.vmap(lambda own: jax.random.permutation(own, GROUP_TOK))(jax.random.split(keys[14], GROUPS)).reshape((GROUPS, GROUP_TOK)).astype(jnp.int32)
    slot_lengths = jax.vmap(lambda own: ragged(own, NCONT, (3 * NCONT + 1) * CONT // 4, CONT, 2))(jax.random.split(keys[15], GROUPS)).reshape((GROUPS, NCONT)).astype(jnp.int32)
    cotangent = normal_values(keys[16], (TOKENS, D), 1.0, 6.0, ((0, 32),))
    return dict(layer_input=layer_input, entry_gain=entry_gain, entry_shift=entry_shift, joint_weight=joint_weight, query_offset=query_offset, value_offset=value_offset, mixing_weight=mixing_weight, attention_offset=attention_offset, middle_gain=middle_gain, middle_shift=middle_shift, expand_weight=expand_weight, expand_offset=expand_offset, shrink_weight=shrink_weight, shrink_offset=shrink_offset, placement=placement, slot_lengths=slot_lengths, cotangent=cotangent)


@jax.custom_vjp
def low(v):
    return lax.optimization_barrier(v.astype(jnp.bfloat16)).astype(jnp.float32)

@jax.custom_vjp
def low_back(v):
    return v

def low_keep(v):
    return (low(v), None)

def low_pass(kept, grad):
    return (grad,)

def back_keep(v):
    return (v, None)

def back_low(kept, grad):
    return (low(grad),)
low.defvjp(low_keep, low_pass)
low_back.defvjp(back_keep, back_low)
highest = lax.Precision.HIGHEST
norm_epsilon = 1e-05
masked_score = -1e+30

def product(left_matrix, right_matrix):
    return jnp.dot(left_matrix, right_matrix, precision=highest, preferred_element_type=jnp.float32)

def layer_norm(values, scale_vector, shift_vector):
    average = lax.optimization_barrier(jnp.mean(values, axis=-1, keepdims=True))
    centered = values - average
    variance = lax.optimization_barrier(jnp.mean(centered * centered, axis=-1, keepdims=True))
    return centered * lax.rsqrt(variance + norm_epsilon) * scale_vector + shift_vector

def key_facts(positions, lengths):
    segment = (positions - PROMPT) // CONT
    within = positions - PROMPT - segment * CONT
    slot_ids = jnp.arange(lengths.shape[0], dtype=jnp.int32)
    slot_limit = lax.optimization_barrier(jnp.sum(jnp.where(segment[:, None] == slot_ids[None, :], lengths[None, :], 0), axis=1))
    return (segment, (positions < PROMPT) | (within < slot_limit))

def block_mask(query_place, key_place, key_segment, key_live):
    query_col = query_place[:, None]
    key_row = key_place[None, :]
    query_segment = (query_col - PROMPT) // CONT
    prompt_keys = (key_row < PROMPT) & ((query_col >= PROMPT) | (key_row <= query_col))
    same_slot = (query_col >= PROMPT) & (key_row >= PROMPT) & (query_segment == key_segment[None, :]) & (key_row <= query_col) & key_live[None, :]
    return prompt_keys | same_slot

def group_forward(param_tuple, tokens, positions, lengths):
    entry_gain, entry_shift, joint_weight, query_offset, value_offset, mixing_weight, attention_offset, middle_gain, middle_shift, expand_weight, expand_offset, shrink_weight, shrink_offset = param_tuple
    entry_normed = low(layer_norm(tokens, entry_gain, entry_shift))
    offsets = jnp.stack([query_offset.reshape(HEADS, HEAD), jnp.zeros((HEADS, HEAD), jnp.float32), value_offset.reshape(HEADS, HEAD)], axis=1)
    joint_values = product(entry_normed, joint_weight).reshape(GROUP_TOK, HEADS, 3, HEAD) + offsets
    joint_values = low(low_back(joint_values))
    queries = joint_values[:, :, 0]
    key_vectors = joint_values[:, :, 1]
    values = joint_values[:, :, 2]
    key_segment, key_live = key_facts(positions, lengths)
    score_scale = HEAD ** (-0.5)

    def one_block(block_args):
        block_queries, block_places = block_args
        scores = jnp.einsum('qhe,khe->hqk', block_queries, key_vectors, precision=highest) * score_scale
        allowed = block_mask(block_places, positions, key_segment, key_live)
        scores = low_back(jnp.where(allowed[None], scores, masked_score))
        soft_weights = low(jax.nn.softmax(scores, axis=-1))
        return jnp.einsum('hqk,khe->qhe', soft_weights, values, precision=highest)
    blocks = GROUP_TOK // QBLOCK
    mixture = lax.map(jax.checkpoint(one_block), (queries.reshape(blocks, QBLOCK, HEADS, HEAD), positions.reshape(blocks, QBLOCK)))
    attended = low(low_back(mixture.reshape(GROUP_TOK, D)))
    branch = low_back(product(attended, mixing_weight) + attention_offset)
    residual = tokens + branch
    middle_normed = low(layer_norm(residual, middle_gain, middle_shift))
    expanded = low_back(product(middle_normed, expand_weight) + expand_offset)
    activated = low(jax.nn.gelu(expanded, approximate=False))
    return residual + product(activated, shrink_weight.T) + shrink_offset

def reference(layer_input, entry_gain, entry_shift, joint_weight, query_offset, value_offset, mixing_weight, attention_offset, middle_gain, middle_shift, expand_weight, expand_offset, shrink_weight, shrink_offset, placement, slot_lengths, cotangent):
    param_tuple = (entry_gain, entry_shift, joint_weight.astype(jnp.float32), query_offset, value_offset, mixing_weight.astype(jnp.float32), attention_offset, middle_gain, middle_shift, expand_weight.astype(jnp.float32), expand_offset, shrink_weight.astype(jnp.float32), shrink_offset)
    tokens_float = layer_input.astype(jnp.float32).reshape(GROUPS, GROUP_TOK, D)

    def whole(tokens_all, params_all):

        def scan_step(running, group_args):
            tokens, positions, lengths = group_args
            return (running, group_forward(params_all, tokens, positions, lengths))
        unused_total, outputs = lax.scan(scan_step, jnp.zeros((), jnp.float32), (tokens_all, placement, slot_lengths))
        return outputs
    output_float, pullback = jax.vjp(whole, tokens_float, param_tuple)
    input_slope, slopes = pullback(cotangent.astype(jnp.float32).reshape(GROUPS, GROUP_TOK, D))
    return (output_float.reshape(TOKENS, D).astype(jnp.bfloat16), input_slope.reshape(TOKENS, D).astype(jnp.bfloat16), slopes[0], slopes[1], slopes[2], slopes[3], slopes[4], slopes[5], slopes[6], slopes[7], slopes[8], slopes[9], slopes[10], slopes[11], slopes[12])
```

```python
import jax
import jax.numpy as jnp
from jax import lax
from jax.sharding import Mesh, PartitionSpec as P

HEADS = 16
CONT = 256
QBLOCK = 512
PLANE = ("grp", "sub")
EVERY = ("grp", "rep", "sub")

norm_epsilon = 1e-05
masked_score = -1e30


def norm_terms(values):
    average = jnp.mean(values, axis=-1, keepdims=True)
    centered = values - average
    variance = jnp.mean(centered * centered, axis=-1, keepdims=True)
    inverse = lax.rsqrt(variance + norm_epsilon)
    return centered * inverse, inverse


def norm_back(slope, gain, normal, inverse):
    scaled = slope * gain
    return inverse * (
        scaled
        - jnp.mean(scaled, axis=-1, keepdims=True)
        - normal * jnp.mean(scaled * normal, axis=-1, keepdims=True)
    )


def exact_gelu(values):
    return jax.nn.gelu(values, approximate=False)


def key_bounds(positions, lengths, prompt):
    segment = (positions - prompt) // CONT
    within = positions - prompt - segment * CONT
    slot_ids = jnp.arange(lengths.shape[0], dtype=jnp.int32)
    slot_limit = jnp.sum(
        jnp.where(segment[:, None] == slot_ids[None, :], lengths[None, :], 0), axis=1
    )
    last = prompt + (segment + 1) * CONT - 1
    last = jnp.where(within < slot_limit, last, -1)
    return jnp.where(positions < prompt, positions.shape[0], last)


def block_mask(query_place, key_place, key_last):
    query_col = query_place[:, None]
    return (key_place[None, :] <= query_col) & (query_col <= key_last[None, :])


def product(left_matrix, right_matrix):
    return jnp.dot(left_matrix, right_matrix, preferred_element_type=jnp.float32)


def product_transposed(left_matrix, right_matrix):
    return lax.dot_general(
        left_matrix,
        right_matrix,
        (((1,), (1,)), ((), ())),
        preferred_element_type=jnp.float32,
    )


def row_outer(left_matrix, right_matrix):
    return lax.dot_general(
        left_matrix, right_matrix, (((0,), (0,)), ((), ())), preferred_element_type=jnp.float32
    )


def attention_forward(grouped, places, key_last, score_scale):
    queries = grouped[:, :, 0]
    key_vectors = grouped[:, :, 1]
    values = grouped[:, :, 2]
    rows_total = grouped.shape[0]

    def one_block(block_index):
        first_row = block_index * QBLOCK
        block_queries = lax.dynamic_slice_in_dim(queries, first_row, QBLOCK, 0)
        block_places = lax.dynamic_slice_in_dim(places, first_row, QBLOCK, 0)
        allowed = block_mask(block_places, places, key_last)
        scores = (
            jnp.einsum(
                "qhe,khe->hqk", block_queries, key_vectors, preferred_element_type=jnp.float32
            )
            * score_scale
        )
        scores = jnp.where(allowed[None], scores, masked_score)
        row_top = jnp.max(scores, axis=2, keepdims=True)
        row_total = jnp.sum(jnp.exp(scores - row_top), axis=2, keepdims=True)
        log_total = row_top + jnp.log(row_total)
        soft_weights = jnp.exp(scores - log_total).astype(jnp.bfloat16)
        mixture = jnp.einsum(
            "hqk,khe->qhe", soft_weights, values, preferred_element_type=jnp.float32
        )
        return (mixture.astype(jnp.bfloat16), jnp.transpose(log_total[:, :, 0]))

    mixture, log_totals = lax.map(one_block, jnp.arange(rows_total // QBLOCK, dtype=jnp.int32))
    return mixture.reshape(rows_total, -1), log_totals.reshape(rows_total, -1)


def attention_backward(grouped, log_totals, slopes, places, key_last, score_scale):
    queries = grouped[:, :, 0]
    key_vectors = grouped[:, :, 1]
    values = grouped[:, :, 2]
    rows_total = grouped.shape[0]

    def one_block(running, block_index):
        key_sum, value_sum = running
        first_row = block_index * QBLOCK
        block_queries = lax.dynamic_slice_in_dim(queries, first_row, QBLOCK, 0)
        block_slopes = lax.dynamic_slice_in_dim(slopes, first_row, QBLOCK, 0)
        block_totals = lax.dynamic_slice_in_dim(log_totals, first_row, QBLOCK, 0)
        block_places = lax.dynamic_slice_in_dim(places, first_row, QBLOCK, 0)
        allowed = block_mask(block_places, places, key_last)
        scores = (
            jnp.einsum(
                "qhe,khe->hqk", block_queries, key_vectors, preferred_element_type=jnp.float32
            )
            * score_scale
        )
        scores = jnp.where(allowed[None], scores, masked_score)
        probable = jnp.exp(scores - jnp.transpose(block_totals)[:, :, None])
        weight_slope = jnp.einsum(
            "qhe,khe->hqk", block_slopes, values, preferred_element_type=jnp.float32
        )
        centre = jnp.sum(probable * weight_slope, axis=2, keepdims=True)
        score_slope = (probable * (weight_slope - centre)).astype(jnp.bfloat16)
        query_slope = (
            jnp.einsum("hqk,khe->qhe", score_slope, key_vectors, preferred_element_type=jnp.float32)
            * score_scale
        )
        key_sum = (
            key_sum
            + jnp.einsum(
                "hqk,qhe->khe", score_slope, block_queries, preferred_element_type=jnp.float32
            )
            * score_scale
        )
        value_sum = value_sum + jnp.einsum(
            "hqk,qhe->khe",
            probable.astype(jnp.bfloat16),
            block_slopes,
            preferred_element_type=jnp.float32,
        )
        return ((key_sum, value_sum), query_slope)

    empty_sums = jnp.zeros(values.shape, jnp.float32)
    (key_sum, value_sum), query_slopes = lax.scan(
        one_block, (empty_sums, empty_sums), jnp.arange(rows_total // QBLOCK, dtype=jnp.int32)
    )
    query_slopes = query_slopes.reshape(values.shape)
    return jnp.stack([query_slopes, key_sum, value_sum], axis=2).astype(jnp.bfloat16)


def plane_columns(weight, plane_count):
    rows, columns = weight.shape
    own = lax.all_to_all(
        weight.reshape(rows, plane_count, columns // plane_count),
        PLANE,
        split_axis=1,
        concat_axis=0,
        tiled=True,
    ).reshape(plane_count * rows, columns // plane_count)
    every = lax.all_gather(own, "rep", axis=0, tiled=True)
    groups, reps, subs = (lax.axis_size(name) for name in EVERY)
    every = every.reshape(reps, groups, subs, rows, -1).transpose(1, 0, 2, 3, 4)
    return every.reshape(reps * groups * subs * rows, -1)


def owner_rows(gradient, plane_count):
    groups, reps, subs = (lax.axis_size(name) for name in EVERY)
    columns = gradient.shape[1]
    rows = gradient.shape[0] // (groups * reps * subs)
    ordered = gradient.astype(jnp.bfloat16).reshape(groups, reps, subs, rows, columns)
    ordered = ordered.transpose(1, 0, 2, 3, 4).reshape(-1, columns)
    summed = lax.psum_scatter(ordered, "rep", scatter_dimension=0, tiled=True)
    own = lax.all_to_all(
        summed.reshape(plane_count, rows, columns), PLANE, split_axis=0, concat_axis=0, tiled=True
    )
    return own.transpose(1, 0, 2).reshape(rows, plane_count * columns).astype(jnp.float32)


def shards(
    layer_input,
    entry_gain,
    entry_shift,
    joint_weight,
    query_offset,
    value_offset,
    mixing_weight,
    attention_offset,
    middle_gain,
    middle_shift,
    expand_weight,
    expand_offset,
    shrink_weight,
    shrink_offset,
    placement,
    slot_lengths,
    cotangent,
):
    token_rows, width = layer_input.shape
    hidden_width = expand_weight.shape[1]
    groups, reps, subs = (lax.axis_size(name) for name in EVERY)
    plane_count = groups * subs
    plane_index = lax.axis_index(PLANE)
    rep_index = lax.axis_index("rep")
    head_size = width // HEADS
    local_heads = HEADS // plane_count
    head_columns = local_heads * head_size
    score_scale = head_size ** (-0.5)

    placements = lax.all_gather(placement, "grp", axis=0, tiled=True)
    lengths_all = lax.all_gather(slot_lengths, "grp", axis=0, tiled=True)
    places = lax.dynamic_index_in_dim(placements, rep_index, 0, keepdims=False)
    lengths = lax.dynamic_index_in_dim(lengths_all, rep_index, 0, keepdims=False)
    prompt = places.shape[0] // 2
    key_last = key_bounds(places, lengths, prompt)

    joint_slice = plane_columns(joint_weight, plane_count)
    expand_slice = plane_columns(expand_weight, plane_count)
    shrink_slice = plane_columns(shrink_weight, plane_count)
    mixing_whole = lax.all_gather(mixing_weight, EVERY, axis=0, tiled=True)

    input_float = layer_input.astype(jnp.float32)
    entry_normal, entry_inverse = norm_terms(input_float)
    entry_normed = (entry_normal * entry_gain + entry_shift).astype(jnp.bfloat16)
    entry_all = lax.all_gather(entry_normed, PLANE, axis=0, tiled=True)
    plane_rows = entry_all.shape[0]

    offsets = jnp.stack(
        [
            query_offset.reshape(HEADS, head_size),
            jnp.zeros((HEADS, head_size), jnp.float32),
            value_offset.reshape(HEADS, head_size),
        ],
        axis=1,
    ).reshape(-1)
    offsets = lax.dynamic_slice_in_dim(offsets, plane_index * 3 * head_columns, 3 * head_columns)
    joint_values = (product(entry_all, joint_slice) + offsets).astype(jnp.bfloat16)
    heads_kept = lax.all_to_all(
        joint_values.reshape(groups, plane_rows // groups, 3 * head_columns),
        "rep",
        split_axis=0,
        concat_axis=0,
        tiled=True,
    ).reshape(plane_rows, local_heads, 3, head_size)
    mixture, log_totals = attention_forward(heads_kept, places, key_last, score_scale)

    def to_tokens(array):
        columns = array.shape[1]
        at_plane = lax.all_to_all(
            array.reshape(reps, plane_rows // reps, columns),
            "rep",
            split_axis=0,
            concat_axis=0,
            tiled=True,
        )
        return at_plane.reshape(plane_count, token_rows, columns)

    attended = lax.all_to_all(to_tokens(mixture), PLANE, split_axis=0, concat_axis=0, tiled=True)
    attended = attended.transpose(1, 0, 2).reshape(token_rows, width)
    residual = input_float + (product(attended, mixing_whole) + attention_offset)
    middle_normal, middle_inverse = norm_terms(residual)
    middle_normed = (middle_normal * middle_gain + middle_shift).astype(jnp.bfloat16)
    middle_all = lax.all_gather(middle_normed, PLANE, axis=0, tiled=True)
    cotangent_all = lax.all_gather(cotangent, PLANE, axis=0, tiled=True)

    hidden_local = hidden_width // plane_count
    offset_local = lax.dynamic_slice_in_dim(expand_offset, plane_index * hidden_local, hidden_local)
    expanded = product(middle_all, expand_slice) + offset_local
    activated_float, gelu_back = jax.vjp(exact_gelu, expanded)
    activated = activated_float.astype(jnp.bfloat16)
    activated_slope = product(cotangent_all, shrink_slice)
    expanded_slope = gelu_back(activated_slope)[0].astype(jnp.bfloat16)
    slope_part = product_transposed(expanded_slope, expand_slice).astype(jnp.bfloat16)
    normed_slope = lax.psum_scatter(slope_part, PLANE, scatter_dimension=0, tiled=True).astype(
        jnp.float32
    )
    output_part = product_transposed(activated, shrink_slice).astype(jnp.bfloat16)
    shrunk = lax.psum_scatter(output_part, PLANE, scatter_dimension=0, tiled=True)
    layer_output = (residual + shrunk.astype(jnp.float32) + shrink_offset).astype(jnp.bfloat16)

    cotangent_float = cotangent.astype(jnp.float32)
    residual_slope = cotangent_float + norm_back(
        normed_slope, middle_gain, middle_normal, middle_inverse
    )
    branch_slope = residual_slope.astype(jnp.bfloat16)
    attended_slope = product_transposed(branch_slope, mixing_whole).astype(jnp.bfloat16)
    slope_plane = lax.all_to_all(
        attended_slope.reshape(token_rows, plane_count, head_columns).transpose(1, 0, 2),
        PLANE,
        split_axis=0,
        concat_axis=0,
        tiled=True,
    )
    head_slopes = lax.all_to_all(
        slope_plane.reshape(groups, plane_rows // groups, head_columns),
        "rep",
        split_axis=0,
        concat_axis=0,
        tiled=True,
    ).reshape(plane_rows, local_heads, head_size)
    joint_heads = attention_backward(
        heads_kept, log_totals, head_slopes, places, key_last, score_scale
    )
    joint_slope = to_tokens(joint_heads.reshape(plane_rows, 3 * head_columns)).reshape(
        plane_rows, 3 * head_columns
    )
    entry_part = product_transposed(joint_slope, joint_slice).astype(jnp.bfloat16)
    entry_slope = lax.psum_scatter(entry_part, PLANE, scatter_dimension=0, tiled=True).astype(
        jnp.float32
    )
    input_gradient = (
        residual_slope + norm_back(entry_slope, entry_gain, entry_normal, entry_inverse)
    ).astype(jnp.bfloat16)

    slope_sums = jnp.sum(joint_slope.astype(jnp.float32), axis=0).reshape(local_heads, 3, head_size)

    def placed(piece, whole_size):
        return lax.dynamic_update_slice_in_dim(
            jnp.zeros((whole_size,), jnp.float32), piece, plane_index * piece.shape[0], 0
        )

    small_sums = lax.psum(
        (
            jnp.sum(entry_slope * entry_normal, axis=0),
            jnp.sum(entry_slope, axis=0),
            placed(slope_sums[:, 0].reshape(-1), width),
            placed(slope_sums[:, 2].reshape(-1), width),
            jnp.sum(branch_slope.astype(jnp.float32), axis=0),
            jnp.sum(normed_slope * middle_normal, axis=0),
            jnp.sum(normed_slope, axis=0),
            placed(jnp.sum(expanded_slope.astype(jnp.float32), axis=0), hidden_width),
            jnp.sum(cotangent_float, axis=0),
        ),
        EVERY,
    )
    shrink_gradient = owner_rows(row_outer(cotangent_all, activated), plane_count)
    expand_gradient = owner_rows(row_outer(middle_all, expanded_slope), plane_count)
    mixing_gradient = lax.psum_scatter(
        row_outer(attended, branch_slope).astype(jnp.bfloat16),
        EVERY,
        scatter_dimension=0,
        tiled=True,
    ).astype(jnp.float32)
    joint_gradient = owner_rows(row_outer(entry_all, joint_slope), plane_count)
    return (
        layer_output,
        input_gradient,
        small_sums[0],
        small_sums[1],
        joint_gradient,
        small_sums[2],
        small_sums[3],
        mixing_gradient,
        small_sums[4],
        small_sums[5],
        small_sums[6],
        expand_gradient,
        small_sums[7],
        shrink_gradient,
        small_sums[8],
    )


def solution(mesh):
    groups, sequence = mesh.shape["grp"], mesh.shape["seq"]
    subs = sequence // groups
    planes = Mesh(mesh.devices.reshape(groups, sequence // subs, subs), EVERY)
    rows, whole, group_rows = P(EVERY, None), P(), P("grp", None)
    return jax.shard_map(
        shards,
        mesh=planes,
        in_specs=(
            (rows, whole, whole, rows, whole, whole, rows, whole, whole, whole, rows, whole, rows)
            + (whole, group_rows, group_rows, rows)
        ),
        out_specs=(
            (rows, rows, whole, whole, rows, whole, whole, rows, whole, whole, whole, rows, whole)
            + (rows, whole)
        ),
        check_vma=False,
    )
```

```python
import functools
import jax
import jax.numpy as jnp
from jax import lax
from jax.experimental import pallas as pl
from jax.experimental.pallas import tpu as pltpu
from jax.sharding import Mesh, PartitionSpec as P
HEADS = 16
CONT = 256
PLANE = ('grp', 'sub')
EVERY = ('grp', 'rep', 'sub')
MESH = pl.DeviceIdType.MESH
ANY = pl.BlockSpec(memory_space=pl.ANY)
VMEM = pl.BlockSpec(memory_space=pltpu.VMEM)
DMA = pltpu.SemaphoreType.DMA
MIB = 1 << 20
norm_epsilon = 1e-05
masked_score = -1e+30
log2_e = 1.4426950408889634

def norm_terms(values):
    average = jnp.mean(values, axis=-1, keepdims=True)
    centered = values - average
    variance = jnp.mean(centered * centered, axis=-1, keepdims=True)
    inverse = lax.rsqrt(variance + norm_epsilon)
    return (centered * inverse, inverse)

def norm_back(slope, gain, normal, inverse):
    scaled = slope * gain
    return inverse * (scaled - jnp.mean(scaled, axis=-1, keepdims=True) - normal * jnp.mean(scaled * normal, axis=-1, keepdims=True))

def exact_gelu(values):
    return jax.nn.gelu(values, approximate=False)

def key_bounds(positions, lengths, prompt):
    segment = (positions - prompt) // CONT
    within = positions - prompt - segment * CONT
    slot_ids = jnp.arange(lengths.shape[0], dtype=jnp.int32)
    slot_limit = jnp.sum(jnp.where(segment[:, None] == slot_ids[None, :], lengths[None, :], 0), axis=1)
    last = prompt + (segment + 1) * CONT - 1
    last = jnp.where(within < slot_limit, last, -1)
    return jnp.where(positions < prompt, positions.shape[0], last)

def product(left_matrix, right_matrix):
    return jnp.dot(left_matrix, right_matrix, preferred_element_type=jnp.float32)

def product_transposed(left_matrix, right_matrix):
    return lax.dot_general(left_matrix, right_matrix, (((1,), (1,)), ((), ())), preferred_element_type=jnp.float32)

def row_outer(left_matrix, right_matrix):
    return lax.dot_general(left_matrix, right_matrix, (((0,), (0,)), ((), ())), preferred_element_type=jnp.float32)

def attention_forward(packed, places, key_last, heads):
    rows, columns = packed.shape
    size = columns // (3 * heads)
    block = 256
    factor = size ** (-0.5) * log2_e

    def kernel(q_ref, k_ref, v_ref, place_ref, first_ref, last_ref, out_ref, total_ref):
        scores = product_transposed(q_ref[...], k_ref[...])
        place = place_ref[...]
        allowed = (first_ref[...] <= place) & (place <= last_ref[...])
        scores = jnp.where(allowed, scores * factor, masked_score)
        top = jnp.max(scores, axis=1, keepdims=True)
        soft = jnp.exp2(scores - top)
        total = jnp.sum(soft, axis=1, keepdims=True)
        mixture = product(soft.astype(jnp.bfloat16), v_ref[...])
        out_ref[...] = (mixture / total).astype(jnp.bfloat16)
        log_total = jnp.broadcast_to(top + jnp.log2(total), (block, 128))
        total_ref[0] = log_total.T[:8]
    return pl.pallas_call(kernel, grid=(heads, rows // block), in_specs=[pl.BlockSpec((block, size), lambda h, i: (i, 3 * h)), pl.BlockSpec((rows, size), lambda h, i: (0, 3 * h + 1)), pl.BlockSpec((rows, size), lambda h, i: (0, 3 * h + 2)), pl.BlockSpec((block, 1), lambda h, i: (i, 0)), pl.BlockSpec((1, rows), lambda h, i: (0, 0)), pl.BlockSpec((1, rows), lambda h, i: (0, 0))], out_specs=[pl.BlockSpec((block, size), lambda h, i: (i, h)), pl.BlockSpec((1, 8, block), lambda h, i: (h, 0, i))], out_shape=[jax.ShapeDtypeStruct((rows, heads * size), jnp.bfloat16), jax.ShapeDtypeStruct((heads, 8, rows), jnp.float32)], compiler_params=pltpu.CompilerParams(vmem_limit_bytes=56 * MIB), cost_estimate=pl.CostEstimate(flops=4 * heads * rows * rows * size, bytes_accessed=4 * rows * heads * size * 2, transcendentals=heads * rows * rows), name='attention_forward')(packed, packed, packed, places[:, None], places[None, :], key_last[None, :])

def attention_backward(packed, totals, slopes, places, key_last, heads):
    rows, columns = packed.shape
    size = columns // (3 * heads)
    block = 256
    scale = size ** (-0.5)
    factor = scale * log2_e

    def kernel(q_ref, k_ref, v_ref, slope_ref, total_ref, place_ref, first_ref, last_ref, out_ref, turned_ref, key_sum, value_sum):
        step = pl.program_id(1)

        @pl.when(step == 0)
        def _():
            turned_ref[...] = k_ref[...].T
            key_sum[...] = jnp.zeros_like(key_sum)
            value_sum[...] = jnp.zeros_like(value_sum)
        queries = q_ref[...]
        slope = slope_ref[...]
        scores = product_transposed(k_ref[...], queries)
        place = place_ref[...]
        allowed = (first_ref[...] <= place) & (place <= last_ref[...])
        soft = jnp.where(allowed, jnp.exp2(scores * factor - total_ref[0, :1]), 0.0)
        weight_slope = product_transposed(v_ref[...], slope)
        centre = jnp.sum(soft * weight_slope, axis=0, keepdims=True)
        score_slope = (soft * (weight_slope - centre)).astype(jnp.bfloat16)
        value_sum[...] += product(soft.astype(jnp.bfloat16), slope)
        key_sum[...] += product(score_slope, queries)
        query_slope = product(turned_ref[...], score_slope)
        here = pl.ds(pl.multiple_of(step * block, block), block)
        out_ref[here, :size] = (query_slope.T * scale).astype(jnp.bfloat16)

        @pl.when(step == pl.num_programs(1) - 1)
        def _():
            out_ref[:, size:2 * size] = (key_sum[...] * scale).astype(jnp.bfloat16)
            out_ref[:, 2 * size:] = value_sum[...].astype(jnp.bfloat16)
    return pl.pallas_call(kernel, grid=(heads, rows // block), in_specs=[pl.BlockSpec((block, size), lambda h, i: (i, 3 * h)), pl.BlockSpec((rows, size), lambda h, i: (0, 3 * h + 1)), pl.BlockSpec((rows, size), lambda h, i: (0, 3 * h + 2)), pl.BlockSpec((block, size), lambda h, i: (i, h)), pl.BlockSpec((1, 8, block), lambda h, i: (h, 0, i)), pl.BlockSpec((1, block), lambda h, i: (0, i)), pl.BlockSpec((rows, 1), lambda h, i: (0, 0)), pl.BlockSpec((rows, 1), lambda h, i: (0, 0))], out_specs=pl.BlockSpec((rows, 3 * size), lambda h, i: (0, h)), out_shape=jax.ShapeDtypeStruct((rows, columns), jnp.bfloat16), scratch_shapes=[pltpu.VMEM((size, rows), jnp.bfloat16), pltpu.VMEM((rows, size), jnp.float32), pltpu.VMEM((rows, size), jnp.float32)], compiler_params=pltpu.CompilerParams(vmem_limit_bytes=56 * MIB), cost_estimate=pl.CostEstimate(flops=10 * heads * rows * rows * size, bytes_accessed=8 * rows * heads * size * 2, transcendentals=heads * rows * rows), name='attention_backward')(packed, packed, packed, slopes, totals, places[None, :], places[:, None], key_last[:, None])

def small_plane():
    return (lax.axis_size('grp'), lax.axis_size('sub')) == (4, 2)

def plane_ids():
    g, r, u = (lax.axis_index(n) for n in ('grp', 'rep', 'sub'))
    y, c = (g // 2, g % 2)
    across, up, partner = ((g, r, 1 - u), ((1 - y) * 2 + c, r, u), (y * 2 + 1 - c, r, u))

    def piece(k):
        return ((1 - y if k & 4 else y) * 2 + (1 - c if k & 2 else c)) * 2 + (1 - u if k & 1 else u)
    return (across, up, partner, piece)

def greet(devices):
    barrier = pltpu.get_barrier_semaphore()
    for device in devices:
        pl.semaphore_signal(barrier, inc=1, device_id=device, device_id_type=MESH)
    pl.semaphore_wait(barrier, len(devices))

def remote(source, target, send, recv, number, device):
    return pltpu.make_async_remote_copy(src_ref=source, dst_ref=target, send_sem=send.at[number], recv_sem=recv.at[number], device_id=device, device_id_type=MESH)

def gather_pieces(slots, send, recv, ids, on_piece):
    across, up, partner, _ = ids
    half = slots.shape[1] // 2
    low, high = (pl.ds(0, half), pl.ds(half, half))

    def copy(number, source, target, device):
        return remote(slots.at[source], slots.at[target], send, recv, number, device)
    x0 = copy(0, (0, low), (1, low), across)
    y1 = copy(1, (0, high), (4, high), up)
    x1 = copy(2, (0, high), (1, high), across)
    y0 = copy(3, (0, low), (4, low), up)
    own = copy(4, 0, 2, partner)
    started = [x0, y1, own, x1, y0]
    for one in started:
        one.start()
    on_piece(0)
    own.wait_recv()
    on_piece(2)

    def forward(number, source, target, device):
        one = copy(number, source, target, device)
        one.start()
        started.append(one)
        return one
    x0.wait_recv()
    d0 = forward(5, (1, low), (5, low), up)
    y1.wait_recv()
    d1 = forward(6, (4, high), (5, high), across)
    x1.wait_recv()
    px = forward(7, 1, 3, partner)
    on_piece(1)
    y0.wait_recv()
    py = forward(8, 4, 6, partner)
    on_piece(4)
    px.wait_recv()
    on_piece(3)
    py.wait_recv()
    on_piece(6)
    d0.wait_recv()
    p0 = forward(9, (5, low), (7, low), partner)
    d1.wait_recv()
    p1 = forward(10, (5, high), (7, high), partner)
    on_piece(5)
    p0.wait_recv()
    p1.wait_recv()
    on_piece(7)
    for one in started:
        one.wait_send()

def gather_kernel(parts, x_ref, out_ref, slots, load, send, recv, store):
    ids = plane_ids()
    first = pltpu.make_async_copy(x_ref, slots.at[0], load)
    first.start()
    greet(ids[:3])
    first.wait()
    stores = []
    small = slots.shape[1] // parts

    def on_piece(k):
        piece = ids[3](k)
        for part in range(parts):
            one = pltpu.make_async_copy(slots.at[k, pl.ds(part * small, small)], out_ref.at[piece // 2, part, lax.rem(piece, 2)], store.at[k, part])
            one.start()
            stores.append(one)
    gather_pieces(slots, send, recv, ids, on_piece)
    for one in stores:
        one.wait()

def plane_gather(x, collective_id, parts=1):
    rows, width = x.shape
    groups, _, subs = (lax.axis_size(n) for n in EVERY)
    if not small_plane():
        every = lax.all_gather(x, PLANE, axis=0).reshape(groups, subs, parts, rows // parts, width)
        return every.transpose(0, 2, 1, 3, 4).reshape(-1, width)
    return pl.pallas_call(functools.partial(gather_kernel, parts), out_shape=jax.ShapeDtypeStruct((groups, parts, subs, rows // parts, width), x.dtype), in_specs=[ANY], out_specs=ANY, scratch_shapes=[pltpu.VMEM((8, rows, width), x.dtype), DMA, DMA((11,)), DMA((11,)), DMA((8, parts))], compiler_params=pltpu.CompilerParams(collective_id=collective_id, has_side_effects=True, vmem_limit_bytes=40 * MIB), name='plane_gather')(x).reshape(-1, width)

def reduce_scratch(rows, width):
    f, h = (jnp.float32, jnp.bfloat16)
    return [pltpu.VMEM((4, rows, width), f), pltpu.VMEM((4, rows, width), h), pltpu.VMEM((4, rows, width), h), pltpu.VMEM((3, rows, width), h), pltpu.VMEM((3, rows, width), h), DMA((10,)), DMA((10,))]
SUM = {0: 0, 1: 1, 4: 2, 5: 3}

def reduce_pieces(refs, ids, make_piece, out):
    sums, give, take, leave, come, send, recv = refs
    across, up, partner, _ = ids
    half = sums.shape[1] // 2
    low, high = (pl.ds(0, half), pl.ds(half, half))
    started = []

    def start(number, source, target, device):
        one = remote(source, target, send, recv, number, device)
        one.start()
        started.append(one)
        return one

    def pair(k, number):
        give[SUM[k]] = make_piece(k + 2).astype(jnp.bfloat16)
        one = start(number, give.at[SUM[k]], take.at[SUM[k]], partner)
        sums[SUM[k]] = make_piece(k)
        return one

    def settle(k, one):
        one.wait_recv()
        sums[SUM[k]] += take[SUM[k]].astype(jnp.float32)
    settle(5, pair(5, 0))
    leave[2] = sums[3].astype(jnp.bfloat16)
    dx = start(4, leave.at[2, low], come.at[2, low], across)
    dy = start(5, leave.at[2, high], come.at[2, high], up)
    settle(1, pair(1, 1))
    leave[0, low] = sums[1, low].astype(jnp.bfloat16)
    xl = start(6, leave.at[0, low], come.at[0, low], across)
    settle(4, pair(4, 2))
    leave[1, high] = sums[2, high].astype(jnp.bfloat16)
    yh = start(7, leave.at[1, high], come.at[1, high], up)
    last = pair(0, 3)
    dy.wait_recv()
    leave[0, high] = (sums[1, high] + come[2, high].astype(jnp.float32)).astype(jnp.bfloat16)
    xh = start(8, leave.at[0, high], come.at[0, high], across)
    dx.wait_recv()
    leave[1, low] = (sums[2, low] + come[2, low].astype(jnp.float32)).astype(jnp.bfloat16)
    yl = start(9, leave.at[1, low], come.at[1, low], up)
    settle(0, last)
    for one in (xl, yh, xh, yl):
        one.wait_recv()
    out[...] = sums[0] + come[0].astype(jnp.float32) + come[1].astype(jnp.float32)
    for one in started:
        one.wait_send()

def product_reduce_kernel(slope_ref, weight_ref, out_ref, slopes, load, *refs):
    ids = plane_ids()
    order = (7, 5, 3, 1, 6, 4, 2, 0)
    loads = {k: pltpu.make_async_copy(slope_ref.at[ids[3](k)], slopes.at[k], load.at[k]) for k in order}
    for k in order:
        loads[k].start()
    greet(ids[:3])

    def make_piece(k):
        loads[k].wait()
        return lax.dot_general(slopes[k], weight_ref[...], (((1,), (1,)), ((), ())), preferred_element_type=jnp.float32)
    reduce_pieces(refs, ids, make_piece, out_ref)

def product_reduce(slopes, weight, collective_id):
    if not small_plane():
        part = product_transposed(slopes.reshape(-1, slopes.shape[2]), weight)
        return lax.psum_scatter(part.astype(jnp.bfloat16), PLANE, scatter_dimension=0, tiled=True).astype(jnp.float32)
    count, rows, inner = slopes.shape
    width = weight.shape[0]
    return pl.pallas_call(product_reduce_kernel, out_shape=jax.ShapeDtypeStruct((rows, width), jnp.float32), in_specs=[ANY, VMEM], out_specs=VMEM, scratch_shapes=[pltpu.VMEM((8, rows, inner), slopes.dtype), DMA((8,)), *reduce_scratch(rows, width)], compiler_params=pltpu.CompilerParams(collective_id=collective_id, has_side_effects=True, vmem_limit_bytes=60 << 20), name='product_reduce')(slopes, weight)

def total_kernel(x_ref, out_ref, *refs):
    axes = ('grp', 'rep', 'sub')
    here = {n: lax.axis_index(n) for n in axes}
    phases = ('grp', 'sub', 'rep')

    def other(name, step):
        size = lax.axis_size(name)
        return tuple((lax.rem(here[n] + step, size) if n == name else here[n] for n in axes))
    greet([other(n, s) for n in phases for s in range(1, lax.axis_size(n))])
    out_ref[...] = x_ref[...]
    for j, name in enumerate(phases):
        slots, send, recv = refs[3 * j:3 * j + 3]
        size = lax.axis_size(name)
        me = here[name]
        slots[me] = out_ref[...]
        copies = []
        for s in range(1, size):
            one = pltpu.make_async_remote_copy(src_ref=out_ref, dst_ref=slots.at[me], send_sem=send.at[s], recv_sem=recv.at[s], device_id=other(name, s), device_id_type=MESH)
            one.start()
            copies.append(one)
        for one in copies:
            one.wait_recv()
        for one in copies:
            one.wait_send()
        value = slots[0]
        for s in range(1, size):
            value = value + slots[s]
        out_ref[...] = value

def total_everywhere(x, collective_id):
    scratch = []
    for name in ('grp', 'sub', 'rep'):
        n = lax.axis_size(name)
        scratch += [pltpu.VMEM((n,) + x.shape, x.dtype), DMA((n,)), DMA((n,))]
    return pl.pallas_call(total_kernel, out_shape=jax.ShapeDtypeStruct(x.shape, x.dtype), in_specs=[VMEM], out_specs=VMEM, scratch_shapes=scratch, compiler_params=pltpu.CompilerParams(collective_id=collective_id, has_side_effects=True), name='total_everywhere')(x)

def exchange_kernel(to_tokens, x_ref, out_ref, send, recv, local):
    groups, reps, subs = (lax.axis_size(n) for n in EVERY)
    g, r, u = (lax.axis_index(n) for n in EVERY)
    count = groups * subs
    place = g * subs + u
    if to_tokens:
        tokens, width = (out_ref.shape[0], x_ref.shape[1])
    else:
        tokens, width = (x_ref.shape[0], out_ref.shape[1])

    def rows(ref, t):
        return ref.at[pl.ds(pl.multiple_of(t * tokens, tokens), tokens), :]

    def columns(ref, t):
        return ref.at[:, pl.ds(pl.multiple_of(t * width, width), width)]
    source, target = (rows, columns) if to_tokens else (columns, rows)
    peers = [lax.rem(place + step, count) for step in range(1, count)]

    def device(t):
        return (t // subs, r, lax.rem(t, subs))
    own = pltpu.make_async_copy(source(x_ref, place), target(out_ref, place), local)
    own.start()
    greet([device(t) for t in peers])
    copies = []
    for step, t in enumerate(peers):
        one = pltpu.make_async_remote_copy(src_ref=source(x_ref, t), dst_ref=target(out_ref, place), send_sem=send.at[step], recv_sem=recv.at[step], device_id=device(t), device_id_type=MESH)
        one.start()
        copies.append(one)
    own.wait()
    for one in copies:
        one.wait_recv()
    for one in copies:
        one.wait_send()

def exchange(x, to_tokens, collective_id):
    count = lax.axis_size('grp') * lax.axis_size('sub')
    shape = (x.shape[0] // count, x.shape[1] * count) if to_tokens else (x.shape[0] * count, x.shape[1] // count)
    return pl.pallas_call(functools.partial(exchange_kernel, to_tokens), out_shape=jax.ShapeDtypeStruct(shape, x.dtype), in_specs=[ANY], out_specs=ANY, scratch_shapes=[DMA((count - 1,)), DMA((count - 1,)), DMA], compiler_params=pltpu.CompilerParams(collective_id=collective_id, has_side_effects=True), name='to_tokens' if to_tokens else 'to_heads')(x)

def outer_reduce_kernel(left_ref, right_ref, out_ref, *refs):
    ids = plane_ids()
    greet(ids[:3])
    wide = left_ref.shape[1] // 8

    def make_piece(k):
        block = left_ref[:, pl.ds(pl.multiple_of(ids[3](k) * wide, wide), wide)]
        return row_outer(block, right_ref[...])
    reduce_pieces(refs, ids, make_piece, out_ref)

def outer_reduce(left, right, collective_id):
    if not small_plane():
        return lax.psum_scatter(row_outer(left, right).astype(jnp.bfloat16), PLANE, scatter_dimension=0, tiled=True).astype(jnp.float32)
    rows, width = (left.shape[1] // 8, right.shape[1])
    return pl.pallas_call(outer_reduce_kernel, out_shape=jax.ShapeDtypeStruct((rows, width), jnp.float32), in_specs=[VMEM, VMEM], out_specs=VMEM, scratch_shapes=reduce_scratch(rows, width), compiler_params=pltpu.CompilerParams(collective_id=collective_id, has_side_effects=True, vmem_limit_bytes=60 * MIB), name='outer_reduce')(left, right)

def plane_of(group):
    groups = lax.axis_size('grp')
    return lax.rem(group, 2) * (groups // 2) + group // 2

def group_of(plane):
    groups = lax.axis_size('grp')
    return lax.rem(plane, groups // 2) * 2 + plane // (groups // 2)

def opening_kernel(x_ref, w_ref, moved_ref, columns_ref, move_send, move_recv, send, recv, local):
    groups, reps, subs = (lax.axis_size(n) for n in EVERY)
    g, r, u = (lax.axis_index(n) for n in EVERY)
    count = groups * subs
    place = g * subs + u
    rows, width = (w_ref.shape[0], columns_ref.shape[1])
    peers = [lax.rem(place + step, count) for step in range(1, count)]

    def device(t):
        return (t // subs, r, lax.rem(t, subs))
    target, source = ((r, plane_of(g), u), (group_of(r), g, u))
    stays = (r == g) & (plane_of(g) == r)

    def block(t):
        return w_ref.at[:, pl.ds(pl.multiple_of(t * width, width), width)]
    landing = columns_ref.at[pl.ds(pl.multiple_of(place * rows, rows), rows), :]
    own = pltpu.make_async_copy(block(place), landing, local.at[0])
    own.start()
    kept = pltpu.make_async_copy(x_ref, moved_ref, local.at[1])
    moved = pltpu.make_async_remote_copy(src_ref=x_ref, dst_ref=moved_ref, send_sem=move_send, recv_sem=move_recv, device_id=target, device_id_type=MESH)
    barrier = pltpu.get_barrier_semaphore()
    for t in peers:
        pl.semaphore_signal(barrier, inc=1, device_id=device(t), device_id_type=MESH)

    @pl.when(stays)
    def _():
        kept.start()

    @pl.when(jnp.logical_not(stays))
    def _():
        pl.semaphore_signal(barrier, inc=1, device_id=source, device_id_type=MESH)
    pl.semaphore_wait(barrier, count - stays.astype(jnp.int32))

    @pl.when(jnp.logical_not(stays))
    def _():
        moved.start()
    copies = []
    for step, t in enumerate(peers):
        one = pltpu.make_async_remote_copy(src_ref=block(t), dst_ref=landing, send_sem=send.at[step], recv_sem=recv.at[step], device_id=device(t), device_id_type=MESH)
        one.start()
        copies.append(one)
    own.wait()
    for one in copies:
        one.wait_recv()
    for one in copies:
        one.wait_send()

    @pl.when(stays)
    def _():
        kept.wait()

    @pl.when(jnp.logical_not(stays))
    def _():
        moved.wait_recv()
        moved.wait_send()

def opening(x, weight, collective_id):
    count = lax.axis_size('grp') * lax.axis_size('sub')
    columns = jax.ShapeDtypeStruct((weight.shape[0] * count, weight.shape[1] // count), weight.dtype)
    return pl.pallas_call(opening_kernel, out_shape=[jax.ShapeDtypeStruct(x.shape, x.dtype), columns], in_specs=[VMEM, ANY], out_specs=[VMEM, ANY], scratch_shapes=[DMA, DMA, DMA((count - 1,)), DMA((count - 1,)), DMA((2,))], compiler_params=pltpu.CompilerParams(collective_id=collective_id, has_side_effects=True), name='opening')(x, weight)

def rep_rows(own):
    groups, reps, subs = (lax.axis_size(name) for name in EVERY)
    every = lax.all_gather(own, 'rep', axis=0, tiled=True)
    every = every.reshape(reps, groups, subs, -1, own.shape[1]).transpose(1, 0, 2, 3, 4)
    return every.reshape(-1, own.shape[1])

def rep_sums(gradient):
    groups, reps, subs = (lax.axis_size(name) for name in EVERY)
    columns = gradient.shape[1]
    ordered = gradient.astype(jnp.bfloat16).reshape(groups, reps, subs, -1, columns)
    ordered = ordered.transpose(1, 0, 2, 3, 4).reshape(-1, columns)
    return lax.psum_scatter(ordered, 'rep', scatter_dimension=0, tiled=True)

def shards(layer_input, entry_gain, entry_shift, joint_weight, query_offset, value_offset, mixing_weight, attention_offset, middle_gain, middle_shift, expand_weight, expand_offset, shrink_weight, shrink_offset, placement, slot_lengths, cotangent):
    token_rows, width = layer_input.shape
    hidden_width = expand_weight.shape[1]
    groups, reps, subs = (lax.axis_size(name) for name in EVERY)
    plane_count = groups * subs
    plane_index = lax.axis_index(PLANE)
    head_size = width // HEADS
    local_heads = HEADS // plane_count
    head_columns = local_heads * head_size
    plane_rows = plane_count * token_rows
    home = [g * reps * subs + r * subs + u for g in range(groups) for r in range(reps) for u in range(subs)]
    away = [(r * reps + g % 2 * (groups // 2) + g // 2) * subs + u for g in range(groups) for r in range(reps) for u in range(subs)]

    def to_plane(array):
        return lax.ppermute(array, EVERY, list(zip(home, away)))

    def from_plane(array):
        return lax.ppermute(array, EVERY, list(zip(away, home)))
    facts = to_plane(jnp.concatenate([placement, slot_lengths], axis=1))[0]
    mixing_own = lax.all_gather(mixing_weight, 'rep', axis=0, tiled=True)
    moved_input, joint_own = opening(layer_input, joint_weight, 12)
    input_float = moved_input.astype(jnp.float32)
    joint_slice = rep_rows(joint_own)
    entry_normal, entry_inverse = norm_terms(input_float)
    entry_normed = (entry_normal * entry_gain + entry_shift).astype(jnp.bfloat16)
    entry_all = plane_gather(entry_normed, 1)
    expand_weight, shrink_weight, cotangent, facts, entry_all = lax.optimization_barrier((expand_weight, shrink_weight, cotangent, facts, entry_all))
    places, lengths = (facts[:placement.shape[1]], facts[placement.shape[1]:])
    prompt = places.shape[0] // 2
    key_last = key_bounds(places, lengths, prompt)
    expand_slice = rep_rows(exchange(expand_weight, False, 13))
    shrink_own = exchange(shrink_weight, False, 14)
    shrink_slice = rep_rows(shrink_own)
    cotangent, shrink_own = lax.optimization_barrier((cotangent, shrink_own))
    cotangent = to_plane(cotangent)
    offsets = jnp.stack([query_offset.reshape(HEADS, head_size), jnp.zeros((HEADS, head_size), jnp.float32), value_offset.reshape(HEADS, head_size)], axis=1).reshape(-1)
    offsets = lax.dynamic_slice_in_dim(offsets, plane_index * 3 * head_columns, 3 * head_columns)
    heads_kept = (product(entry_all, joint_slice) + offsets).astype(jnp.bfloat16)
    mixture, log_totals = attention_forward(heads_kept, places, key_last, local_heads)
    attended = exchange(mixture, True, 3)
    mixing_own, cotangent, attended = lax.optimization_barrier((mixing_own, cotangent, attended))
    mixing_whole = plane_gather(mixing_own, 2, reps)
    residual = input_float + (product(attended, mixing_whole) + attention_offset)
    middle_normal, middle_inverse = norm_terms(residual)
    middle_normed = (middle_normal * middle_gain + middle_shift).astype(jnp.bfloat16)
    middle_all = plane_gather(middle_normed, 5)
    cotangent, middle_all = lax.optimization_barrier((cotangent, middle_all))
    cotangent_all = plane_gather(cotangent, 4)
    hidden_local = hidden_width // plane_count
    offset_local = lax.dynamic_slice_in_dim(expand_offset, plane_index * hidden_local, hidden_local)
    expanded = product(middle_all, expand_slice) + offset_local
    activated_float, gelu_back = jax.vjp(exact_gelu, expanded)
    activated = activated_float.astype(jnp.bfloat16)
    shrink_part = row_outer(cotangent_all, activated).astype(jnp.bfloat16)
    shrink_part, cotangent_all = lax.optimization_barrier((shrink_part, cotangent_all))
    shrink_sums = rep_sums(shrink_part)
    activated_slope = product(cotangent_all, shrink_slice)
    expanded_slope = gelu_back(activated_slope)[0].astype(jnp.bfloat16)
    normed_slope = product_reduce(expanded_slope.reshape(plane_count, token_rows, hidden_local), expand_slice, 6)
    normed_slope, middle_all = lax.optimization_barrier((normed_slope, middle_all))
    expand_part = row_outer(middle_all, expanded_slope).astype(jnp.bfloat16)
    expand_part, normed_slope = lax.optimization_barrier((expand_part, normed_slope))
    expand_sums = rep_sums(expand_part)
    cotangent_float = cotangent.astype(jnp.float32)
    residual_slope = cotangent_float + norm_back(normed_slope, middle_gain, middle_normal, middle_inverse)
    branch_slope = residual_slope.astype(jnp.bfloat16)
    attended_slope = product_transposed(branch_slope, mixing_whole).astype(jnp.bfloat16)
    head_slopes = exchange(attended_slope, False, 7)
    joint_slope = attention_backward(heads_kept, log_totals, head_slopes, places, key_last, local_heads)
    shrink_sums, joint_slope = lax.optimization_barrier((shrink_sums, joint_slope))
    joint_part = row_outer(entry_all, joint_slope).astype(jnp.bfloat16)
    joint_part, joint_slope = lax.optimization_barrier((joint_part, joint_slope))
    joint_sums = rep_sums(joint_part)
    entry_slope = product_reduce(joint_slope.reshape(plane_count, token_rows, 3 * head_columns), joint_slice, 9)
    expand_sums, entry_slope = lax.optimization_barrier((expand_sums, entry_slope))
    input_gradient = from_plane((residual_slope + norm_back(entry_slope, entry_gain, entry_normal, entry_inverse)).astype(jnp.bfloat16))
    activated, attended, entry_slope = lax.optimization_barrier((activated, attended, entry_slope))
    shrunk = product_reduce(activated.reshape(plane_count, token_rows, hidden_local), shrink_slice, 8)
    joint_sums, shrunk = lax.optimization_barrier((joint_sums, shrunk))
    layer_output = from_plane((residual + shrunk + shrink_offset).astype(jnp.bfloat16))
    attended_by_sub = attended.reshape(token_rows, groups, reps, subs, -1).transpose(0, 1, 3, 2, 4)
    mixing_sums = outer_reduce(attended_by_sub.reshape(token_rows, width), branch_slope, 11)
    mixing_gradient = lax.psum_scatter(mixing_sums.astype(jnp.bfloat16), 'rep', scatter_dimension=0, tiled=True).astype(jnp.float32)
    slope_sums = jnp.sum(joint_slope.astype(jnp.float32), axis=0).reshape(local_heads, 3, head_size)

    def placed(piece, whole_size):
        return lax.dynamic_update_slice_in_dim(jnp.zeros((whole_size,), jnp.float32), piece, plane_index * piece.shape[0], 0)
    small = [jnp.sum(entry_slope * entry_normal, axis=0), jnp.sum(entry_slope, axis=0), placed(slope_sums[:, 0].reshape(-1), width), placed(slope_sums[:, 2].reshape(-1), width), jnp.sum(branch_slope.astype(jnp.float32), axis=0), jnp.sum(normed_slope * middle_normal, axis=0), jnp.sum(normed_slope, axis=0), placed(jnp.sum(expanded_slope.astype(jnp.float32), axis=0), hidden_width), jnp.sum(cotangent_float, axis=0)]
    small_all = total_everywhere(jnp.concatenate(small).reshape(-1, 128), 10).reshape(-1)
    small_sums, first = ([], 0)
    for piece in small:
        small_sums.append(small_all[first:first + piece.shape[0]])
        first += piece.shape[0]
    shrink_gradient = exchange(shrink_sums, True, 15).astype(jnp.float32)
    expand_gradient = exchange(expand_sums, True, 16).astype(jnp.float32)
    joint_gradient = exchange(joint_sums, True, 17).astype(jnp.float32)
    return (layer_output, input_gradient, small_sums[0], small_sums[1], joint_gradient, small_sums[2], small_sums[3], mixing_gradient, small_sums[4], small_sums[5], small_sums[6], expand_gradient, small_sums[7], shrink_gradient, small_sums[8])

def solution(mesh):
    groups, sequence = (mesh.shape['grp'], mesh.shape['seq'])
    subs = sequence // groups
    planes = Mesh(mesh.devices.reshape(groups, sequence // subs, subs), EVERY)
    rows, whole, group_rows = (P(EVERY, None), P(), P('grp', None))
    return jax.shard_map(shards, mesh=planes, in_specs=(rows, whole, whole, rows, whole, whole, rows, whole, whole, whole, rows, whole, rows) + (whole, group_rows, group_rows, rows), out_specs=(rows, rows, whole, whole, rows, whole, whole, rows, whole, whole, whole, rows, whole) + (rows, whole), check_vma=False)
```

```python
import functools
import jax
import jax.numpy as jnp
from jax import lax
from jax.experimental import pallas as pl
from jax.experimental.pallas import tpu as pltpu
from jax.sharding import Mesh, PartitionSpec as P
HEADS = 16
CONT = 256
PLANE = ('grp', 'sub')
EVERY = ('grp', 'rep', 'sub')
MESH = pl.DeviceIdType.MESH
ANY = pl.BlockSpec(memory_space=pl.ANY)
VMEM = pl.BlockSpec(memory_space=pltpu.VMEM)
DMA = pltpu.SemaphoreType.DMA
MIB = 1 << 20
norm_epsilon = 1e-05
masked_score = -1e+30
log2_e = 1.4426950408889634

def norm_terms(values):
    average = jnp.mean(values, axis=-1, keepdims=True)
    centered = values - average
    variance = jnp.mean(centered * centered, axis=-1, keepdims=True)
    inverse = lax.rsqrt(variance + norm_epsilon)
    return (centered * inverse, inverse)

def norm_back(slope, gain, normal, inverse):
    scaled = slope * gain
    return inverse * (scaled - jnp.mean(scaled, axis=-1, keepdims=True) - normal * jnp.mean(scaled * normal, axis=-1, keepdims=True))

def exact_gelu(values):
    return jax.nn.gelu(values, approximate=False)

def key_bounds(positions, lengths, prompt):
    segment = (positions - prompt) // CONT
    within = positions - prompt - segment * CONT
    slot_ids = jnp.arange(lengths.shape[0], dtype=jnp.int32)
    slot_limit = jnp.sum(jnp.where(segment[:, None] == slot_ids[None, :], lengths[None, :], 0), axis=1)
    last = prompt + (segment + 1) * CONT - 1
    last = jnp.where(within < slot_limit, last, -1)
    return jnp.where(positions < prompt, positions.shape[0], last)

def product(left_matrix, right_matrix):
    return jnp.dot(left_matrix, right_matrix, preferred_element_type=jnp.float32)

def product_transposed(left_matrix, right_matrix):
    return lax.dot_general(left_matrix, right_matrix, (((1,), (1,)), ((), ())), preferred_element_type=jnp.float32)

def row_outer(left_matrix, right_matrix):
    return lax.dot_general(left_matrix, right_matrix, (((0,), (0,)), ((), ())), preferred_element_type=jnp.float32)

def attention_forward(packed, places, key_last, heads):
    rows, columns = packed.shape
    size = columns // (3 * heads)
    block = 256
    factor = size ** (-0.5) * log2_e

    def kernel(q_ref, k_ref, v_ref, place_ref, first_ref, last_ref, out_ref, total_ref):
        scores = product_transposed(q_ref[...], k_ref[...])
        place = place_ref[...]
        allowed = (first_ref[...] <= place) & (place <= last_ref[...])
        scores = jnp.where(allowed, scores * factor, masked_score)
        top = jnp.max(scores, axis=1, keepdims=True)
        soft = jnp.exp2(scores - top)
        total = jnp.sum(soft, axis=1, keepdims=True)
        mixture = product(soft.astype(jnp.bfloat16), v_ref[...])
        out_ref[...] = (mixture / total).astype(jnp.bfloat16)
        log_total = jnp.broadcast_to(top + jnp.log2(total), (block, 128))
        total_ref[0] = log_total.T[:8]
    return pl.pallas_call(kernel, grid=(heads, rows // block), in_specs=[pl.BlockSpec((block, size), lambda h, i: (i, 3 * h)), pl.BlockSpec((rows, size), lambda h, i: (0, 3 * h + 1)), pl.BlockSpec((rows, size), lambda h, i: (0, 3 * h + 2)), pl.BlockSpec((block, 1), lambda h, i: (i, 0)), pl.BlockSpec((1, rows), lambda h, i: (0, 0)), pl.BlockSpec((1, rows), lambda h, i: (0, 0))], out_specs=[pl.BlockSpec((block, size), lambda h, i: (i, h)), pl.BlockSpec((1, 8, block), lambda h, i: (h, 0, i))], out_shape=[jax.ShapeDtypeStruct((rows, heads * size), jnp.bfloat16), jax.ShapeDtypeStruct((heads, 8, rows), jnp.float32)], compiler_params=pltpu.CompilerParams(vmem_limit_bytes=56 * MIB), cost_estimate=pl.CostEstimate(flops=4 * heads * rows * rows * size, bytes_accessed=4 * rows * heads * size * 2, transcendentals=heads * rows * rows), name='attention_forward')(packed, packed, packed, places[:, None], places[None, :], key_last[None, :])

def attention_backward(packed, totals, slopes, places, key_last, heads):
    rows, columns = packed.shape
    size = columns // (3 * heads)
    block = 256
    scale = size ** (-0.5)
    factor = scale * log2_e

    def kernel(q_ref, k_ref, v_ref, slope_ref, total_ref, place_ref, first_ref, last_ref, out_ref, turned_ref, key_sum, value_sum):
        step = pl.program_id(1)

        @pl.when(step == 0)
        def _():
            turned_ref[...] = k_ref[...].T
            key_sum[...] = jnp.zeros_like(key_sum)
            value_sum[...] = jnp.zeros_like(value_sum)
        queries = q_ref[...]
        slope = slope_ref[...]
        scores = product_transposed(k_ref[...], queries)
        place = place_ref[...]
        allowed = (first_ref[...] <= place) & (place <= last_ref[...])
        soft = jnp.where(allowed, jnp.exp2(scores * factor - total_ref[0, :1]), 0.0)
        weight_slope = product_transposed(v_ref[...], slope)
        centre = jnp.sum(soft * weight_slope, axis=0, keepdims=True)
        score_slope = (soft * (weight_slope - centre)).astype(jnp.bfloat16)
        value_sum[...] += product(soft.astype(jnp.bfloat16), slope)
        key_sum[...] += product(score_slope, queries)
        query_slope = product(turned_ref[...], score_slope)
        here = pl.ds(pl.multiple_of(step * block, block), block)
        out_ref[here, :size] = (query_slope.T * scale).astype(jnp.bfloat16)

        @pl.when(step == pl.num_programs(1) - 1)
        def _():
            out_ref[:, size:2 * size] = (key_sum[...] * scale).astype(jnp.bfloat16)
            out_ref[:, 2 * size:] = value_sum[...].astype(jnp.bfloat16)
    return pl.pallas_call(kernel, grid=(heads, rows // block), in_specs=[pl.BlockSpec((block, size), lambda h, i: (i, 3 * h)), pl.BlockSpec((rows, size), lambda h, i: (0, 3 * h + 1)), pl.BlockSpec((rows, size), lambda h, i: (0, 3 * h + 2)), pl.BlockSpec((block, size), lambda h, i: (i, h)), pl.BlockSpec((1, 8, block), lambda h, i: (h, 0, i)), pl.BlockSpec((1, block), lambda h, i: (0, i)), pl.BlockSpec((rows, 1), lambda h, i: (0, 0)), pl.BlockSpec((rows, 1), lambda h, i: (0, 0))], out_specs=pl.BlockSpec((rows, 3 * size), lambda h, i: (0, h)), out_shape=jax.ShapeDtypeStruct((rows, columns), jnp.bfloat16), scratch_shapes=[pltpu.VMEM((size, rows), jnp.bfloat16), pltpu.VMEM((rows, size), jnp.float32), pltpu.VMEM((rows, size), jnp.float32)], compiler_params=pltpu.CompilerParams(vmem_limit_bytes=56 * MIB), cost_estimate=pl.CostEstimate(flops=10 * heads * rows * rows * size, bytes_accessed=8 * rows * heads * size * 2, transcendentals=heads * rows * rows), name='attention_backward')(packed, packed, packed, slopes, totals, places[None, :], places[:, None], key_last[:, None])

def small_plane():
    return (lax.axis_size('grp'), lax.axis_size('sub')) == (4, 2)

def plane_ids():
    g, r, u = (lax.axis_index(n) for n in ('grp', 'rep', 'sub'))
    y, c = (g // 2, g % 2)
    across, up, partner = ((g, r, 1 - u), ((1 - y) * 2 + c, r, u), (y * 2 + 1 - c, r, u))

    def piece(k):
        above, beside, side = (k // 4, k // 2 % 2, k % 2)
        return ((y + above) % 2 * 2 + (c + beside) % 2) * 2 + (u + side) % 2
    return (across, up, partner, piece)

def greet(devices):
    barrier = pltpu.get_barrier_semaphore()
    for device in devices:
        pl.semaphore_signal(barrier, inc=1, device_id=device, device_id_type=MESH)
    pl.semaphore_wait(barrier, len(devices))

def remote(source, target, send, recv, number, device):
    return pltpu.make_async_remote_copy(src_ref=source, dst_ref=target, send_sem=send.at[number], recv_sem=recv.at[number], device_id=device, device_id_type=MESH)

def gather_pieces(slots, send, recv, ids, on_piece):
    across, up, partner, _ = ids
    half = slots.shape[1] // 2
    low, high = (pl.ds(0, half), pl.ds(half, half))

    def copy(number, source, target, device):
        return remote(slots.at[source], slots.at[target], send, recv, number, device)
    x0 = copy(0, (0, low), (1, low), across)
    y1 = copy(1, (0, high), (4, high), up)
    x1 = copy(2, (0, high), (1, high), across)
    y0 = copy(3, (0, low), (4, low), up)
    own = copy(4, 0, 2, partner)
    started = [x0, y1, own, x1, y0]
    for one in started:
        one.start()
    on_piece(0)
    own.wait_recv()
    on_piece(2)

    def forward(number, source, target, device):
        one = copy(number, source, target, device)
        one.start()
        started.append(one)
        return one
    x0.wait_recv()
    d0 = forward(5, (1, low), (5, low), up)
    y1.wait_recv()
    d1 = forward(6, (4, high), (5, high), across)
    x1.wait_recv()
    px = forward(7, 1, 3, partner)
    on_piece(1)
    y0.wait_recv()
    py = forward(8, 4, 6, partner)
    on_piece(4)
    px.wait_recv()
    on_piece(3)
    py.wait_recv()
    on_piece(6)
    d0.wait_recv()
    p0 = forward(9, (5, low), (7, low), partner)
    d1.wait_recv()
    p1 = forward(10, (5, high), (7, high), partner)
    on_piece(5)
    p0.wait_recv()
    p1.wait_recv()
    on_piece(7)
    for one in started:
        one.wait_send()

def gather_kernel(parts, x_ref, out_ref, slots, load, send, recv, store):
    ids = plane_ids()
    first = pltpu.make_async_copy(x_ref, slots.at[0], load)
    first.start()
    greet(ids[:3])
    first.wait()
    stores = []
    small = slots.shape[1] // parts

    def on_piece(k):
        piece = ids[3](k)
        for part in range(parts):
            one = pltpu.make_async_copy(slots.at[k, pl.ds(part * small, small)], out_ref.at[piece // 2, part, lax.rem(piece, 2)], store.at[k, part])
            one.start()
            stores.append(one)
    gather_pieces(slots, send, recv, ids, on_piece)
    for one in stores:
        one.wait()

def plane_gather(x, collective_id, parts=1):
    rows, width = x.shape
    groups, _, subs = (lax.axis_size(n) for n in EVERY)
    if not small_plane():
        every = lax.all_gather(x, PLANE, axis=0).reshape(groups, subs, parts, rows // parts, width)
        return every.transpose(0, 2, 1, 3, 4).reshape(-1, width)
    return pl.pallas_call(functools.partial(gather_kernel, parts), out_shape=jax.ShapeDtypeStruct((groups, parts, subs, rows // parts, width), x.dtype), in_specs=[ANY], out_specs=ANY, scratch_shapes=[pltpu.VMEM((8, rows, width), x.dtype), DMA, DMA((11,)), DMA((11,)), DMA((8, parts))], compiler_params=pltpu.CompilerParams(collective_id=collective_id, has_side_effects=True, vmem_limit_bytes=40 * MIB), name='plane_gather')(x).reshape(-1, width)

def reduce_scratch(rows, width):
    wide, narrow = (jnp.float32, jnp.bfloat16)
    return [pltpu.VMEM((4, rows, width), wide), pltpu.VMEM((4, rows, width), narrow), pltpu.VMEM((4, rows, width), narrow), pltpu.VMEM((3, rows, width), narrow), pltpu.VMEM((3, rows, width), narrow), DMA((10,)), DMA((10,))]

def reduce_order(step):
    return 7 - 2 * step + 7 * (step // 4)

def reduce_step(step, piece, refs, ids, out):
    sums, give, take, leave, come, send, recv = refs
    across, up, partner, _ = ids
    half = sums.shape[1] // 2
    low, high = (pl.ds(0, half), pl.ds(half, half))
    pair = step // 2

    def to_partner(number):
        return remote(give.at[number], take.at[number], send, recv, number, partner)

    def part(number, which, rows, device):
        return remote(leave.at[which, rows], come.at[which, rows], send, recv, number, device)

    def down(value):
        return value.astype(jnp.bfloat16)

    def up_cast(value):
        return value.astype(jnp.float32)

    @pl.when(lax.rem(step, 2) == 0)
    def _():
        give[pair] = down(piece)
        to_partner(pair).start()

    @pl.when(lax.rem(step, 2) == 1)
    def _():
        sums[pair] = piece
        to_partner(pair).wait_recv()
        sums[pair] += up_cast(take[pair])
    diagonal_across, diagonal_up = (part(4, 2, low, across), part(5, 2, high, up))
    across_low, up_high = (part(6, 0, low, across), part(7, 1, high, up))
    across_high, up_low = (part(8, 0, high, across), part(9, 1, low, up))

    @pl.when(step == 1)
    def _():
        leave[2] = down(sums[0])
        diagonal_across.start()
        diagonal_up.start()

    @pl.when(step == 3)
    def _():
        leave[0, low] = down(sums[1, low])
        across_low.start()

    @pl.when(step == 5)
    def _():
        leave[1, high] = down(sums[2, high])
        up_high.start()

    @pl.when(step == 7)
    def _():
        diagonal_up.wait_recv()
        leave[0, high] = down(sums[1, high] + up_cast(come[2, high]))
        across_high.start()
        diagonal_across.wait_recv()
        leave[1, low] = down(sums[2, low] + up_cast(come[2, low]))
        up_low.start()
        for one in (across_low, up_high, across_high, up_low):
            one.wait_recv()
        out[...] = sums[3] + up_cast(come[0]) + up_cast(come[1])
        for number in range(4):
            to_partner(number).wait_send()
        for one in (diagonal_across, diagonal_up, across_low, up_high, across_high, up_low):
            one.wait_send()

def product_reduce_kernel(slope_ref, weight_ref, out_ref, slopes, load, *refs):
    ids = plane_ids()
    step = pl.program_id(0)

    def fetch(number):
        return pltpu.make_async_copy(slope_ref.at[ids[3](number)], slopes.at[number], load.at[number])

    @pl.when(step == 0)
    def _():
        for early in range(8):
            fetch(reduce_order(early)).start()
        greet(ids[:3])
    k = reduce_order(step)
    fetch(k).wait()
    reduce_step(step, product_transposed(slopes[k], weight_ref[...]), refs, ids, out_ref)

def remote_params(collective_id, limit):
    return pltpu.CompilerParams(collective_id=collective_id, has_side_effects=True, vmem_limit_bytes=limit * MIB)

def product_reduce(slopes, weight, collective_id):
    count, rows, inner = slopes.shape
    width = weight.shape[0]
    if not small_plane():
        part = product_transposed(slopes.reshape(-1, inner), weight)
        return lax.psum_scatter(part.astype(jnp.bfloat16), PLANE, scatter_dimension=0, tiled=True).astype(jnp.float32)
    return pl.pallas_call(product_reduce_kernel, grid=(8,), out_shape=jax.ShapeDtypeStruct((rows, width), jnp.float32), in_specs=[ANY, VMEM], out_specs=VMEM, scratch_shapes=[pltpu.VMEM((8, rows, inner), slopes.dtype), DMA((8,)), *reduce_scratch(rows, width)], compiler_params=remote_params(collective_id, 60), name='product_reduce')(slopes, weight)

def total_kernel(x_ref, out_ref, *refs):
    axes = ('grp', 'rep', 'sub')
    here = {n: lax.axis_index(n) for n in axes}
    phases = ('grp', 'sub', 'rep')

    def other(name, step):
        size = lax.axis_size(name)
        return tuple((lax.rem(here[n] + step, size) if n == name else here[n] for n in axes))
    greet([other(n, s) for n in phases for s in range(1, lax.axis_size(n))])
    out_ref[...] = x_ref[...]
    for j, name in enumerate(phases):
        slots, send, recv = refs[3 * j:3 * j + 3]
        size = lax.axis_size(name)
        me = here[name]
        slots[me] = out_ref[...]
        copies = []
        for s in range(1, size):
            one = pltpu.make_async_remote_copy(src_ref=out_ref, dst_ref=slots.at[me], send_sem=send.at[s], recv_sem=recv.at[s], device_id=other(name, s), device_id_type=MESH)
            one.start()
            copies.append(one)
        for one in copies:
            one.wait_recv()
        for one in copies:
            one.wait_send()
        value = slots[0]
        for s in range(1, size):
            value = value + slots[s]
        out_ref[...] = value

def total_everywhere(x, collective_id):
    scratch = []
    for name in ('grp', 'sub', 'rep'):
        n = lax.axis_size(name)
        scratch += [pltpu.VMEM((n,) + x.shape, x.dtype), DMA((n,)), DMA((n,))]
    return pl.pallas_call(total_kernel, out_shape=jax.ShapeDtypeStruct(x.shape, x.dtype), in_specs=[VMEM], out_specs=VMEM, scratch_shapes=scratch, compiler_params=pltpu.CompilerParams(collective_id=collective_id, has_side_effects=True), name='total_everywhere')(x)

def exchange_kernel(to_tokens, x_ref, out_ref, send, recv, local):
    groups, reps, subs = (lax.axis_size(n) for n in EVERY)
    g, r, u = (lax.axis_index(n) for n in EVERY)
    count = groups * subs
    place = g * subs + u
    if to_tokens:
        tokens, width = (out_ref.shape[0], x_ref.shape[1])
    else:
        tokens, width = (x_ref.shape[0], out_ref.shape[1])

    def rows(ref, t):
        return ref.at[pl.ds(pl.multiple_of(t * tokens, tokens), tokens), :]

    def columns(ref, t):
        return ref.at[:, pl.ds(pl.multiple_of(t * width, width), width)]
    source, target = (rows, columns) if to_tokens else (columns, rows)
    peers = [lax.rem(place + step, count) for step in range(1, count)]

    def device(t):
        return (t // subs, r, lax.rem(t, subs))
    own = pltpu.make_async_copy(source(x_ref, place), target(out_ref, place), local)
    own.start()
    greet([device(t) for t in peers])
    copies = []
    for step, t in enumerate(peers):
        one = pltpu.make_async_remote_copy(src_ref=source(x_ref, t), dst_ref=target(out_ref, place), send_sem=send.at[step], recv_sem=recv.at[step], device_id=device(t), device_id_type=MESH)
        one.start()
        copies.append(one)
    own.wait()
    for one in copies:
        one.wait_recv()
    for one in copies:
        one.wait_send()

def exchange(x, to_tokens, collective_id):
    count = lax.axis_size('grp') * lax.axis_size('sub')
    shape = (x.shape[0] // count, x.shape[1] * count) if to_tokens else (x.shape[0] * count, x.shape[1] // count)
    return pl.pallas_call(functools.partial(exchange_kernel, to_tokens), out_shape=jax.ShapeDtypeStruct(shape, x.dtype), in_specs=[ANY], out_specs=ANY, scratch_shapes=[DMA((count - 1,)), DMA((count - 1,)), DMA], compiler_params=pltpu.CompilerParams(collective_id=collective_id, has_side_effects=True), name='to_tokens' if to_tokens else 'to_heads')(x)

def plane_of(group):
    groups = lax.axis_size('grp')
    return lax.rem(group, 2) * (groups // 2) + group // 2

def group_of(plane):
    groups = lax.axis_size('grp')
    return lax.rem(plane, groups // 2) * 2 + plane // (groups // 2)

def opening_kernel(x_ref, *refs):
    count = lax.axis_size('grp') * lax.axis_size('sub')
    weights = (len(refs) - 6) // 2
    sources, (moved_ref, *landings) = (refs[:weights], refs[weights:2 * weights + 1])
    move_send, move_recv, send, recv, local = refs[2 * weights + 1:]
    subs = lax.axis_size('sub')
    g, r, u = (lax.axis_index(n) for n in EVERY)
    place = g * subs + u
    peers = [lax.rem(place + step, count) for step in range(1, count)]

    def device(t):
        return (t // subs, r, lax.rem(t, subs))
    target, source = ((r, plane_of(g), u), (group_of(r), g, u))
    stays = (r == g) & (plane_of(g) == r)

    def block(number, t):
        width = landings[number].shape[1]
        return sources[number].at[:, pl.ds(pl.multiple_of(t * width, width), width)]

    def landing(number):
        rows = sources[number].shape[0]
        return landings[number].at[pl.ds(pl.multiple_of(place * rows, rows), rows), :]
    owns = [pltpu.make_async_copy(block(number, place), landing(number), local.at[number]) for number in range(weights)]
    for one in owns:
        one.start()
    kept = pltpu.make_async_copy(x_ref, moved_ref, local.at[weights])
    moved = pltpu.make_async_remote_copy(src_ref=x_ref, dst_ref=moved_ref, send_sem=move_send, recv_sem=move_recv, device_id=target, device_id_type=MESH)
    barrier = pltpu.get_barrier_semaphore()
    for t in peers:
        pl.semaphore_signal(barrier, inc=1, device_id=device(t), device_id_type=MESH)

    @pl.when(stays)
    def _():
        kept.start()

    @pl.when(jnp.logical_not(stays))
    def _():
        pl.semaphore_signal(barrier, inc=1, device_id=source, device_id_type=MESH)
    pl.semaphore_wait(barrier, count - stays.astype(jnp.int32))

    @pl.when(jnp.logical_not(stays))
    def _():
        moved.start()
    copies = []
    for number in range(weights):
        for step, t in enumerate(peers):
            one = pltpu.make_async_remote_copy(src_ref=block(number, t), dst_ref=landing(number), send_sem=send.at[number, step], recv_sem=recv.at[number, step], device_id=device(t), device_id_type=MESH)
            one.start()
            copies.append(one)
    for one in owns:
        one.wait()
    for one in copies:
        one.wait_recv()
    for one in copies:
        one.wait_send()

    @pl.when(stays)
    def _():
        kept.wait()

    @pl.when(jnp.logical_not(stays))
    def _():
        moved.wait_recv()
        moved.wait_send()

def opening(x, weights, collective_id):
    count = lax.axis_size('grp') * lax.axis_size('sub')
    number = len(weights)
    columns = [jax.ShapeDtypeStruct((w.shape[0] * count, w.shape[1] // count), w.dtype) for w in weights]
    return pl.pallas_call(opening_kernel, out_shape=[jax.ShapeDtypeStruct(x.shape, x.dtype), *columns], in_specs=[VMEM] + [ANY] * number, out_specs=[VMEM] + [ANY] * number, scratch_shapes=[DMA, DMA, DMA((number, count - 1)), DMA((number, count - 1)), DMA((number + 1,))], compiler_params=pltpu.CompilerParams(collective_id=collective_id, has_side_effects=True), name='opening')(x, *weights)

def attend_kernel(heads, head_ref, place_ref, first_ref, last_ref, mixing_ref, attended_ref, total_ref, out_ref, *refs):
    ids = plane_ids()
    step = pl.program_id(0)

    @pl.when(step == 0)
    def _():
        greet(ids[:3])
    rows = out_ref.shape[0]
    size = attended_ref.shape[1] // heads
    factor = size ** (-0.5) * log2_e
    first_row = pl.multiple_of(ids[3](reduce_order(step)) * rows, rows)
    here = pl.ds(first_row, rows)
    place = place_ref[here, :]
    allowed = (first_ref[...] <= place) & (place <= last_ref[...])
    for h in range(heads):
        q, k, v = (3 * h + j for j in range(3))
        scores = product_transposed(head_ref[here, q * size:(q + 1) * size], head_ref[:, k * size:(k + 1) * size])
        scores = jnp.where(allowed, scores * factor, masked_score)
        top = jnp.max(scores, axis=1, keepdims=True)
        soft = jnp.exp2(scores - top)
        total = jnp.sum(soft, axis=1, keepdims=True)
        mixture = product(soft.astype(jnp.bfloat16), head_ref[:, v * size:(v + 1) * size])
        attended_ref[here, h * size:(h + 1) * size] = (mixture / total).astype(jnp.bfloat16)
        log_total = jnp.broadcast_to(top + jnp.log2(total), (rows, 128))
        total_ref[h, :, here] = log_total.T[:8]
    reduce_step(step, product(attended_ref[here, :], mixing_ref[...]), refs, ids, out_ref)

def attend(packed, places, key_last, mixing, heads, token_rows, collective_id):
    rows = packed.shape[0]
    inner, width = mixing.shape
    if not small_plane():
        attended, totals = attention_forward(packed, places, key_last, heads)
        part = product(attended, mixing).astype(jnp.bfloat16)
        return (attended, totals, lax.psum_scatter(part, PLANE, scatter_dimension=0, tiled=True).astype(jnp.float32))
    return pl.pallas_call(functools.partial(attend_kernel, heads), grid=(8,), out_shape=[jax.ShapeDtypeStruct((rows, inner), jnp.bfloat16), jax.ShapeDtypeStruct((heads, 8, rows), jnp.float32), jax.ShapeDtypeStruct((token_rows, width), jnp.float32)], in_specs=[VMEM] * 5, out_specs=[VMEM] * 3, scratch_shapes=reduce_scratch(token_rows, width), compiler_params=remote_params(collective_id, 60), name='attend')(packed, places[:, None], places[None, :], key_last[None, :], mixing)

def gather_order(step):
    return step + 2 * (step % 2) - 1 + (8 - step) // 8 - step // 7

def gather_step(step, slots, send, recv, ids):
    across, up, partner, _ = ids
    half = slots.shape[1] // 2
    low, high = (pl.ds(0, half), pl.ds(half, half))

    def copy(number, source, target, device):
        return remote(slots.at[source], slots.at[target], send, recv, number, device)
    across_low = copy(0, (0, low), (1, low), across)
    up_high = copy(1, (0, high), (4, high), up)
    across_high = copy(2, (0, high), (1, high), across)
    up_low = copy(3, (0, low), (4, low), up)
    own = copy(4, 0, 2, partner)
    far_low = copy(5, (1, low), (5, low), up)
    far_high = copy(6, (4, high), (5, high), across)
    pass_across = copy(7, 1, 3, partner)
    pass_up = copy(8, 4, 6, partner)
    pass_low = copy(9, (5, low), (7, low), partner)
    pass_high = copy(10, (5, high), (7, high), partner)

    @pl.when(step == 0)
    def _():
        for one in (across_low, up_high, own, across_high, up_low):
            one.start()

    @pl.when(step == 1)
    def _():
        own.wait_recv()

    @pl.when(step == 2)
    def _():
        across_low.wait_recv()
        far_low.start()
        up_high.wait_recv()
        far_high.start()
        across_high.wait_recv()
        pass_across.start()

    @pl.when(step == 3)
    def _():
        up_low.wait_recv()
        pass_up.start()

    @pl.when(step == 4)
    def _():
        pass_across.wait_recv()

    @pl.when(step == 5)
    def _():
        pass_up.wait_recv()

    @pl.when(step == 6)
    def _():
        far_low.wait_recv()
        pass_low.start()
        far_high.wait_recv()
        pass_high.start()

    @pl.when(step == 7)
    def _():
        pass_low.wait_recv()
        pass_high.wait_recv()
        for one in (across_low, up_high, across_high, up_low, own, far_low, far_high, pass_across, pass_up, pass_low, pass_high):
            one.wait_send()

def attend_back_kernel(heads, branch_ref, head_ref, mixing_ref, total_ref, place_ref, first_ref, last_ref, every_ref, out_ref, turned, key_sum, value_sum, slots, load, send, recv, store):
    ids = plane_ids()
    step = pl.program_id(0)
    rows = slots.shape[1]
    size = head_ref.shape[1] // (3 * heads)
    scale = size ** (-0.5)
    factor = scale * log2_e

    @pl.when(step == 0)
    def _():
        first = pltpu.make_async_copy(branch_ref, slots.at[0], load)
        first.start()
        for h in range(heads):
            turned[h] = head_ref[:, (3 * h + 1) * size:(3 * h + 2) * size].T
        key_sum[...] = jnp.zeros_like(key_sum)
        value_sum[...] = jnp.zeros_like(value_sum)
        greet(ids[:3])
        first.wait()
    gather_step(step, slots, send, recv, ids)
    k = gather_order(step)
    place_of = ids[3](k)

    def keep(number):
        return pltpu.make_async_copy(slots.at[number], every_ref.at[ids[3](number)], store.at[number])
    keep(k).start()
    here = pl.ds(pl.multiple_of(place_of * rows, rows), rows)
    slopes = product_transposed(slots[k], mixing_ref[...]).astype(jnp.bfloat16)
    place = place_ref[:, here]
    allowed = (first_ref[...] <= place) & (place <= last_ref[...])
    for h in range(heads):
        queries = head_ref[here, 3 * h * size:(3 * h + 1) * size]
        keys = head_ref[:, (3 * h + 1) * size:(3 * h + 2) * size]
        values = head_ref[:, (3 * h + 2) * size:(3 * h + 3) * size]
        slope = slopes[:, h * size:(h + 1) * size]
        scores = product_transposed(keys, queries)
        soft = jnp.where(allowed, jnp.exp2(scores * factor - total_ref[h, :1, here]), 0.0)
        weight_slope = product_transposed(values, slope)
        centre = jnp.sum(soft * weight_slope, axis=0, keepdims=True)
        score_slope = (soft * (weight_slope - centre)).astype(jnp.bfloat16)
        value_sum[h] += product(soft.astype(jnp.bfloat16), slope)
        key_sum[h] += product(score_slope, queries)
        query_slope = product(turned[h], score_slope)
        out_ref[here, 3 * h * size:(3 * h + 1) * size] = (query_slope.T * scale).astype(jnp.bfloat16)

    @pl.when(step == 7)
    def _():
        for h in range(heads):
            out_ref[:, (3 * h + 1) * size:(3 * h + 2) * size] = (key_sum[h] * scale).astype(jnp.bfloat16)
            out_ref[:, (3 * h + 2) * size:(3 * h + 3) * size] = value_sum[h].astype(jnp.bfloat16)
        for number in range(8):
            keep(number).wait()

def attend_back(branch_slope, packed, mixing, totals, places, key_last, heads, collective_id):
    rows, columns = packed.shape
    token_rows, width = branch_slope.shape
    size = columns // (3 * heads)
    if not small_plane():
        every = lax.all_gather(branch_slope, PLANE, axis=0, tiled=True)
        slopes = product_transposed(every, mixing).astype(jnp.bfloat16)
        return (every, attention_backward(packed, totals, slopes, places, key_last, heads))
    every, slopes = pl.pallas_call(functools.partial(attend_back_kernel, heads), grid=(8,), out_shape=[jax.ShapeDtypeStruct((8, token_rows, width), jnp.bfloat16), jax.ShapeDtypeStruct((rows, columns), jnp.bfloat16)], in_specs=[ANY] + [VMEM] * 6, out_specs=[ANY, VMEM], scratch_shapes=[pltpu.VMEM((heads, size, rows), jnp.bfloat16), pltpu.VMEM((heads, rows, size), jnp.float32), pltpu.VMEM((heads, rows, size), jnp.float32), pltpu.VMEM((8, token_rows, width), jnp.bfloat16), DMA, DMA((11,)), DMA((11,)), DMA((8,))], compiler_params=remote_params(collective_id, 62), name='attend_back')(branch_slope, packed, mixing, totals, places[None, :], places[:, None], key_last[:, None])
    return (every.reshape(rows, width), slopes)

def sub_rows(own):
    rows, width = own.shape
    reps, subs = (lax.axis_size('rep'), lax.axis_size('sub'))
    shares = own.reshape(subs, reps // subs, -1, width)
    if subs != 2:
        every = lax.all_to_all(shares, 'sub', split_axis=0, concat_axis=0, tiled=True)
        return every.transpose(1, 0, 2, 3).reshape(rows, width)
    me = lax.axis_index('sub')
    kept = jnp.where(me == 0, shares[0], shares[1])
    come = lax.ppermute(jnp.where(me == 0, shares[1], shares[0]), 'sub', [(0, 1), (1, 0)])
    first, second = (jnp.where(me == 0, kept, come), jnp.where(me == 0, come, kept))
    return jnp.stack([first, second], axis=1).reshape(rows, width)

def sub_owned(part, reps):
    rows, width = part.shape
    subs = lax.axis_size('sub')
    shares = part.reshape(reps // subs, subs, -1, width).transpose(1, 0, 2, 3)
    if subs != 2:
        every = lax.all_to_all(shares, 'sub', split_axis=0, concat_axis=0, tiled=True)
        return every.reshape(rows, width)
    me = lax.axis_index('sub')
    kept = jnp.where(me == 0, shares[0], shares[1])
    come = lax.ppermute(jnp.where(me == 0, shares[1], shares[0]), 'sub', [(0, 1), (1, 0)])
    first, second = (jnp.where(me == 0, kept, come), jnp.where(me == 0, come, kept))
    return jnp.concatenate([first, second], axis=0).reshape(rows, width)

def rep_rows(own):
    groups, reps, subs = (lax.axis_size(name) for name in EVERY)
    every = lax.all_gather(own, 'rep', axis=0, tiled=True)
    every = every.reshape(reps, groups, subs, -1, own.shape[1]).transpose(1, 0, 2, 3, 4)
    return every.reshape(-1, own.shape[1])

def rep_sums(gradient):
    groups, reps, subs = (lax.axis_size(name) for name in EVERY)
    columns = gradient.shape[1]
    ordered = gradient.astype(jnp.bfloat16).reshape(groups, reps, subs, -1, columns)
    ordered = ordered.transpose(1, 0, 2, 3, 4).reshape(-1, columns)
    return lax.psum_scatter(ordered, 'rep', scatter_dimension=0, tiled=True)

def owner_rows(summed, plane_count):
    columns = summed.shape[1]
    own = lax.all_to_all(summed.reshape(plane_count, -1, columns), PLANE, split_axis=0, concat_axis=0, tiled=True)
    return own.transpose(1, 0, 2).reshape(-1, plane_count * columns).astype(jnp.float32)

def shards(layer_input, entry_gain, entry_shift, joint_weight, query_offset, value_offset, mixing_weight, attention_offset, middle_gain, middle_shift, expand_weight, expand_offset, shrink_weight, shrink_offset, placement, slot_lengths, cotangent):
    token_rows, width = layer_input.shape
    hidden_width = expand_weight.shape[1]
    groups, reps, subs = (lax.axis_size(name) for name in EVERY)
    plane_count = groups * subs
    plane_index = lax.axis_index(PLANE)
    head_size = width // HEADS
    local_heads = HEADS // plane_count
    head_columns = local_heads * head_size
    plane_rows = plane_count * token_rows
    home = [g * reps * subs + r * subs + u for g in range(groups) for r in range(reps) for u in range(subs)]
    away = [(r * reps + g % 2 * (groups // 2) + g // 2) * subs + u for g in range(groups) for r in range(reps) for u in range(subs)]

    def to_plane(array):
        return lax.ppermute(array, EVERY, list(zip(home, away)))

    def from_plane(array):
        return lax.ppermute(array, EVERY, list(zip(away, home)))
    facts = to_plane(jnp.concatenate([placement, slot_lengths], axis=1))[0]
    mixing_own = lax.all_gather(mixing_weight, 'rep', axis=0, tiled=True)
    moved_input, joint_own, expand_own, shrink_own = opening(layer_input, (joint_weight, expand_weight, shrink_weight), 12)
    joint_own, mixing_own = lax.optimization_barrier((joint_own, mixing_own))
    input_float = moved_input.astype(jnp.float32)
    joint_slice = rep_rows(joint_own)
    entry_normal, entry_inverse = norm_terms(input_float)
    entry_normed = (entry_normal * entry_gain + entry_shift).astype(jnp.bfloat16)
    entry_all = plane_gather(entry_normed, 1)
    cotangent, facts, entry_all = lax.optimization_barrier((cotangent, facts, entry_all))
    places, lengths = (facts[:placement.shape[1]], facts[placement.shape[1]:])
    prompt = places.shape[0] // 2
    key_last = key_bounds(places, lengths, prompt)
    expand_slice = rep_rows(expand_own)
    shrink_slice = rep_rows(shrink_own)
    cotangent = to_plane(cotangent)
    mixing_slice = sub_rows(mixing_own)
    offsets = jnp.stack([query_offset.reshape(HEADS, head_size), jnp.zeros((HEADS, head_size), jnp.float32), value_offset.reshape(HEADS, head_size)], axis=1).reshape(-1)
    offsets = lax.dynamic_slice_in_dim(offsets, plane_index * 3 * head_columns, 3 * head_columns)
    heads_kept = (product(entry_all, joint_slice) + offsets).astype(jnp.bfloat16)
    attended, log_totals, branch = attend(heads_kept, places, key_last, mixing_slice, local_heads, token_rows, 3)
    residual = input_float + (branch + attention_offset)
    middle_normal, middle_inverse = norm_terms(residual)
    middle_normed = (middle_normal * middle_gain + middle_shift).astype(jnp.bfloat16)
    middle_all = plane_gather(middle_normed, 5)
    cotangent, middle_all = lax.optimization_barrier((cotangent, middle_all))
    cotangent_all = plane_gather(cotangent, 4)
    hidden_local = hidden_width // plane_count
    offset_local = lax.dynamic_slice_in_dim(expand_offset, plane_index * hidden_local, hidden_local)
    expanded = product(middle_all, expand_slice) + offset_local
    activated_float, gelu_back = jax.vjp(exact_gelu, expanded)
    activated = activated_float.astype(jnp.bfloat16)
    shrink_part = row_outer(cotangent_all, activated).astype(jnp.bfloat16)
    shrink_part, cotangent_all = lax.optimization_barrier((shrink_part, cotangent_all))
    shrink_sums = rep_sums(shrink_part)
    activated_slope = product(cotangent_all, shrink_slice)
    expanded_slope = gelu_back(activated_slope)[0].astype(jnp.bfloat16)
    normed_slope = product_reduce(expanded_slope.reshape(plane_count, token_rows, hidden_local), expand_slice, 6)
    normed_slope, middle_all = lax.optimization_barrier((normed_slope, middle_all))
    expand_part = row_outer(middle_all, expanded_slope).astype(jnp.bfloat16)
    expand_part, normed_slope = lax.optimization_barrier((expand_part, normed_slope))
    expand_sums = rep_sums(expand_part)
    cotangent_float = cotangent.astype(jnp.float32)
    residual_slope = cotangent_float + norm_back(normed_slope, middle_gain, middle_normal, middle_inverse)
    branch_slope = residual_slope.astype(jnp.bfloat16)
    branch_all, joint_slope = attend_back(branch_slope, heads_kept, mixing_slice, log_totals, places, key_last, local_heads, 7)
    shrink_gradient = owner_rows(shrink_sums, plane_count)
    shrink_gradient, joint_slope = lax.optimization_barrier((shrink_gradient, joint_slope))
    joint_part = row_outer(entry_all, joint_slope).astype(jnp.bfloat16)
    joint_part, joint_slope, expand_sums, attended = lax.optimization_barrier((joint_part, joint_slope, expand_sums, attended))
    joint_sums = rep_sums(joint_part)
    entry_slope = product_reduce(joint_slope.reshape(plane_count, token_rows, 3 * head_columns), joint_slice, 9)
    own_gradient = (residual_slope + norm_back(entry_slope, entry_gain, entry_normal, entry_inverse)).astype(jnp.bfloat16)
    own_gradient, attended, expand_sums = lax.optimization_barrier((own_gradient, attended, expand_sums))
    input_gradient = from_plane(own_gradient)
    expand_gradient = owner_rows(expand_sums, plane_count)
    mixing_part = sub_owned(row_outer(attended, branch_all).astype(jnp.bfloat16), reps)
    mixing_part, activated, joint_sums = lax.optimization_barrier((mixing_part, activated, joint_sums))
    mixing_sums = lax.psum_scatter(mixing_part, 'rep', scatter_dimension=0, tiled=True)
    shrunk = product_reduce(activated.reshape(plane_count, token_rows, hidden_local), shrink_slice, 8)
    shrunk, mixing_sums, input_gradient, expand_gradient = lax.optimization_barrier((shrunk, mixing_sums, input_gradient, expand_gradient))
    own_output = (residual + shrunk + shrink_offset).astype(jnp.bfloat16)
    layer_output = from_plane(own_output)
    mixing_gradient = mixing_sums.astype(jnp.float32)
    slope_sums = jnp.sum(joint_slope.astype(jnp.float32), axis=0).reshape(local_heads, 3, head_size)

    def placed(piece, whole_size):
        return lax.dynamic_update_slice_in_dim(jnp.zeros((whole_size,), jnp.float32), piece, plane_index * piece.shape[0], 0)
    small = [jnp.sum(entry_slope * entry_normal, axis=0), jnp.sum(entry_slope, axis=0), placed(slope_sums[:, 0].reshape(-1), width), placed(slope_sums[:, 2].reshape(-1), width), jnp.sum(branch_slope.astype(jnp.float32), axis=0), jnp.sum(normed_slope * middle_normal, axis=0), jnp.sum(normed_slope, axis=0), placed(jnp.sum(expanded_slope.astype(jnp.float32), axis=0), hidden_width), jnp.sum(cotangent_float, axis=0)]
    small_own = jnp.concatenate(small).reshape(-1, 128)
    small_own, own_output = lax.optimization_barrier((small_own, own_output))
    small_all = total_everywhere(small_own, 10).reshape(-1)
    small_sums, first = ([], 0)
    for piece in small:
        small_sums.append(small_all[first:first + piece.shape[0]])
        first += piece.shape[0]
    joint_gradient = owner_rows(joint_sums, plane_count)
    return (layer_output, input_gradient, small_sums[0], small_sums[1], joint_gradient, small_sums[2], small_sums[3], mixing_gradient, small_sums[4], small_sums[5], small_sums[6], expand_gradient, small_sums[7], shrink_gradient, small_sums[8])

def solution(mesh):
    groups, sequence = (mesh.shape['grp'], mesh.shape['seq'])
    subs = sequence // groups
    planes = Mesh(mesh.devices.reshape(groups, sequence // subs, subs), EVERY)
    rows, whole, group_rows = (P(EVERY, None), P(), P('grp', None))
    return jax.shard_map(shards, mesh=planes, in_specs=(rows, whole, whole, rows, whole, whole, rows, whole, whole, whole, rows, whole, rows) + (whole, group_rows, group_rows, rows), out_specs=(rows, rows, whole, whole, rows, whole, whole, rows, whole, whole, whole, rows, whole) + (rows, whole), check_vma=False)
```

```python
import functools
import jax
import jax.numpy as jnp
from jax import lax
from jax.experimental import pallas as pl
from jax.experimental.pallas import tpu as pltpu
from jax.sharding import Mesh, PartitionSpec as P
HEADS = 16
CONT = 256
PLANE = ('grp', 'sub')
EVERY = ('grp', 'rep', 'sub')
MESH = pl.DeviceIdType.MESH
ANY = pl.BlockSpec(memory_space=pl.ANY)
VMEM = pl.BlockSpec(memory_space=pltpu.VMEM)
DMA = pltpu.SemaphoreType.DMA
MIB = 1 << 20
norm_epsilon = 1e-05
masked_score = -1e+30
log2_e = 1.4426950408889634
root_half = 0.7071067811865476
normal_peak = 0.3989422804014327

def norm_terms(values):
    average = jnp.mean(values, axis=-1, keepdims=True)
    centered = values - average
    variance = jnp.mean(centered * centered, axis=-1, keepdims=True)
    inverse = lax.rsqrt(variance + norm_epsilon)
    return (centered * inverse, inverse)

def norm_back(slope, gain, normal, inverse):
    scaled = slope * gain
    return inverse * (scaled - jnp.mean(scaled, axis=-1, keepdims=True) - normal * jnp.mean(scaled * normal, axis=-1, keepdims=True))

def key_bounds(positions, lengths, prompt):
    segment = (positions - prompt) // CONT
    within = positions - prompt - segment * CONT
    slot_ids = jnp.arange(lengths.shape[0], dtype=jnp.int32)
    slot_limit = jnp.sum(jnp.where(segment[:, None] == slot_ids[None, :], lengths[None, :], 0), axis=1)
    last = prompt + (segment + 1) * CONT - 1
    last = jnp.where(within < slot_limit, last, -1)
    return jnp.where(positions < prompt, positions.shape[0], last)

def product(left_matrix, right_matrix):
    return jnp.dot(left_matrix, right_matrix, preferred_element_type=jnp.float32)

def product_transposed(left_matrix, right_matrix):
    return lax.dot_general(left_matrix, right_matrix, (((1,), (1,)), ((), ())), preferred_element_type=jnp.float32)

def row_outer(left_matrix, right_matrix):
    return lax.dot_general(left_matrix, right_matrix, (((0,), (0,)), ((), ())), preferred_element_type=jnp.float32)

def attention_forward(packed, places, key_last, heads):
    rows, columns = packed.shape
    size = columns // (3 * heads)
    block = 256
    factor = size ** (-0.5) * log2_e

    def kernel(q_ref, k_ref, v_ref, place_ref, first_ref, last_ref, out_ref, total_ref):
        scores = product_transposed(q_ref[...], k_ref[...])
        place = place_ref[...]
        allowed = (first_ref[...] <= place) & (place <= last_ref[...])
        scores = jnp.where(allowed, scores * factor, masked_score)
        top = jnp.max(scores, axis=1, keepdims=True)
        soft = jnp.exp2(scores - top)
        total = jnp.sum(soft, axis=1, keepdims=True)
        mixture = product(soft.astype(jnp.bfloat16), v_ref[...])
        out_ref[...] = (mixture / total).astype(jnp.bfloat16)
        log_total = jnp.broadcast_to(top + jnp.log2(total), (block, 128))
        total_ref[0] = log_total.T[:8]
    return pl.pallas_call(kernel, grid=(heads, rows // block), in_specs=[pl.BlockSpec((block, size), lambda h, i: (i, 3 * h)), pl.BlockSpec((rows, size), lambda h, i: (0, 3 * h + 1)), pl.BlockSpec((rows, size), lambda h, i: (0, 3 * h + 2)), pl.BlockSpec((block, 1), lambda h, i: (i, 0)), pl.BlockSpec((1, rows), lambda h, i: (0, 0)), pl.BlockSpec((1, rows), lambda h, i: (0, 0))], out_specs=[pl.BlockSpec((block, size), lambda h, i: (i, h)), pl.BlockSpec((1, 8, block), lambda h, i: (h, 0, i))], out_shape=[jax.ShapeDtypeStruct((rows, heads * size), jnp.bfloat16), jax.ShapeDtypeStruct((heads, 8, rows), jnp.float32)], compiler_params=pltpu.CompilerParams(vmem_limit_bytes=56 * MIB), cost_estimate=pl.CostEstimate(flops=4 * heads * rows * rows * size, bytes_accessed=4 * rows * heads * size * 2, transcendentals=heads * rows * rows), name='attention_forward')(packed, packed, packed, places[:, None], places[None, :], key_last[None, :])

def attention_backward(packed, totals, slopes, places, key_last, heads):
    rows, columns = packed.shape
    size = columns // (3 * heads)
    block = 256
    scale = size ** (-0.5)
    factor = scale * log2_e

    def kernel(q_ref, k_ref, v_ref, slope_ref, total_ref, place_ref, first_ref, last_ref, out_ref, turned_ref, key_sum, value_sum):
        step = pl.program_id(1)

        @pl.when(step == 0)
        def _():
            turned_ref[...] = k_ref[...].T
            key_sum[...] = jnp.zeros_like(key_sum)
            value_sum[...] = jnp.zeros_like(value_sum)
        queries = q_ref[...]
        slope = slope_ref[...]
        scores = product_transposed(k_ref[...], queries)
        place = place_ref[...]
        allowed = (first_ref[...] <= place) & (place <= last_ref[...])
        soft = jnp.where(allowed, jnp.exp2(scores * factor - total_ref[0, :1]), 0.0)
        weight_slope = product_transposed(v_ref[...], slope)
        centre = jnp.sum(soft * weight_slope, axis=0, keepdims=True)
        score_slope = (soft * (weight_slope - centre)).astype(jnp.bfloat16)
        value_sum[...] += product(soft.astype(jnp.bfloat16), slope)
        key_sum[...] += product(score_slope, queries)
        query_slope = product(turned_ref[...], score_slope)
        here = pl.ds(pl.multiple_of(step * block, block), block)
        out_ref[here, :size] = (query_slope.T * scale).astype(jnp.bfloat16)

        @pl.when(step == pl.num_programs(1) - 1)
        def _():
            out_ref[:, size:2 * size] = (key_sum[...] * scale).astype(jnp.bfloat16)
            out_ref[:, 2 * size:] = value_sum[...].astype(jnp.bfloat16)
    return pl.pallas_call(kernel, grid=(heads, rows // block), in_specs=[pl.BlockSpec((block, size), lambda h, i: (i, 3 * h)), pl.BlockSpec((rows, size), lambda h, i: (0, 3 * h + 1)), pl.BlockSpec((rows, size), lambda h, i: (0, 3 * h + 2)), pl.BlockSpec((block, size), lambda h, i: (i, h)), pl.BlockSpec((1, 8, block), lambda h, i: (h, 0, i)), pl.BlockSpec((1, block), lambda h, i: (0, i)), pl.BlockSpec((rows, 1), lambda h, i: (0, 0)), pl.BlockSpec((rows, 1), lambda h, i: (0, 0))], out_specs=pl.BlockSpec((rows, 3 * size), lambda h, i: (0, h)), out_shape=jax.ShapeDtypeStruct((rows, columns), jnp.bfloat16), scratch_shapes=[pltpu.VMEM((size, rows), jnp.bfloat16), pltpu.VMEM((rows, size), jnp.float32), pltpu.VMEM((rows, size), jnp.float32)], compiler_params=pltpu.CompilerParams(vmem_limit_bytes=56 * MIB), cost_estimate=pl.CostEstimate(flops=10 * heads * rows * rows * size, bytes_accessed=8 * rows * heads * size * 2, transcendentals=heads * rows * rows), name='attention_backward')(packed, packed, packed, slopes, totals, places[None, :], places[:, None], key_last[:, None])

def small_plane():
    return (lax.axis_size('grp'), lax.axis_size('sub')) == (4, 2)

def plane_ids():
    g, r, u = (lax.axis_index(n) for n in ('grp', 'rep', 'sub'))
    y, c = (g // 2, g % 2)
    across, up, partner = ((g, r, 1 - u), ((1 - y) * 2 + c, r, u), (y * 2 + 1 - c, r, u))

    def piece(k):
        above, beside, side = (k // 4, k // 2 % 2, k % 2)
        return ((y + above) % 2 * 2 + (c + beside) % 2) * 2 + (u + side) % 2
    return (across, up, partner, piece)

def greet(devices):
    barrier = pltpu.get_barrier_semaphore()
    for device in devices:
        pl.semaphore_signal(barrier, inc=1, device_id=device, device_id_type=MESH)
    pl.semaphore_wait(barrier, len(devices))

def remote(source, target, send, recv, number, device):
    return pltpu.make_async_remote_copy(src_ref=source, dst_ref=target, send_sem=send.at[number], recv_sem=recv.at[number], device_id=device, device_id_type=MESH)

def plane_peers():
    groups, _, subs = (lax.axis_size(n) for n in EVERY)
    g, r, u = (lax.axis_index(n) for n in EVERY)
    count = groups * subs
    place = g * subs + u
    return (place, [(t // subs, r, lax.rem(t, subs)) for t in (lax.rem(place + step, count) for step in range(1, count))])

def owner_cargo(source, target, send, recv, local):
    count = lax.axis_size('grp') * lax.axis_size('sub')
    subs = lax.axis_size('sub')
    rows, width = (target.shape[0], source.shape[1])
    place, peers = plane_peers()

    def block(t):
        return source.at[pl.ds(pl.multiple_of(t * rows, rows), rows), :]
    landing = target.at[:, pl.ds(pl.multiple_of(place * width, width), width)]
    own = pltpu.make_async_copy(block(place), landing, local)
    away = [remote(block(device[0] * subs + device[2]), landing, send, recv, number, device) for number, device in enumerate(peers)]

    def start():
        own.start()
        for one in away:
            one.start()

    def finish():
        own.wait()
        for one in away:
            one.wait_recv()
        for one in away:
            one.wait_send()
    return (start, finish)

def owner_scratch():
    count = lax.axis_size('grp') * lax.axis_size('sub')
    return [DMA((count - 1,)), DMA((count - 1,)), DMA]

def position_of(turn):
    groups = lax.axis_size('grp')
    return lax.rem(turn, 2) * (groups // 2) + turn // 2

def turn_of(position):
    half = lax.axis_size('grp') // 2
    return lax.rem(position, half) * 2 + position // half

def home_devices():
    g, r, u = (lax.axis_index(n) for n in EVERY)
    groups = lax.axis_size('grp')
    rep = lax.rem(turn_of(g) + groups - r, groups)
    return ((r, rep, u), (position_of(lax.rem(g + r, groups)), g, u), (r == g) & (rep == r))

def column_cargo(source, target, send, recv, local):
    subs = lax.axis_size('sub')
    rows, width = (source.shape[0], target.shape[1])
    place, peers = plane_peers()

    def block(t):
        return source.at[:, pl.ds(pl.multiple_of(t * width, width), width)]
    landing = target.at[pl.ds(pl.multiple_of(place * rows, rows), rows), :]
    own = pltpu.make_async_copy(block(place), landing, local)
    away = [remote(block(device[0] * subs + device[2]), landing, send, recv, number, device) for number, device in enumerate(peers)]

    def start():
        own.start()
        for one in away:
            one.start()

    def finish():
        own.wait()
        for one in away:
            one.wait_recv()
        for one in away:
            one.wait_send()
    return (start, finish)

def column_shape(weight):
    count = lax.axis_size('grp') * lax.axis_size('sub')
    return jax.ShapeDtypeStruct((weight.shape[0] * count, weight.shape[1] // count), weight.dtype)

def row_loads(source, target, sem):
    groups, reps = (lax.axis_size('grp'), lax.axis_size('rep'))
    rows = source.shape[0] // (groups * reps)
    return [pltpu.make_async_copy(source.at[pl.ds((r * groups + g) * rows, rows)], target.at[pl.ds((g * reps + r) * rows, rows)], sem.at[g, r]) for g in range(groups) for r in range(reps)]

def row_loads_scratch(shape, dtype):
    return [pltpu.VMEM(shape, dtype), DMA((lax.axis_size('grp'), lax.axis_size('rep')))]

def home_cargo(source, target, send, recv, local):
    goal, _, stays = home_devices()
    kept = pltpu.make_async_copy(source, target, local)
    moved = pltpu.make_async_remote_copy(src_ref=source, dst_ref=target, send_sem=send, recv_sem=recv, device_id=goal, device_id_type=MESH)

    def start():

        @pl.when(stays)
        def _():
            kept.start()

        @pl.when(jnp.logical_not(stays))
        def _():
            moved.start()

    def finish():

        @pl.when(stays)
        def _():
            kept.wait()

        @pl.when(jnp.logical_not(stays))
        def _():
            moved.wait_recv()
            moved.wait_send()
    return (start, finish)

def greet_all(devices, homes):
    barrier = pltpu.get_barrier_semaphore()
    for device in devices:
        pl.semaphore_signal(barrier, inc=1, device_id=device, device_id_type=MESH)
    if not homes:
        pl.semaphore_wait(barrier, len(devices))
        return
    _, origin, stays = home_devices()

    @pl.when(jnp.logical_not(stays))
    def _():
        pl.semaphore_signal(barrier, inc=1, device_id=origin, device_id_type=MESH)
    pl.semaphore_wait(barrier, len(devices) + 1 - stays.astype(jnp.int32))

def gather_kernel(weights, x_ref, *refs):
    sources, out_ref, landings = (refs[:weights], refs[weights], refs[weights + 1:2 * weights + 1])
    slots, load, send, recv, store, *cargo = refs[2 * weights + 1:]
    ids = plane_ids()
    step = pl.program_id(0)
    cargos = [column_cargo(sources[i], landings[i], *cargo[3 * i:3 * i + 3]) for i in range(weights)]

    @pl.when(step == 0)
    def _():
        first = pltpu.make_async_copy(x_ref, slots.at[0], load)
        first.start()
        greet(plane_peers()[1] if weights else ids[:3])
        first.wait()
    gather_step(step, slots, send, recv, ids)

    def keep(number):
        return pltpu.make_async_copy(slots.at[number], out_ref.at[ids[3](number)], store.at[number])
    keep(gather_order(step)).start()
    if weights:

        @pl.when(step == 2)
        def _():
            for start, _ in cargos:
                start()

    @pl.when(step == 7)
    def _():
        for _, finish in cargos:
            finish()
        for number in range(8):
            keep(number).wait()

def plane_gather(x, weights, collective_id):
    rows, width = x.shape
    if not small_plane():
        return [lax.all_gather(x, PLANE, axis=0, tiled=True)] + [exchange(w, False, collective_id + 20 + i) for i, w in enumerate(weights)]
    number = len(weights)
    every, *columns = pl.pallas_call(functools.partial(gather_kernel, number), grid=(8,), out_shape=[jax.ShapeDtypeStruct((8, rows, width), x.dtype)] + [column_shape(w) for w in weights], in_specs=[ANY] * (1 + number), out_specs=[ANY] * (1 + number), scratch_shapes=[pltpu.VMEM((8, rows, width), x.dtype), DMA, DMA((11,)), DMA((11,)), DMA((8,))] + owner_scratch() * number, compiler_params=remote_params(collective_id, 40), name='plane_gather')(x, *weights)
    return [every.reshape(8 * rows, width)] + columns

def reduce_scratch(rows, width):
    wide, narrow = (jnp.float32, jnp.bfloat16)
    return [pltpu.VMEM((4, rows, width), wide), pltpu.VMEM((4, rows, width), narrow), pltpu.VMEM((4, rows, width), narrow), pltpu.VMEM((3, rows, width), narrow), pltpu.VMEM((3, rows, width), narrow), DMA((10,)), DMA((10,))]

def reduce_order(step):
    return 7 - 2 * step + 7 * (step // 4)

def reduce_step(step, piece, refs, ids, out, before=None):
    sums, give, take, leave, come, send, recv = refs
    across, up, partner, _ = ids
    half = sums.shape[1] // 2
    low, high = (pl.ds(0, half), pl.ds(half, half))
    pair = step // 2

    def to_partner(number):
        return remote(give.at[number], take.at[number], send, recv, number, partner)

    def part(number, which, rows, device):
        return remote(leave.at[which, rows], come.at[which, rows], send, recv, number, device)

    def down(value):
        return value.astype(jnp.bfloat16)

    def up_cast(value):
        return value.astype(jnp.float32)

    @pl.when(lax.rem(step, 2) == 0)
    def _():
        give[pair] = down(piece)
        to_partner(pair).start()

    @pl.when(lax.rem(step, 2) == 1)
    def _():
        sums[pair] = piece
    if before is not None:
        before()

    @pl.when(lax.rem(step, 2) == 1)
    def _():
        to_partner(pair).wait_recv()
        sums[pair] += up_cast(take[pair])
    diagonal_across, diagonal_up = (part(4, 2, low, across), part(5, 2, high, up))
    across_low, up_high = (part(6, 0, low, across), part(7, 1, high, up))
    across_high, up_low = (part(8, 0, high, across), part(9, 1, low, up))

    @pl.when(step == 1)
    def _():
        leave[2] = down(sums[0])
        diagonal_across.start()
        diagonal_up.start()

    @pl.when(step == 3)
    def _():
        leave[0, low] = down(sums[1, low])
        across_low.start()

    @pl.when(step == 5)
    def _():
        leave[1, high] = down(sums[2, high])
        up_high.start()

    @pl.when(step == 7)
    def _():
        diagonal_up.wait_recv()
        leave[0, high] = down(sums[1, high] + up_cast(come[2, high]))
        across_high.start()
        diagonal_across.wait_recv()
        leave[1, low] = down(sums[2, low] + up_cast(come[2, low]))
        up_low.start()
        for one in (across_low, up_high, across_high, up_low):
            one.wait_recv()
        out[...] = sums[3] + up_cast(come[0]) + up_cast(come[1])
        for number in range(4):
            to_partner(number).wait_send()
        for one in (diagonal_across, diagonal_up, across_low, up_high, across_high, up_low):
            one.wait_send()

def product_reduce_kernel(owns, homes, slope_ref, weight_ref, *refs):
    ids = plane_ids()
    step = pl.program_id(0)
    refs = list(refs)
    parcels = [refs.pop(0) for _ in range(owns + homes)]
    out_ref = refs.pop(0)
    landings = [refs.pop(0) for _ in range(owns + homes)]
    slopes, load, weight, weight_load, *refs = refs
    tail = refs[7:]
    rows_in = row_loads(weight_ref, weight, weight_load)
    early, late = ([], [])
    if owns:
        late.append(owner_cargo(parcels[0], landings[0], *tail[:3]))
    if homes:
        early.append(home_cargo(parcels[-1], landings[-1], *tail[-3:]))

    def fetch(number):
        return pltpu.make_async_copy(slope_ref.at[ids[3](number)], slopes.at[number], load.at[number])

    @pl.when(step == 0)
    def _():
        for one in rows_in:
            one.start()
        for number in range(8):
            fetch(reduce_order(number)).start()
        greet_all(plane_peers()[1] if owns else ids[:3], homes)
        for start, _ in early:
            start()
        for one in rows_in:
            one.wait()
    k = reduce_order(step)
    fetch(k).wait()
    reduce_step(step, product_transposed(slopes[k], weight[...]), refs[:7], ids, out_ref)
    if owns:

        @pl.when(step == 5)
        def _():
            for start, _ in late:
                start()
    if owns or homes:

        @pl.when(step == 7)
        def _():
            for _, finish in late + early:
                finish()

def remote_params(collective_id, limit):
    return pltpu.CompilerParams(collective_id=collective_id, has_side_effects=True, vmem_limit_bytes=limit * MIB)

def owner_shape(parcel):
    count = lax.axis_size('grp') * lax.axis_size('sub')
    return jax.ShapeDtypeStruct((parcel.shape[0] // count, parcel.shape[1] * count), parcel.dtype)

def product_reduce(slopes, weight, owned, homed, collective_id):
    count, rows, inner = slopes.shape
    width = weight.shape[0]
    owns, homes = (owned is not None, homed is not None)
    if not small_plane():
        part = product_transposed(slopes.reshape(-1, inner), rep_rows_last(weight))
        whole = [lax.psum_scatter(part.astype(jnp.bfloat16), PLANE, scatter_dimension=0, tiled=True).astype(jnp.float32)]
        return whole + ([exchange(owned, True, collective_id)] if owns else []) + ([from_plane(homed)] if homes else [])
    cargo = ([owned] if owns else []) + ([homed] if homes else [])
    shapes = ([owner_shape(owned)] if owns else []) + ([jax.ShapeDtypeStruct(homed.shape, homed.dtype)] if homes else [])
    return pl.pallas_call(functools.partial(product_reduce_kernel, owns, homes), grid=(8,), out_shape=[jax.ShapeDtypeStruct((rows, width), jnp.float32)] + shapes, in_specs=[ANY, ANY] + [ANY] * len(cargo), out_specs=[VMEM] + [ANY] * len(cargo), scratch_shapes=[pltpu.VMEM((8, rows, inner), slopes.dtype), DMA((8,)), *row_loads_scratch(weight.shape, weight.dtype), *reduce_scratch(rows, width)] + (owner_scratch() if owns else []) + ([DMA, DMA, DMA] if homes else []), compiler_params=remote_params(collective_id, 60), name='product_reduce')(slopes, weight, *cargo)

def closing_kernel(number, x_ref, homed_ref, *refs):
    owned_refs, (out_ref, homed_out), owned_outs = (refs[:number], refs[number:number + 2], refs[number + 2:2 * number + 2])
    refs = refs[2 * number + 2:]
    here = {n: lax.axis_index(n) for n in EVERY}
    phases = ('grp', 'sub', 'rep')
    home_start, home_finish = home_cargo(homed_ref, homed_out, *refs[:3])
    owners = [owner_cargo(owned_refs[i], owned_outs[i], *refs[3 + 3 * i:6 + 3 * i]) for i in range(number)]
    refs = refs[3 + 3 * number:]

    def other(name, step):
        size = lax.axis_size(name)
        return tuple((lax.rem(here[n] + step, size) if n == name else here[n] for n in EVERY))
    greet_all(plane_peers()[1] + [other('rep', s) for s in range(1, lax.axis_size('rep'))], True)
    home_start()
    out_ref[...] = x_ref[...]
    for j, name in enumerate(phases):
        slots, send, recv = refs[3 * j:3 * j + 3]
        size = lax.axis_size(name)
        me = here[name]
        slots[me] = out_ref[...]
        copies = []
        for s in range(1, size):
            one = pltpu.make_async_remote_copy(src_ref=out_ref, dst_ref=slots.at[me], send_sem=send.at[s], recv_sem=recv.at[s], device_id=other(name, s), device_id_type=MESH)
            one.start()
            copies.append(one)
        if name == 'rep':
            for start, _ in owners:
                start()
        for one in copies:
            one.wait_recv()
        for one in copies:
            one.wait_send()
        value = slots[0]
        for s in range(1, size):
            value = value + slots[s]
        out_ref[...] = value
    for _, finish in owners:
        finish()
    home_finish()

def closing(x, homed, owned, collective_id):
    scratch = []
    for name in ('grp', 'sub', 'rep'):
        n = lax.axis_size(name)
        scratch += [pltpu.VMEM((n,) + x.shape, x.dtype), DMA((n,)), DMA((n,))]
    number = len(owned)
    return pl.pallas_call(functools.partial(closing_kernel, number), out_shape=[jax.ShapeDtypeStruct(x.shape, x.dtype), jax.ShapeDtypeStruct(homed.shape, homed.dtype)] + [owner_shape(one) for one in owned], in_specs=[VMEM] + [ANY] * (1 + number), out_specs=[VMEM] + [ANY] * (1 + number), scratch_shapes=[DMA, DMA, DMA] + owner_scratch() * number + scratch, compiler_params=pltpu.CompilerParams(collective_id=collective_id, has_side_effects=True), name='closing')(x, homed, *owned)

def exchange_kernel(to_tokens, x_ref, out_ref, send, recv, local):
    groups, reps, subs = (lax.axis_size(n) for n in EVERY)
    g, r, u = (lax.axis_index(n) for n in EVERY)
    count = groups * subs
    place = g * subs + u
    if to_tokens:
        tokens, width = (out_ref.shape[0], x_ref.shape[1])
    else:
        tokens, width = (x_ref.shape[0], out_ref.shape[1])

    def rows(ref, t):
        return ref.at[pl.ds(pl.multiple_of(t * tokens, tokens), tokens), :]

    def columns(ref, t):
        return ref.at[:, pl.ds(pl.multiple_of(t * width, width), width)]
    source, target = (rows, columns) if to_tokens else (columns, rows)
    peers = [lax.rem(place + step, count) for step in range(1, count)]

    def device(t):
        return (t // subs, r, lax.rem(t, subs))
    own = pltpu.make_async_copy(source(x_ref, place), target(out_ref, place), local)
    own.start()
    greet([device(t) for t in peers])
    copies = []
    for step, t in enumerate(peers):
        one = pltpu.make_async_remote_copy(src_ref=source(x_ref, t), dst_ref=target(out_ref, place), send_sem=send.at[step], recv_sem=recv.at[step], device_id=device(t), device_id_type=MESH)
        one.start()
        copies.append(one)
    own.wait()
    for one in copies:
        one.wait_recv()
    for one in copies:
        one.wait_send()

def exchange(x, to_tokens, collective_id):
    count = lax.axis_size('grp') * lax.axis_size('sub')
    shape = (x.shape[0] // count, x.shape[1] * count) if to_tokens else (x.shape[0] * count, x.shape[1] // count)
    return pl.pallas_call(functools.partial(exchange_kernel, to_tokens), out_shape=jax.ShapeDtypeStruct(shape, x.dtype), in_specs=[ANY], out_specs=ANY, scratch_shapes=[DMA((count - 1,)), DMA((count - 1,)), DMA], compiler_params=pltpu.CompilerParams(collective_id=collective_id, has_side_effects=True), name='to_tokens' if to_tokens else 'to_heads')(x)

def opening_kernel(x_ref, *refs):
    weights = (len(refs) - 8) // 2
    sources, (moved_ref, *landings) = (refs[:weights], refs[weights:2 * weights + 1])
    transit, move_send, move_recv, move_local, send, recv, local = refs[2 * weights + 1:]
    groups, _, subs = (lax.axis_size(n) for n in EVERY)
    g, r, u = (lax.axis_index(n) for n in EVERY)
    place, peers = plane_peers()
    relay = position_of(lax.rem(g + r, groups))
    beyond = lax.rem(turn_of(g) + groups - r, groups)

    def block(number, t):
        width = landings[number].shape[1]
        return sources[number].at[:, pl.ds(pl.multiple_of(t * width, width), width)]

    def landing(number):
        rows = sources[number].shape[0]
        return landings[number].at[pl.ds(pl.multiple_of(place * rows, rows), rows), :]

    def hop(number, source, target, device, stays):
        kept = pltpu.make_async_copy(source, target, move_local.at[number])
        moved = remote(source, target, move_send, move_recv, number, device)

        def start():

            @pl.when(stays)
            def _():
                kept.start()

            @pl.when(jnp.logical_not(stays))
            def _():
                moved.start()

        def arrive():

            @pl.when(stays)
            def _():
                kept.wait()

            @pl.when(jnp.logical_not(stays))
            def _():
                moved.wait_recv()

        def leave():

            @pl.when(jnp.logical_not(stays))
            def _():
                moved.wait_send()
        return (start, arrive, leave)
    first = hop(0, x_ref, transit, (relay, r, u), relay == g)
    second = hop(1, transit, moved_ref, (g, beyond, u), beyond == r)
    owns = [pltpu.make_async_copy(block(number, place), landing(number), local.at[number]) for number in range(weights)]
    for one in owns:
        one.start()
    barrier = pltpu.get_barrier_semaphore()
    for device in peers:
        pl.semaphore_signal(barrier, inc=1, device_id=device, device_id_type=MESH)

    @pl.when(beyond != r)
    def _():
        pl.semaphore_signal(barrier, inc=1, device_id=(g, beyond, u), device_id_type=MESH)
    pl.semaphore_wait(barrier, len(peers) + (beyond != r).astype(jnp.int32))
    first[0]()
    copies = []
    for number in range(weights):
        for step, device in enumerate(peers):
            one = pltpu.make_async_remote_copy(src_ref=block(number, device[0] * subs + device[2]), dst_ref=landing(number), send_sem=send.at[number, step], recv_sem=recv.at[number, step], device_id=device, device_id_type=MESH)
            one.start()
            copies.append(one)
    first[1]()
    second[0]()
    for one in owns:
        one.wait()
    for one in copies:
        one.wait_recv()
    for one in copies:
        one.wait_send()
    first[2]()
    second[1]()
    second[2]()

def opening(x, weights, collective_id):
    count = lax.axis_size('grp') * lax.axis_size('sub')
    number = len(weights)
    columns = [jax.ShapeDtypeStruct((w.shape[0] * count, w.shape[1] // count), w.dtype) for w in weights]
    return pl.pallas_call(opening_kernel, out_shape=[jax.ShapeDtypeStruct(x.shape, x.dtype), *columns], in_specs=[VMEM] + [ANY] * number, out_specs=[VMEM] + [ANY] * number, scratch_shapes=[pltpu.VMEM(x.shape, x.dtype), DMA((2,)), DMA((2,)), DMA((2,)), DMA((number, count - 1)), DMA((number, count - 1)), DMA((number,))], compiler_params=pltpu.CompilerParams(collective_id=collective_id, has_side_effects=True), name='opening')(x, *weights)

def attend_kernel(heads, head_ref, place_ref, first_ref, last_ref, mixing_ref, attended_ref, total_ref, out_ref, *refs):
    ids = plane_ids()
    step = pl.program_id(0)

    @pl.when(step == 0)
    def _():
        greet(ids[:3])
    rows = out_ref.shape[0]
    size = attended_ref.shape[1] // heads
    factor = size ** (-0.5) * log2_e
    first_row = pl.multiple_of(ids[3](reduce_order(step)) * rows, rows)
    here = pl.ds(first_row, rows)
    place = place_ref[here, :]
    allowed = (first_ref[...] <= place) & (place <= last_ref[...])
    for h in range(heads):
        q, k, v = (3 * h + j for j in range(3))
        scores = product_transposed(head_ref[here, q * size:(q + 1) * size], head_ref[:, k * size:(k + 1) * size])
        scores = jnp.where(allowed, scores * factor, masked_score)
        top = jnp.max(scores, axis=1, keepdims=True)
        soft = jnp.exp2(scores - top)
        total = jnp.sum(soft, axis=1, keepdims=True)
        mixture = product(soft.astype(jnp.bfloat16), head_ref[:, v * size:(v + 1) * size])
        attended_ref[here, h * size:(h + 1) * size] = (mixture / total).astype(jnp.bfloat16)
        log_total = jnp.broadcast_to(top + jnp.log2(total), (rows, 128))
        total_ref[h, :, here] = log_total.T[:8]
    reduce_step(step, product(attended_ref[here, :], mixing_ref[...]), refs, ids, out_ref)

def attend(packed, places, key_last, mixing, heads, token_rows, collective_id):
    rows = packed.shape[0]
    inner, width = mixing.shape
    if not small_plane():
        attended, totals = attention_forward(packed, places, key_last, heads)
        part = product(attended, mixing).astype(jnp.bfloat16)
        return (attended, totals, lax.psum_scatter(part, PLANE, scatter_dimension=0, tiled=True).astype(jnp.float32))
    return pl.pallas_call(functools.partial(attend_kernel, heads), grid=(8,), out_shape=[jax.ShapeDtypeStruct((rows, inner), jnp.bfloat16), jax.ShapeDtypeStruct((heads, 8, rows), jnp.float32), jax.ShapeDtypeStruct((token_rows, width), jnp.float32)], in_specs=[VMEM] * 5, out_specs=[VMEM] * 3, scratch_shapes=reduce_scratch(token_rows, width), compiler_params=remote_params(collective_id, 60), name='attend')(packed, places[:, None], places[None, :], key_last[None, :], mixing)

def gather_order(step):
    return step + 2 * (step % 2) - 1 + (8 - step) // 8 - step // 7

def gather_step(step, slots, send, recv, ids):
    across, up, partner, _ = ids
    half = slots.shape[1] // 2
    low, high = (pl.ds(0, half), pl.ds(half, half))

    def copy(number, source, target, device):
        return remote(slots.at[source], slots.at[target], send, recv, number, device)
    across_low = copy(0, (0, low), (1, low), across)
    up_high = copy(1, (0, high), (4, high), up)
    across_high = copy(2, (0, high), (1, high), across)
    up_low = copy(3, (0, low), (4, low), up)
    own = copy(4, 0, 2, partner)
    far_low = copy(5, (1, low), (5, low), up)
    far_high = copy(6, (4, high), (5, high), across)
    pass_across = copy(7, 1, 3, partner)
    pass_up = copy(8, 4, 6, partner)
    pass_low = copy(9, (5, low), (7, low), partner)
    pass_high = copy(10, (5, high), (7, high), partner)

    @pl.when(step == 0)
    def _():
        for one in (across_low, up_high, own, across_high, up_low):
            one.start()

    @pl.when(step == 1)
    def _():
        own.wait_recv()

    @pl.when(step == 2)
    def _():
        across_low.wait_recv()
        far_low.start()
        up_high.wait_recv()
        far_high.start()
        across_high.wait_recv()
        pass_across.start()

    @pl.when(step == 3)
    def _():
        up_low.wait_recv()
        pass_up.start()

    @pl.when(step == 4)
    def _():
        pass_across.wait_recv()

    @pl.when(step == 5)
    def _():
        pass_up.wait_recv()

    @pl.when(step == 6)
    def _():
        far_low.wait_recv()
        pass_low.start()
        far_high.wait_recv()
        pass_high.start()

    @pl.when(step == 7)
    def _():
        pass_low.wait_recv()
        pass_high.wait_recv()
        for one in (across_low, up_high, across_high, up_low, own, far_low, far_high, pass_across, pass_up, pass_low, pass_high):
            one.wait_send()

def attend_back_kernel(heads, branch_ref, owned_ref, head_ref, mixing_ref, attended_ref, total_ref, place_ref, first_ref, last_ref, part_ref, out_ref, owned_out, turned, key_sum, value_sum, part_sum, slots, load, send, recv, *cargo):
    ids = plane_ids()
    step = pl.program_id(0)
    start, finish = owner_cargo(owned_ref, owned_out, *cargo)
    rows = slots.shape[1]
    size = head_ref.shape[1] // (3 * heads)
    scale = size ** (-0.5)
    factor = scale * log2_e

    @pl.when(step == 0)
    def _():
        first = pltpu.make_async_copy(branch_ref, slots.at[0], load)
        first.start()
        for h in range(heads):
            turned[h] = head_ref[:, (3 * h + 1) * size:(3 * h + 2) * size].T
        key_sum[...] = jnp.zeros_like(key_sum)
        value_sum[...] = jnp.zeros_like(value_sum)
        part_sum[...] = jnp.zeros_like(part_sum)
        greet(plane_peers()[1])
        first.wait()
    gather_step(step, slots, send, recv, ids)
    k = gather_order(step)

    @pl.when(step == 4)
    def _():
        start()
    here = pl.ds(pl.multiple_of(ids[3](k) * rows, rows), rows)
    part_sum[...] += row_outer(attended_ref[here, :], slots[k])
    slopes = product_transposed(slots[k], mixing_ref[...]).astype(jnp.bfloat16)
    place = place_ref[:, here]
    allowed = (first_ref[...] <= place) & (place <= last_ref[...])
    for h in range(heads):
        queries = head_ref[here, 3 * h * size:(3 * h + 1) * size]
        keys = head_ref[:, (3 * h + 1) * size:(3 * h + 2) * size]
        values = head_ref[:, (3 * h + 2) * size:(3 * h + 3) * size]
        slope = slopes[:, h * size:(h + 1) * size]
        scores = product_transposed(keys, queries)
        soft = jnp.where(allowed, jnp.exp2(scores * factor - total_ref[h, :1, here]), 0.0)
        weight_slope = product_transposed(values, slope)
        centre = jnp.sum(soft * weight_slope, axis=0, keepdims=True)
        score_slope = (soft * (weight_slope - centre)).astype(jnp.bfloat16)
        value_sum[h] += product(soft.astype(jnp.bfloat16), slope)
        key_sum[h] += product(score_slope, queries)
        query_slope = product(turned[h], score_slope)
        out_ref[here, 3 * h * size:(3 * h + 1) * size] = (query_slope.T * scale).astype(jnp.bfloat16)

    @pl.when(step == 7)
    def _():
        for h in range(heads):
            out_ref[:, (3 * h + 1) * size:(3 * h + 2) * size] = (key_sum[h] * scale).astype(jnp.bfloat16)
            out_ref[:, (3 * h + 2) * size:(3 * h + 3) * size] = value_sum[h].astype(jnp.bfloat16)
        part_ref[...] = part_sum[...].astype(jnp.bfloat16)
        finish()

def attend_back(branch_slope, owned, packed, mixing, attended, totals, places, key_last, heads, collective_id):
    rows, columns = packed.shape
    token_rows, width = branch_slope.shape
    size = columns // (3 * heads)
    if not small_plane():
        every = lax.all_gather(branch_slope, PLANE, axis=0, tiled=True)
        slopes = product_transposed(every, mixing).astype(jnp.bfloat16)
        part = row_outer(attended, every).astype(jnp.bfloat16)
        slopes = attention_backward(packed, totals, slopes, places, key_last, heads)
        return (part, slopes, exchange(owned, True, collective_id))
    return pl.pallas_call(functools.partial(attend_back_kernel, heads), grid=(8,), out_shape=[jax.ShapeDtypeStruct(mixing.shape, jnp.bfloat16), jax.ShapeDtypeStruct((rows, columns), jnp.bfloat16), owner_shape(owned)], in_specs=[ANY] * 2 + [VMEM] * 7, out_specs=[VMEM, VMEM, ANY], scratch_shapes=[pltpu.VMEM((heads, size, rows), jnp.bfloat16), pltpu.VMEM((heads, rows, size), jnp.float32), pltpu.VMEM((heads, rows, size), jnp.float32), pltpu.VMEM(mixing.shape, jnp.float32), pltpu.VMEM((8, token_rows, width), jnp.bfloat16), DMA, DMA((11,)), DMA((11,)), *owner_scratch()], compiler_params=remote_params(collective_id, 62), name='attend_back')(branch_slope, owned, packed, mixing, attended, totals, places[None, :], places[:, None], key_last[:, None])

def add_outer(total, left, right):
    turned = left.T
    for first in range(0, total.shape[1], 256):
        here = pl.ds(first, 256)
        total[:, here] += product(turned, right[:, first:first + 256])

def rep_order(total, narrow, part_ref, sem):
    groups, reps = (lax.axis_size('grp'), lax.axis_size('rep'))
    rows = total.shape[0] // (groups * reps)
    for g in range(groups):
        for r in range(reps):
            come, go = (pl.ds((g * reps + r) * rows, rows), pl.ds((r * groups + g) * rows, rows))
            narrow[come, :] = total[come, :].astype(jnp.bfloat16)
            pltpu.make_async_copy(narrow.at[come], part_ref.at[go], sem.at[g, r]).start()

def rep_order_wait(narrow, part_ref, sem):
    groups, reps = (lax.axis_size('grp'), lax.axis_size('rep'))
    rows = narrow.shape[0] // (groups * reps)
    for g in range(groups):
        for r in range(reps):
            come, go = (pl.ds((g * reps + r) * rows, rows), pl.ds((r * groups + g) * rows, rows))
            pltpu.make_async_copy(narrow.at[come], part_ref.at[go], sem.at[g, r]).wait()

def hidden_kernel(middle_ref, cotangent_ref, expand_ref, offset_ref, every_ref, active_ref, rise_ref, part_ref, slots, cotangents, actives, rises, total, load, send, recv, store, fetch_cotangent, active_store, rise_store, expand, expand_load, narrow, part_store):
    ids = plane_ids()
    step = pl.program_id(0)
    turn = lax.rem(step, 2)

    def fetch(number, side):
        return pltpu.make_async_copy(cotangent_ref.at[ids[3](gather_order(number))], cotangents.at[side], fetch_cotangent.at[side])

    @pl.when(step == 0)
    def _():
        first = pltpu.make_async_copy(middle_ref, slots.at[0], load)
        first.start()
        rows_in = row_loads(expand_ref, expand, expand_load)
        for one in rows_in:
            one.start()
        fetch(0, 0).start()
        total[...] = jnp.zeros_like(total)
        greet(ids[:3])
        first.wait()
        for one in rows_in:
            one.wait()
    gather_step(step, slots, send, recv, ids)
    k = gather_order(step)

    def keep(number):
        return pltpu.make_async_copy(slots.at[number], every_ref.at[ids[3](number)], store.at[number])

    def put(number, side):
        piece = ids[3](number)
        return (pltpu.make_async_copy(actives.at[side], active_ref.at[piece], active_store.at[side]), pltpu.make_async_copy(rises.at[side], rise_ref.at[piece], rise_store.at[side]))
    keep(k).start()

    @pl.when(step >= 2)
    def _():
        for one in put(k, turn):
            one.wait()
    expanded = product(slots[k], expand[...]) + offset_ref[...]
    below = 0.5 * (1.0 + lax.erf(expanded * root_half))
    actives[turn] = (expanded * below).astype(jnp.bfloat16)
    rises[turn] = below + expanded * (jnp.exp(-0.5 * expanded * expanded) * normal_peak)
    for one in put(k, turn):
        one.start()
    fetch(step, turn).wait()

    @pl.when(step < 7)
    def _():
        fetch(step + 1, 1 - turn).start()
    add_outer(total, cotangents[turn], actives[turn])

    @pl.when(step == 7)
    def _():
        rep_order(total, narrow, part_ref, part_store)
        for late in range(2):
            for one in put(k, late):
                one.wait()
        for number in range(8):
            keep(number).wait()
        rep_order_wait(narrow, part_ref, part_store)

def hidden(middle, cotangent_all, expand_slice, offset, collective_id):
    rows, width = middle.shape
    count = lax.axis_size('grp') * lax.axis_size('sub')
    inner = expand_slice.shape[1]
    if not small_plane():
        every = lax.all_gather(middle, PLANE, axis=0, tiled=True)
        expanded = product(every, rep_rows_last(expand_slice)) + offset
        below = 0.5 * (1.0 + lax.erf(expanded * root_half))
        rise = below + expanded * (jnp.exp(-0.5 * expanded * expanded) * normal_peak)
        active = (expanded * below).astype(jnp.bfloat16)
        return (every, active, rise, rep_rows_first(row_outer(cotangent_all, active)))
    every, active, rise, part = pl.pallas_call(hidden_kernel, grid=(8,), out_shape=[jax.ShapeDtypeStruct((8, rows, width), middle.dtype), jax.ShapeDtypeStruct((8, rows, inner), jnp.bfloat16), jax.ShapeDtypeStruct((8, rows, inner), jnp.float32), jax.ShapeDtypeStruct((width, inner), jnp.bfloat16)], in_specs=[ANY, ANY, ANY, VMEM], out_specs=[ANY] * 4, scratch_shapes=[pltpu.VMEM((8, rows, width), middle.dtype), pltpu.VMEM((2, rows, width), jnp.bfloat16), pltpu.VMEM((2, rows, inner), jnp.bfloat16), pltpu.VMEM((2, rows, inner), jnp.float32), pltpu.VMEM((width, inner), jnp.float32), DMA, DMA((11,)), DMA((11,)), DMA((8,)), DMA((2,)), DMA((2,)), DMA((2,)), *row_loads_scratch(expand_slice.shape, expand_slice.dtype), *row_loads_scratch(expand_slice.shape, jnp.bfloat16)], compiler_params=remote_params(collective_id, 60), name='hidden')(middle, cotangent_all.reshape(8, rows, width), expand_slice, offset[None, :])
    return (every.reshape(count * rows, width), active.reshape(count * rows, inner), rise.reshape(count * rows, inner), part)

def hidden_back_kernel(cotangent_ref, middle_ref, rise_ref, shrink_ref, expand_ref, slope_ref, out_ref, part_ref, cotangents, middles, rises, slopes, total, fetches, store, shrink, shrink_load, expand, expand_load, narrow, part_store, *refs):
    ids = plane_ids()
    step = pl.program_id(0)

    def fetch(number, side):
        piece = ids[3](reduce_order(number))
        return [pltpu.make_async_copy(source.at[piece], target.at[side], fetches.at[kind, side]) for kind, (source, target) in enumerate(((cotangent_ref, cotangents), (rise_ref, rises), (middle_ref, middles)))]

    def put(number, side):
        return pltpu.make_async_copy(slopes.at[side], slope_ref.at[ids[3](reduce_order(number))], store.at[side])
    turn = lax.rem(step, 2)

    @pl.when(step == 0)
    def _():
        rows_in = row_loads(shrink_ref, shrink, shrink_load) + row_loads(expand_ref, expand, expand_load)
        for one in rows_in:
            one.start()
        for one in fetch(0, 0):
            one.start()
        total[...] = jnp.zeros_like(total)
        greet(ids[:3])
        for one in rows_in:
            one.wait()
    for one in fetch(step, turn):
        one.wait()

    @pl.when(step < 7)
    def _():
        for one in fetch(step + 1, 1 - turn):
            one.start()

    @pl.when(step >= 2)
    def _():
        put(step, turn).wait()
    slope = product(cotangents[turn], shrink[...]) * rises[turn]
    slopes[turn] = slope.astype(jnp.bfloat16)
    put(step, turn).start()

    def before():
        add_outer(total, middles[turn], slopes[turn])

        @pl.when(step == 7)
        def _():
            rep_order(total, narrow, part_ref, part_store)
    reduce_step(step, product_transposed(slopes[turn], expand[...]), refs, ids, out_ref, before)

    @pl.when(step == 7)
    def _():
        put(6, 0).wait()
        put(7, 1).wait()
        rep_order_wait(narrow, part_ref, part_store)

def hidden_back(cotangent_all, middle_all, rise, shrink_slice, expand_slice, token_rows, collective_id):
    rows, width = cotangent_all.shape
    inner = shrink_slice.shape[1]
    if not small_plane():
        slope = (product(cotangent_all, rep_rows_last(shrink_slice)) * rise).astype(jnp.bfloat16)
        part = product_transposed(slope, rep_rows_last(expand_slice)).astype(jnp.bfloat16)
        normed = lax.psum_scatter(part, PLANE, scatter_dimension=0, tiled=True).astype(jnp.float32)
        return (slope, normed, rep_rows_first(row_outer(middle_all, slope)))
    pieces = (8, token_rows, width)
    slope, normed, part = pl.pallas_call(hidden_back_kernel, grid=(8,), out_shape=[jax.ShapeDtypeStruct((8, token_rows, inner), jnp.bfloat16), jax.ShapeDtypeStruct((token_rows, width), jnp.float32), jax.ShapeDtypeStruct((width, inner), jnp.bfloat16)], in_specs=[ANY] * 5, out_specs=[ANY, VMEM, ANY], scratch_shapes=[pltpu.VMEM((2, token_rows, width), jnp.bfloat16), pltpu.VMEM((2, token_rows, width), jnp.bfloat16), pltpu.VMEM((2, token_rows, inner), jnp.float32), pltpu.VMEM((2, token_rows, inner), jnp.bfloat16), pltpu.VMEM((width, inner), jnp.float32), DMA((3, 2)), DMA((2,)), *row_loads_scratch(shrink_slice.shape, shrink_slice.dtype), *row_loads_scratch(expand_slice.shape, expand_slice.dtype), *row_loads_scratch(expand_slice.shape, jnp.bfloat16), *reduce_scratch(token_rows, width)], compiler_params=remote_params(collective_id, 63), name='hidden_back')(cotangent_all.reshape(pieces), middle_all.reshape(pieces), rise.reshape(8, token_rows, inner), shrink_slice, expand_slice)
    return (slope.reshape(rows, inner), normed, part)

def plane_moves():
    groups, reps, subs = (lax.axis_size(n) for n in EVERY)
    moves = []
    for g in range(groups):
        for r in range(reps):
            turn = (g + r) % groups
            position = turn % 2 * (groups // 2) + turn // 2
            for u in range(subs):
                moves.append(tuple(((a * reps + b) * subs + u for a, b in ((g, r), (position, r), (position, g)))))
    return moves

def to_door(array):
    return lax.ppermute(array, EVERY, [(home, door) for home, door, _ in plane_moves()])

def to_keeper(array):
    return lax.ppermute(array, EVERY, [(door, away) for _, door, away in plane_moves()])

def to_plane_at_once(array):
    return lax.ppermute(array, EVERY, [(home, away) for home, _, away in plane_moves()])

def from_plane(array):
    return lax.ppermute(array, EVERY, [(away, home) for home, _, away in plane_moves()])

def plane_order(places):
    groups = lax.axis_size('grp')
    blocks = jnp.roll(places.reshape(groups, -1), lax.axis_index('rep'), axis=0)
    return blocks.reshape(groups // 2, 2, -1).transpose(1, 0, 2).reshape(-1)

def rep_rows(own):
    return lax.all_gather(own, 'rep', axis=0, tiled=True)

def rep_rows_last(every):
    groups, reps, subs = (lax.axis_size(name) for name in EVERY)
    columns = every.shape[1]
    ordered = every.reshape(reps, groups, subs, -1, columns).transpose(1, 0, 2, 3, 4)
    return ordered.reshape(-1, columns)

def rep_rows_first(gradient):
    groups, reps, subs = (lax.axis_size(name) for name in EVERY)
    columns = gradient.shape[1]
    ordered = gradient.astype(jnp.bfloat16).reshape(groups, reps, subs, -1, columns)
    return ordered.transpose(1, 0, 2, 3, 4).reshape(-1, columns)

def rep_sums(ordered):
    return lax.psum_scatter(ordered, 'rep', scatter_dimension=0, tiled=True)

def sub_turn(block):
    groups, reps, subs = (lax.axis_size(name) for name in EVERY)
    low = reps // subs
    moves = [((g * reps + r) * subs + u, (g * reps + u * low + r % low) * subs + r // low) for g in range(groups) for r in range(reps) for u in range(subs)]
    return lax.ppermute(block, EVERY, moves)

def sub_rows(own):
    rows, width = own.shape
    reps, subs = (lax.axis_size('rep'), lax.axis_size('sub'))
    shares = own.reshape(subs, reps // subs, -1, width)
    if subs != 2:
        every = lax.all_to_all(shares, 'sub', split_axis=0, concat_axis=0, tiled=True)
        return every.transpose(1, 0, 2, 3).reshape(rows, width)
    me = lax.axis_index('sub')
    kept = jnp.where(me == 0, shares[0], shares[1])
    come = lax.ppermute(jnp.where(me == 0, shares[1], shares[0]), 'sub', [(0, 1), (1, 0)])
    first, second = (jnp.where(me == 0, kept, come), jnp.where(me == 0, come, kept))
    return jnp.stack([first, second], axis=1).reshape(rows, width)

def mixing_sums_of(part):
    reps, subs = (lax.axis_size('rep'), lax.axis_size('sub'))
    rows, width = part.shape
    ordered = part.reshape(reps // subs, subs, rows // reps, width).transpose(1, 0, 2, 3)
    return lax.psum_scatter(ordered.reshape(rows, width), 'rep', scatter_dimension=0, tiled=True)

def shards(layer_input, entry_gain, entry_shift, joint_weight, query_offset, value_offset, mixing_weight, attention_offset, middle_gain, middle_shift, expand_weight, expand_offset, shrink_weight, shrink_offset, placement, slot_lengths, cotangent):
    token_rows, width = layer_input.shape
    hidden_width = expand_weight.shape[1]
    groups, reps, subs = (lax.axis_size(name) for name in EVERY)
    plane_count = groups * subs
    plane_index = lax.axis_index(PLANE)
    head_size = width // HEADS
    local_heads = HEADS // plane_count
    head_columns = local_heads * head_size
    plane_rows = plane_count * token_rows
    facts = to_plane_at_once(jnp.concatenate([placement, slot_lengths], axis=1))[0]
    mixing_own = rep_rows(mixing_weight)
    moved_input, joint_own, expand_own, shrink_own = opening(layer_input, (joint_weight, expand_weight, shrink_weight), 12)
    joint_own, mixing_own = lax.optimization_barrier((joint_own, mixing_own))
    input_float = moved_input.astype(jnp.float32)
    joint_every = rep_rows(joint_own)
    entry_normal, entry_inverse = norm_terms(input_float)
    entry_normed = (entry_normal * entry_gain + entry_shift).astype(jnp.bfloat16)
    entry_all, = plane_gather(entry_normed, (), 1)
    cotangent, facts, entry_all = lax.optimization_barrier((cotangent, facts, entry_all))
    cotangent = to_door(cotangent)
    places = plane_order(facts[:placement.shape[1]])
    lengths = facts[placement.shape[1]:]
    prompt = places.shape[0] // 2
    key_last = key_bounds(places, lengths, prompt)
    expand_slice = rep_rows(expand_own)
    shrink_slice = rep_rows(shrink_own)
    cotangent = to_keeper(cotangent)
    mixing_slice = sub_rows(mixing_own)
    offsets = jnp.stack([query_offset.reshape(HEADS, head_size), jnp.zeros((HEADS, head_size), jnp.float32), value_offset.reshape(HEADS, head_size)], axis=1).reshape(-1)
    offsets = lax.dynamic_slice_in_dim(offsets, plane_index * 3 * head_columns, 3 * head_columns)
    heads_kept = (product(entry_all, rep_rows_last(joint_every)) + offsets).astype(jnp.bfloat16)
    attended, log_totals, branch = attend(heads_kept, places, key_last, mixing_slice, local_heads, token_rows, 3)
    residual = input_float + (branch + attention_offset)
    middle_normal, middle_inverse = norm_terms(residual)
    middle_normed = (middle_normal * middle_gain + middle_shift).astype(jnp.bfloat16)
    cotangent, middle_normed = lax.optimization_barrier((cotangent, middle_normed))
    cotangent_all, = plane_gather(cotangent, (), 4)
    middle_normed, cotangent_all = lax.optimization_barrier((middle_normed, cotangent_all))
    hidden_local = hidden_width // plane_count
    offset_local = lax.dynamic_slice_in_dim(expand_offset, plane_index * hidden_local, hidden_local)
    middle_all, activated, rise, shrink_part = hidden(middle_normed, cotangent_all, expand_slice, offset_local, 5)
    shrink_sums = rep_sums(shrink_part)
    expanded_slope, normed_slope, expand_part = hidden_back(cotangent_all, middle_all, rise, shrink_slice, expand_slice, token_rows, 6)
    expand_sums = rep_sums(expand_part)
    cotangent_float = cotangent.astype(jnp.float32)
    residual_slope = cotangent_float + norm_back(normed_slope, middle_gain, middle_normal, middle_inverse)
    branch_slope = residual_slope.astype(jnp.bfloat16)
    mixing_part, joint_slope, shrink_rows = attend_back(branch_slope, shrink_sums, heads_kept, mixing_slice, attended, log_totals, places, key_last, local_heads, 7)
    shrink_gradient = shrink_rows.astype(jnp.float32)
    joint_part = rep_rows_first(row_outer(entry_all, joint_slope))
    joint_part, joint_slope, expand_sums, mixing_part = lax.optimization_barrier((joint_part, joint_slope, expand_sums, mixing_part))
    joint_sums = rep_sums(joint_part)
    activated, joint_slope = lax.optimization_barrier((activated, joint_slope))
    shrunk, = product_reduce(activated.reshape(plane_count, token_rows, hidden_local), shrink_slice, None, None, 8)
    own_output = (residual + shrunk + shrink_offset).astype(jnp.bfloat16)
    own_output, joint_slope = lax.optimization_barrier((own_output, joint_slope))
    joint_sums, mixing_part = lax.optimization_barrier((joint_sums, mixing_part))
    mixing_sums = mixing_sums_of(mixing_part)
    entry_slope, layer_output = product_reduce(joint_slope.reshape(plane_count, token_rows, 3 * head_columns), joint_every, None, own_output, 9)
    own_gradient = (residual_slope + norm_back(entry_slope, entry_gain, entry_normal, entry_inverse)).astype(jnp.bfloat16)
    slope_sums = jnp.sum(joint_slope.astype(jnp.float32), axis=0).reshape(local_heads, 3, head_size)

    def placed(piece, whole_size):
        return lax.dynamic_update_slice_in_dim(jnp.zeros((whole_size,), jnp.float32), piece, plane_index * piece.shape[0], 0)
    small = [jnp.sum(entry_slope * entry_normal, axis=0), jnp.sum(entry_slope, axis=0), placed(slope_sums[:, 0].reshape(-1), width), placed(slope_sums[:, 2].reshape(-1), width), jnp.sum(branch_slope.astype(jnp.float32), axis=0), jnp.sum(normed_slope * middle_normal, axis=0), jnp.sum(normed_slope, axis=0), placed(jnp.sum(expanded_slope.astype(jnp.float32), axis=0), hidden_width), jnp.sum(cotangent_float, axis=0)]
    small_own = jnp.concatenate(small).reshape(-1, 128)
    small_all, input_gradient, joint_rows, expand_rows = closing(small_own, own_gradient, (joint_sums, expand_sums), 10)
    expand_gradient = expand_rows.astype(jnp.float32)
    joint_gradient = joint_rows.astype(jnp.float32)
    mixing_gradient = sub_turn(mixing_sums).astype(jnp.float32)
    small_all = small_all.reshape(-1)
    small_sums, first = ([], 0)
    for piece in small:
        small_sums.append(small_all[first:first + piece.shape[0]])
        first += piece.shape[0]
    return (layer_output, input_gradient, small_sums[0], small_sums[1], joint_gradient, small_sums[2], small_sums[3], mixing_gradient, small_sums[4], small_sums[5], small_sums[6], expand_gradient, small_sums[7], shrink_gradient, small_sums[8])

def solution(mesh):
    groups, sequence = (mesh.shape['grp'], mesh.shape['seq'])
    subs = sequence // groups
    planes = Mesh(mesh.devices.reshape(groups, sequence // subs, subs), EVERY)
    rows, whole, group_rows = (P(EVERY, None), P(), P('grp', None))
    return jax.shard_map(shards, mesh=planes, in_specs=(rows, whole, whole, rows, whole, whole, rows, whole, whole, whole, rows, whole, rows) + (whole, group_rows, group_rows, rows), out_specs=(rows, rows, whole, whole, rows, whole, whole, rows, whole, whole, whole, rows, whole) + (rows, whole), check_vma=False)
```

```python
import functools
import jax
import jax.numpy as jnp
from jax import lax
from jax.experimental import pallas as pl
from jax.experimental.pallas import tpu as pltpu
from jax.sharding import Mesh, PartitionSpec as P
HEADS = 16
CONT = 256
PLANE = ('grp', 'sub')
EVERY = ('grp', 'rep', 'sub')
MESH = pl.DeviceIdType.MESH
ANY = pl.BlockSpec(memory_space=pl.ANY)
VMEM = pl.BlockSpec(memory_space=pltpu.VMEM)
DMA = pltpu.SemaphoreType.DMA
MIB = 1 << 20
norm_epsilon = 1e-05
masked_score = -1e+30
log2_e = 1.4426950408889634
root_half = 0.7071067811865476
normal_peak = 0.3989422804014327

def norm_terms(values):
    average = jnp.mean(values, axis=-1, keepdims=True)
    centered = values - average
    variance = jnp.mean(centered * centered, axis=-1, keepdims=True)
    inverse = lax.rsqrt(variance + norm_epsilon)
    return (centered * inverse, inverse)

def norm_back(slope, gain, normal, inverse):
    scaled = slope * gain
    return inverse * (scaled - jnp.mean(scaled, axis=-1, keepdims=True) - normal * jnp.mean(scaled * normal, axis=-1, keepdims=True))

def key_bounds(positions, lengths, prompt):
    segment = (positions - prompt) // CONT
    within = positions - prompt - segment * CONT
    slot_ids = jnp.arange(lengths.shape[0], dtype=jnp.int32)
    slot_limit = jnp.sum(jnp.where(segment[:, None] == slot_ids[None, :], lengths[None, :], 0), axis=1)
    last = prompt + (segment + 1) * CONT - 1
    last = jnp.where(within < slot_limit, last, -1)
    return jnp.where(positions < prompt, positions.shape[0], last)

def product(left_matrix, right_matrix):
    return jnp.dot(left_matrix, right_matrix, preferred_element_type=jnp.float32)

def product_transposed(left_matrix, right_matrix):
    return lax.dot_general(left_matrix, right_matrix, (((1,), (1,)), ((), ())), preferred_element_type=jnp.float32)

def row_outer(left_matrix, right_matrix):
    return lax.dot_general(left_matrix, right_matrix, (((0,), (0,)), ((), ())), preferred_element_type=jnp.float32)

def attention_forward(packed, places, key_last, heads):
    rows, columns = packed.shape
    size = columns // (3 * heads)
    block = 256
    factor = size ** (-0.5) * log2_e

    def kernel(q_ref, k_ref, v_ref, place_ref, first_ref, last_ref, out_ref, total_ref):
        scores = product_transposed(q_ref[...], k_ref[...])
        place = place_ref[...]
        allowed = (first_ref[...] <= place) & (place <= last_ref[...])
        scores = jnp.where(allowed, scores * factor, masked_score)
        top = jnp.max(scores, axis=1, keepdims=True)
        soft = jnp.exp2(scores - top)
        total = jnp.sum(soft, axis=1, keepdims=True)
        mixture = product(soft.astype(jnp.bfloat16), v_ref[...])
        out_ref[...] = (mixture / total).astype(jnp.bfloat16)
        log_total = jnp.broadcast_to(top + jnp.log2(total), (block, 128))
        total_ref[0] = log_total.T[:8]
    return pl.pallas_call(kernel, grid=(heads, rows // block), in_specs=[pl.BlockSpec((block, size), lambda h, i: (i, 3 * h)), pl.BlockSpec((rows, size), lambda h, i: (0, 3 * h + 1)), pl.BlockSpec((rows, size), lambda h, i: (0, 3 * h + 2)), pl.BlockSpec((block, 1), lambda h, i: (i, 0)), pl.BlockSpec((1, rows), lambda h, i: (0, 0)), pl.BlockSpec((1, rows), lambda h, i: (0, 0))], out_specs=[pl.BlockSpec((block, size), lambda h, i: (i, h)), pl.BlockSpec((1, 8, block), lambda h, i: (h, 0, i))], out_shape=[jax.ShapeDtypeStruct((rows, heads * size), jnp.bfloat16), jax.ShapeDtypeStruct((heads, 8, rows), jnp.float32)], compiler_params=pltpu.CompilerParams(vmem_limit_bytes=56 * MIB), cost_estimate=pl.CostEstimate(flops=4 * heads * rows * rows * size, bytes_accessed=4 * rows * heads * size * 2, transcendentals=heads * rows * rows), name='attention_forward')(packed, packed, packed, places[:, None], places[None, :], key_last[None, :])

def attention_backward(packed, totals, slopes, places, key_last, heads):
    rows, columns = packed.shape
    size = columns // (3 * heads)
    block = 256
    scale = size ** (-0.5)
    factor = scale * log2_e

    def kernel(q_ref, k_ref, v_ref, slope_ref, total_ref, place_ref, first_ref, last_ref, out_ref, turned_ref, key_sum, value_sum):
        step = pl.program_id(1)

        @pl.when(step == 0)
        def _():
            turned_ref[...] = k_ref[...].T
            key_sum[...] = jnp.zeros_like(key_sum)
            value_sum[...] = jnp.zeros_like(value_sum)
        queries = q_ref[...]
        slope = slope_ref[...]
        scores = product_transposed(k_ref[...], queries)
        place = place_ref[...]
        allowed = (first_ref[...] <= place) & (place <= last_ref[...])
        soft = jnp.where(allowed, jnp.exp2(scores * factor - total_ref[0, :1]), 0.0)
        weight_slope = product_transposed(v_ref[...], slope)
        centre = jnp.sum(soft * weight_slope, axis=0, keepdims=True)
        score_slope = (soft * (weight_slope - centre)).astype(jnp.bfloat16)
        value_sum[...] += product(soft.astype(jnp.bfloat16), slope)
        key_sum[...] += product(score_slope, queries)
        query_slope = product(turned_ref[...], score_slope)
        here = pl.ds(pl.multiple_of(step * block, block), block)
        out_ref[here, :size] = (query_slope.T * scale).astype(jnp.bfloat16)

        @pl.when(step == pl.num_programs(1) - 1)
        def _():
            out_ref[:, size:2 * size] = (key_sum[...] * scale).astype(jnp.bfloat16)
            out_ref[:, 2 * size:] = value_sum[...].astype(jnp.bfloat16)
    return pl.pallas_call(kernel, grid=(heads, rows // block), in_specs=[pl.BlockSpec((block, size), lambda h, i: (i, 3 * h)), pl.BlockSpec((rows, size), lambda h, i: (0, 3 * h + 1)), pl.BlockSpec((rows, size), lambda h, i: (0, 3 * h + 2)), pl.BlockSpec((block, size), lambda h, i: (i, h)), pl.BlockSpec((1, 8, block), lambda h, i: (h, 0, i)), pl.BlockSpec((1, block), lambda h, i: (0, i)), pl.BlockSpec((rows, 1), lambda h, i: (0, 0)), pl.BlockSpec((rows, 1), lambda h, i: (0, 0))], out_specs=pl.BlockSpec((rows, 3 * size), lambda h, i: (0, h)), out_shape=jax.ShapeDtypeStruct((rows, columns), jnp.bfloat16), scratch_shapes=[pltpu.VMEM((size, rows), jnp.bfloat16), pltpu.VMEM((rows, size), jnp.float32), pltpu.VMEM((rows, size), jnp.float32)], compiler_params=pltpu.CompilerParams(vmem_limit_bytes=56 * MIB), cost_estimate=pl.CostEstimate(flops=10 * heads * rows * rows * size, bytes_accessed=8 * rows * heads * size * 2, transcendentals=heads * rows * rows), name='attention_backward')(packed, packed, packed, slopes, totals, places[None, :], places[:, None], key_last[:, None])

def small_plane():
    return (lax.axis_size('grp'), lax.axis_size('sub')) == (4, 2)

def plane_ids():
    g, r, u = (lax.axis_index(n) for n in ('grp', 'rep', 'sub'))
    y, c = (g // 2, g % 2)
    across, up, partner = ((g, r, 1 - u), ((1 - y) * 2 + c, r, u), (y * 2 + 1 - c, r, u))

    def piece(k):
        above, beside, side = (k // 4, k // 2 % 2, k % 2)
        return ((y + above) % 2 * 2 + (c + beside) % 2) * 2 + (u + side) % 2
    return (across, up, partner, piece)

def greet(devices):
    barrier = pltpu.get_barrier_semaphore()
    for device in devices:
        pl.semaphore_signal(barrier, inc=1, device_id=device, device_id_type=MESH)
    pl.semaphore_wait(barrier, len(devices))

def remote(source, target, send, recv, number, device):
    return pltpu.make_async_remote_copy(src_ref=source, dst_ref=target, send_sem=send.at[number], recv_sem=recv.at[number], device_id=device, device_id_type=MESH)

def plane_peers():
    groups, _, subs = (lax.axis_size(n) for n in EVERY)
    g, r, u = (lax.axis_index(n) for n in EVERY)
    count = groups * subs
    place = g * subs + u
    return (place, [(t // subs, r, lax.rem(t, subs)) for t in (lax.rem(place + step, count) for step in range(1, count))])

def owner_cargo(source, target, send, recv, local):
    count = lax.axis_size('grp') * lax.axis_size('sub')
    subs = lax.axis_size('sub')
    rows, width = (target.shape[0], source.shape[1])
    place, peers = plane_peers()

    def block(t):
        return source.at[pl.ds(pl.multiple_of(t * rows, rows), rows), :]
    landing = target.at[:, pl.ds(pl.multiple_of(place * width, width), width)]
    own = pltpu.make_async_copy(block(place), landing, local)
    away = [remote(block(device[0] * subs + device[2]), landing, send, recv, number, device) for number, device in enumerate(peers)]

    def start():
        own.start()
        for one in away:
            one.start()

    def finish():
        own.wait()
        for one in away:
            one.wait_recv()
        for one in away:
            one.wait_send()
    return (start, finish)

def owner_scratch():
    count = lax.axis_size('grp') * lax.axis_size('sub')
    return [DMA((count - 1,)), DMA((count - 1,)), DMA]

def position_of(turn):
    groups = lax.axis_size('grp')
    return lax.rem(turn, 2) * (groups // 2) + turn // 2

def turn_of(position):
    half = lax.axis_size('grp') // 2
    return lax.rem(position, half) * 2 + position // half

def home_devices():
    g, r, u = (lax.axis_index(n) for n in EVERY)
    groups = lax.axis_size('grp')
    rep = lax.rem(turn_of(g) + groups - r, groups)
    return ((r, rep, u), (position_of(lax.rem(g + r, groups)), g, u), (r == g) & (rep == r))

def column_cargo(source, target, send, recv, local):
    subs = lax.axis_size('sub')
    rows, width = (source.shape[0], target.shape[1])
    place, peers = plane_peers()

    def block(t):
        return source.at[:, pl.ds(pl.multiple_of(t * width, width), width)]
    landing = target.at[pl.ds(pl.multiple_of(place * rows, rows), rows), :]
    own = pltpu.make_async_copy(block(place), landing, local)
    away = [remote(block(device[0] * subs + device[2]), landing, send, recv, number, device) for number, device in enumerate(peers)]

    def start():
        own.start()
        for one in away:
            one.start()

    def finish():
        own.wait()
        for one in away:
            one.wait_recv()
        for one in away:
            one.wait_send()
    return (start, finish)

def column_shape(weight):
    count = lax.axis_size('grp') * lax.axis_size('sub')
    return jax.ShapeDtypeStruct((weight.shape[0] * count, weight.shape[1] // count), weight.dtype)

def row_loads(source, target, sem):
    groups, reps = (lax.axis_size('grp'), lax.axis_size('rep'))
    rows = source.shape[0] // (groups * reps)
    return [pltpu.make_async_copy(source.at[pl.ds((r * groups + g) * rows, rows)], target.at[pl.ds((g * reps + r) * rows, rows)], sem.at[g, r]) for g in range(groups) for r in range(reps)]

def row_loads_scratch(shape, dtype):
    return [pltpu.VMEM(shape, dtype), DMA((lax.axis_size('grp'), lax.axis_size('rep')))]

def home_cargo(source, target, send, recv, local):
    goal, _, stays = home_devices()
    kept = pltpu.make_async_copy(source, target, local)
    moved = pltpu.make_async_remote_copy(src_ref=source, dst_ref=target, send_sem=send, recv_sem=recv, device_id=goal, device_id_type=MESH)

    def start():

        @pl.when(stays)
        def _():
            kept.start()

        @pl.when(jnp.logical_not(stays))
        def _():
            moved.start()

    def finish():

        @pl.when(stays)
        def _():
            kept.wait()

        @pl.when(jnp.logical_not(stays))
        def _():
            moved.wait_recv()
            moved.wait_send()
    return (start, finish)

def greet_all(devices, homes):
    barrier = pltpu.get_barrier_semaphore()
    for device in devices:
        pl.semaphore_signal(barrier, inc=1, device_id=device, device_id_type=MESH)
    if not homes:
        pl.semaphore_wait(barrier, len(devices))
        return
    _, origin, stays = home_devices()

    @pl.when(jnp.logical_not(stays))
    def _():
        pl.semaphore_signal(barrier, inc=1, device_id=origin, device_id_type=MESH)
    pl.semaphore_wait(barrier, len(devices) + 1 - stays.astype(jnp.int32))

def gather_kernel(weights, x_ref, *refs):
    sources, out_ref, landings = (refs[:weights], refs[weights], refs[weights + 1:2 * weights + 1])
    slots, load, send, recv, store, *cargo = refs[2 * weights + 1:]
    ids = plane_ids()
    step = pl.program_id(0)
    cargos = [column_cargo(sources[i], landings[i], *cargo[3 * i:3 * i + 3]) for i in range(weights)]

    @pl.when(step == 0)
    def _():
        first = pltpu.make_async_copy(x_ref, slots.at[0], load)
        first.start()
        greet(plane_peers()[1] if weights else ids[:3])
        first.wait()
    gather_step(step, slots, send, recv, ids)

    def keep(number):
        return pltpu.make_async_copy(slots.at[number], out_ref.at[ids[3](number)], store.at[number])
    keep(gather_order(step)).start()
    if weights:

        @pl.when(step == 2)
        def _():
            for start, _ in cargos:
                start()

    @pl.when(step == 7)
    def _():
        for _, finish in cargos:
            finish()
        for number in range(8):
            keep(number).wait()

def plane_gather(x, weights, collective_id):
    rows, width = x.shape
    if not small_plane():
        return [lax.all_gather(x, PLANE, axis=0, tiled=True)] + [exchange(w, False, collective_id + 20 + i) for i, w in enumerate(weights)]
    number = len(weights)
    every, *columns = pl.pallas_call(functools.partial(gather_kernel, number), grid=(8,), out_shape=[jax.ShapeDtypeStruct((8, rows, width), x.dtype)] + [column_shape(w) for w in weights], in_specs=[ANY] * (1 + number), out_specs=[ANY] * (1 + number), scratch_shapes=[pltpu.VMEM((8, rows, width), x.dtype), DMA, DMA((11,)), DMA((11,)), DMA((8,))] + owner_scratch() * number, compiler_params=remote_params(collective_id, 40), name='plane_gather')(x, *weights)
    return [every.reshape(8 * rows, width)] + columns

def reduce_scratch(rows, width):
    wide, narrow = (jnp.float32, jnp.bfloat16)
    return [pltpu.VMEM((4, rows, width), wide), pltpu.VMEM((4, rows, width), narrow), pltpu.VMEM((4, rows, width), narrow), pltpu.VMEM((3, rows, width), narrow), pltpu.VMEM((3, rows, width), narrow), DMA((10,)), DMA((10,))]

def reduce_order(step):
    return 7 - 2 * step + 7 * (step // 4)

def reduce_step(step, piece, refs, ids, out, before=None):
    sums, give, take, leave, come, send, recv = refs
    across, up, partner, _ = ids
    half = sums.shape[1] // 2
    low, high = (pl.ds(0, half), pl.ds(half, half))
    pair = step // 2

    def to_partner(number):
        return remote(give.at[number], take.at[number], send, recv, number, partner)

    def part(number, which, rows, device):
        return remote(leave.at[which, rows], come.at[which, rows], send, recv, number, device)

    def down(value):
        return value.astype(jnp.bfloat16)

    def up_cast(value):
        return value.astype(jnp.float32)

    @pl.when(lax.rem(step, 2) == 0)
    def _():
        give[pair] = down(piece)
        to_partner(pair).start()

    @pl.when(lax.rem(step, 2) == 1)
    def _():
        sums[pair] = piece
    if before is not None:
        before()

    @pl.when(lax.rem(step, 2) == 1)
    def _():
        to_partner(pair).wait_recv()
        sums[pair] += up_cast(take[pair])
    diagonal_across, diagonal_up = (part(4, 2, low, across), part(5, 2, high, up))
    across_low, up_high = (part(6, 0, low, across), part(7, 1, high, up))
    across_high, up_low = (part(8, 0, high, across), part(9, 1, low, up))

    @pl.when(step == 1)
    def _():
        leave[2] = down(sums[0])
        diagonal_across.start()
        diagonal_up.start()

    @pl.when(step == 3)
    def _():
        leave[0, low] = down(sums[1, low])
        across_low.start()

    @pl.when(step == 5)
    def _():
        leave[1, high] = down(sums[2, high])
        up_high.start()

    @pl.when(step == 7)
    def _():
        diagonal_up.wait_recv()
        leave[0, high] = down(sums[1, high] + up_cast(come[2, high]))
        across_high.start()
        diagonal_across.wait_recv()
        leave[1, low] = down(sums[2, low] + up_cast(come[2, low]))
        up_low.start()
        for one in (across_low, up_high, across_high, up_low):
            one.wait_recv()
        out[...] = sums[3] + up_cast(come[0]) + up_cast(come[1])
        for number in range(4):
            to_partner(number).wait_send()
        for one in (diagonal_across, diagonal_up, across_low, up_high, across_high, up_low):
            one.wait_send()

def product_reduce_kernel(owns, homes, slope_ref, weight_ref, *refs):
    ids = plane_ids()
    step = pl.program_id(0)
    refs = list(refs)
    parcels = [refs.pop(0) for _ in range(owns + homes)]
    out_ref = refs.pop(0)
    landings = [refs.pop(0) for _ in range(owns + homes)]
    slopes, load, weight, weight_load, *refs = refs
    tail = refs[7:]
    rows_in = row_loads(weight_ref, weight, weight_load)
    early, late = ([], [])
    if owns:
        late.append(owner_cargo(parcels[0], landings[0], *tail[:3]))
    if homes:
        early.append(home_cargo(parcels[-1], landings[-1], *tail[-3:]))

    def fetch(number):
        return pltpu.make_async_copy(slope_ref.at[ids[3](number)], slopes.at[number], load.at[number])

    @pl.when(step == 0)
    def _():
        for one in rows_in:
            one.start()
        for number in range(8):
            fetch(reduce_order(number)).start()
        greet_all(plane_peers()[1] if owns else ids[:3], homes)
        for start, _ in early:
            start()
        for one in rows_in:
            one.wait()
    k = reduce_order(step)
    fetch(k).wait()
    reduce_step(step, product_transposed(slopes[k], weight[...]), refs[:7], ids, out_ref)
    if owns:

        @pl.when(step == 5)
        def _():
            for start, _ in late:
                start()
    if owns or homes:

        @pl.when(step == 7)
        def _():
            for _, finish in late + early:
                finish()

def remote_params(collective_id, limit):
    return pltpu.CompilerParams(collective_id=collective_id, has_side_effects=True, vmem_limit_bytes=limit * MIB)

def owner_shape(parcel):
    count = lax.axis_size('grp') * lax.axis_size('sub')
    return jax.ShapeDtypeStruct((parcel.shape[0] // count, parcel.shape[1] * count), parcel.dtype)

def product_reduce(slopes, weight, owned, homed, collective_id):
    count, rows, inner = slopes.shape
    width = weight.shape[0]
    owns, homes = (owned is not None, homed is not None)
    if not small_plane():
        part = product_transposed(slopes.reshape(-1, inner), rep_rows_last(weight))
        whole = [lax.psum_scatter(part.astype(jnp.bfloat16), PLANE, scatter_dimension=0, tiled=True).astype(jnp.float32)]
        return whole + ([exchange(owned, True, collective_id)] if owns else []) + ([from_plane(homed)] if homes else [])
    cargo = ([owned] if owns else []) + ([homed] if homes else [])
    shapes = ([owner_shape(owned)] if owns else []) + ([jax.ShapeDtypeStruct(homed.shape, homed.dtype)] if homes else [])
    return pl.pallas_call(functools.partial(product_reduce_kernel, owns, homes), grid=(8,), out_shape=[jax.ShapeDtypeStruct((rows, width), jnp.float32)] + shapes, in_specs=[ANY, ANY] + [ANY] * len(cargo), out_specs=[VMEM] + [ANY] * len(cargo), scratch_shapes=[pltpu.VMEM((8, rows, inner), slopes.dtype), DMA((8,)), *row_loads_scratch(weight.shape, weight.dtype), *reduce_scratch(rows, width)] + (owner_scratch() if owns else []) + ([DMA, DMA, DMA] if homes else []), compiler_params=remote_params(collective_id, 60), name='product_reduce')(slopes, weight, *cargo)

def closing_kernel(number, x_ref, homed_ref, *refs):
    owned_refs, (out_ref, homed_out), owned_outs = (refs[:number], refs[number:number + 2], refs[number + 2:2 * number + 2])
    refs = refs[2 * number + 2:]
    here = {n: lax.axis_index(n) for n in EVERY}
    phases = ('grp', 'sub', 'rep')
    home_start, home_finish = home_cargo(homed_ref, homed_out, *refs[:3])
    owners = [owner_cargo(owned_refs[i], owned_outs[i], *refs[3 + 3 * i:6 + 3 * i]) for i in range(number)]
    refs = refs[3 + 3 * number:]

    def other(name, step):
        size = lax.axis_size(name)
        return tuple((lax.rem(here[n] + step, size) if n == name else here[n] for n in EVERY))
    greet_all(plane_peers()[1] + [other('rep', s) for s in range(1, lax.axis_size('rep'))], True)
    home_start()
    out_ref[...] = x_ref[...]
    for j, name in enumerate(phases):
        slots, send, recv = refs[3 * j:3 * j + 3]
        size = lax.axis_size(name)
        me = here[name]
        slots[me] = out_ref[...]
        copies = []
        for s in range(1, size):
            one = pltpu.make_async_remote_copy(src_ref=out_ref, dst_ref=slots.at[me], send_sem=send.at[s], recv_sem=recv.at[s], device_id=other(name, s), device_id_type=MESH)
            one.start()
            copies.append(one)
        if name == 'rep':
            for start, _ in owners:
                start()
        for one in copies:
            one.wait_recv()
        for one in copies:
            one.wait_send()
        value = slots[0]
        for s in range(1, size):
            value = value + slots[s]
        out_ref[...] = value
    for _, finish in owners:
        finish()
    home_finish()

def closing(x, homed, owned, collective_id):
    scratch = []
    for name in ('grp', 'sub', 'rep'):
        n = lax.axis_size(name)
        scratch += [pltpu.VMEM((n,) + x.shape, x.dtype), DMA((n,)), DMA((n,))]
    number = len(owned)
    return pl.pallas_call(functools.partial(closing_kernel, number), out_shape=[jax.ShapeDtypeStruct(x.shape, x.dtype), jax.ShapeDtypeStruct(homed.shape, homed.dtype)] + [owner_shape(one) for one in owned], in_specs=[VMEM] + [ANY] * (1 + number), out_specs=[VMEM] + [ANY] * (1 + number), scratch_shapes=[DMA, DMA, DMA] + owner_scratch() * number + scratch, compiler_params=pltpu.CompilerParams(collective_id=collective_id, has_side_effects=True), name='closing')(x, homed, *owned)

def exchange_kernel(to_tokens, x_ref, out_ref, send, recv, local):
    groups, reps, subs = (lax.axis_size(n) for n in EVERY)
    g, r, u = (lax.axis_index(n) for n in EVERY)
    count = groups * subs
    place = g * subs + u
    if to_tokens:
        tokens, width = (out_ref.shape[0], x_ref.shape[1])
    else:
        tokens, width = (x_ref.shape[0], out_ref.shape[1])

    def rows(ref, t):
        return ref.at[pl.ds(pl.multiple_of(t * tokens, tokens), tokens), :]

    def columns(ref, t):
        return ref.at[:, pl.ds(pl.multiple_of(t * width, width), width)]
    source, target = (rows, columns) if to_tokens else (columns, rows)
    peers = [lax.rem(place + step, count) for step in range(1, count)]

    def device(t):
        return (t // subs, r, lax.rem(t, subs))
    own = pltpu.make_async_copy(source(x_ref, place), target(out_ref, place), local)
    own.start()
    greet([device(t) for t in peers])
    copies = []
    for step, t in enumerate(peers):
        one = pltpu.make_async_remote_copy(src_ref=source(x_ref, t), dst_ref=target(out_ref, place), send_sem=send.at[step], recv_sem=recv.at[step], device_id=device(t), device_id_type=MESH)
        one.start()
        copies.append(one)
    own.wait()
    for one in copies:
        one.wait_recv()
    for one in copies:
        one.wait_send()

def exchange(x, to_tokens, collective_id):
    count = lax.axis_size('grp') * lax.axis_size('sub')
    shape = (x.shape[0] // count, x.shape[1] * count) if to_tokens else (x.shape[0] * count, x.shape[1] // count)
    return pl.pallas_call(functools.partial(exchange_kernel, to_tokens), out_shape=jax.ShapeDtypeStruct(shape, x.dtype), in_specs=[ANY], out_specs=ANY, scratch_shapes=[DMA((count - 1,)), DMA((count - 1,)), DMA], compiler_params=pltpu.CompilerParams(collective_id=collective_id, has_side_effects=True), name='to_tokens' if to_tokens else 'to_heads')(x)

def opening_kernel(x_ref, *refs):
    weights = (len(refs) - 8) // 2
    sources, (moved_ref, *landings) = (refs[:weights], refs[weights:2 * weights + 1])
    transit, move_send, move_recv, move_local, send, recv, local = refs[2 * weights + 1:]
    groups, _, subs = (lax.axis_size(n) for n in EVERY)
    g, r, u = (lax.axis_index(n) for n in EVERY)
    place, peers = plane_peers()
    relay = position_of(lax.rem(g + r, groups))
    beyond = lax.rem(turn_of(g) + groups - r, groups)

    def block(number, t):
        width = landings[number].shape[1]
        return sources[number].at[:, pl.ds(pl.multiple_of(t * width, width), width)]

    def landing(number):
        rows = sources[number].shape[0]
        return landings[number].at[pl.ds(pl.multiple_of(place * rows, rows), rows), :]

    def hop(number, source, target, device, stays):
        kept = pltpu.make_async_copy(source, target, move_local.at[number])
        moved = remote(source, target, move_send, move_recv, number, device)

        def start():

            @pl.when(stays)
            def _():
                kept.start()

            @pl.when(jnp.logical_not(stays))
            def _():
                moved.start()

        def arrive():

            @pl.when(stays)
            def _():
                kept.wait()

            @pl.when(jnp.logical_not(stays))
            def _():
                moved.wait_recv()

        def leave():

            @pl.when(jnp.logical_not(stays))
            def _():
                moved.wait_send()
        return (start, arrive, leave)
    first = hop(0, x_ref, transit, (relay, r, u), relay == g)
    second = hop(1, transit, moved_ref, (g, beyond, u), beyond == r)
    owns = [pltpu.make_async_copy(block(number, place), landing(number), local.at[number]) for number in range(weights)]
    for one in owns:
        one.start()
    barrier = pltpu.get_barrier_semaphore()
    for device in peers:
        pl.semaphore_signal(barrier, inc=1, device_id=device, device_id_type=MESH)

    @pl.when(beyond != r)
    def _():
        pl.semaphore_signal(barrier, inc=1, device_id=(g, beyond, u), device_id_type=MESH)
    pl.semaphore_wait(barrier, len(peers) + (beyond != r).astype(jnp.int32))
    first[0]()
    copies = []
    for number in range(weights):
        for step, device in enumerate(peers):
            one = pltpu.make_async_remote_copy(src_ref=block(number, device[0] * subs + device[2]), dst_ref=landing(number), send_sem=send.at[number, step], recv_sem=recv.at[number, step], device_id=device, device_id_type=MESH)
            one.start()
            copies.append(one)
    first[1]()
    second[0]()
    for one in owns:
        one.wait()
    for one in copies:
        one.wait_recv()
    for one in copies:
        one.wait_send()
    first[2]()
    second[1]()
    second[2]()

def opening(x, weights, collective_id):
    count = lax.axis_size('grp') * lax.axis_size('sub')
    number = len(weights)
    columns = [jax.ShapeDtypeStruct((w.shape[0] * count, w.shape[1] // count), w.dtype) for w in weights]
    return pl.pallas_call(opening_kernel, out_shape=[jax.ShapeDtypeStruct(x.shape, x.dtype), *columns], in_specs=[VMEM] + [ANY] * number, out_specs=[VMEM] + [ANY] * number, scratch_shapes=[pltpu.VMEM(x.shape, x.dtype), DMA((2,)), DMA((2,)), DMA((2,)), DMA((number, count - 1)), DMA((number, count - 1)), DMA((number,))], compiler_params=pltpu.CompilerParams(collective_id=collective_id, has_side_effects=True), name='opening')(x, *weights)

def attend_kernel(heads, head_ref, place_ref, first_ref, last_ref, mixing_ref, attended_ref, total_ref, out_ref, *refs):
    ids = plane_ids()
    step = pl.program_id(0)

    @pl.when(step == 0)
    def _():
        greet(ids[:3])
    rows = out_ref.shape[0]
    size = attended_ref.shape[1] // heads
    factor = size ** (-0.5) * log2_e
    first_row = pl.multiple_of(ids[3](reduce_order(step)) * rows, rows)
    here = pl.ds(first_row, rows)
    place = place_ref[here, :]
    allowed = (first_ref[...] <= place) & (place <= last_ref[...])
    for h in range(heads):
        q, k, v = (3 * h + j for j in range(3))
        scores = product_transposed(head_ref[here, q * size:(q + 1) * size], head_ref[:, k * size:(k + 1) * size])
        scores = jnp.where(allowed, scores * factor, masked_score)
        top = jnp.max(scores, axis=1, keepdims=True)
        soft = jnp.exp2(scores - top)
        total = jnp.sum(soft, axis=1, keepdims=True)
        mixture = product(soft.astype(jnp.bfloat16), head_ref[:, v * size:(v + 1) * size])
        attended_ref[here, h * size:(h + 1) * size] = (mixture / total).astype(jnp.bfloat16)
        log_total = jnp.broadcast_to(top + jnp.log2(total), (rows, 128))
        total_ref[h, :, here] = log_total.T[:8]
    reduce_step(step, product(attended_ref[here, :], mixing_ref[...]), refs, ids, out_ref)

def attend(packed, places, key_last, mixing, heads, token_rows, collective_id):
    rows = packed.shape[0]
    inner, width = mixing.shape
    if not small_plane():
        attended, totals = attention_forward(packed, places, key_last, heads)
        part = product(attended, mixing).astype(jnp.bfloat16)
        return (attended, totals, lax.psum_scatter(part, PLANE, scatter_dimension=0, tiled=True).astype(jnp.float32))
    return pl.pallas_call(functools.partial(attend_kernel, heads), grid=(8,), out_shape=[jax.ShapeDtypeStruct((rows, inner), jnp.bfloat16), jax.ShapeDtypeStruct((heads, 8, rows), jnp.float32), jax.ShapeDtypeStruct((token_rows, width), jnp.float32)], in_specs=[VMEM] * 5, out_specs=[VMEM] * 3, scratch_shapes=reduce_scratch(token_rows, width), compiler_params=remote_params(collective_id, 60), name='attend')(packed, places[:, None], places[None, :], key_last[None, :], mixing)

def gather_order(step):
    return step + 2 * (step % 2) - 1 + (8 - step) // 8 - step // 7

def gather_step(step, slots, send, recv, ids):
    across, up, partner, _ = ids
    half = slots.shape[1] // 2
    low, high = (pl.ds(0, half), pl.ds(half, half))

    def copy(number, source, target, device):
        return remote(slots.at[source], slots.at[target], send, recv, number, device)
    across_low = copy(0, (0, low), (1, low), across)
    up_high = copy(1, (0, high), (4, high), up)
    across_high = copy(2, (0, high), (1, high), across)
    up_low = copy(3, (0, low), (4, low), up)
    own = copy(4, 0, 2, partner)
    far_low = copy(5, (1, low), (5, low), up)
    far_high = copy(6, (4, high), (5, high), across)
    pass_across = copy(7, 1, 3, partner)
    pass_up = copy(8, 4, 6, partner)
    pass_low = copy(9, (5, low), (7, low), partner)
    pass_high = copy(10, (5, high), (7, high), partner)

    @pl.when(step == 0)
    def _():
        for one in (across_low, up_high, own, across_high, up_low):
            one.start()

    @pl.when(step == 1)
    def _():
        own.wait_recv()

    @pl.when(step == 2)
    def _():
        across_low.wait_recv()
        far_low.start()
        up_high.wait_recv()
        far_high.start()
        across_high.wait_recv()
        pass_across.start()

    @pl.when(step == 3)
    def _():
        up_low.wait_recv()
        pass_up.start()

    @pl.when(step == 4)
    def _():
        pass_across.wait_recv()

    @pl.when(step == 5)
    def _():
        pass_up.wait_recv()

    @pl.when(step == 6)
    def _():
        far_low.wait_recv()
        pass_low.start()
        far_high.wait_recv()
        pass_high.start()

    @pl.when(step == 7)
    def _():
        pass_low.wait_recv()
        pass_high.wait_recv()
        for one in (across_low, up_high, across_high, up_low, own, far_low, far_high, pass_across, pass_up, pass_low, pass_high):
            one.wait_send()

def attend_back_kernel(heads, branch_ref, homed_ref, head_ref, mixing_ref, attended_ref, total_ref, place_ref, first_ref, last_ref, part_ref, out_ref, homed_out, turned, key_sum, value_sum, part_sum, slots, load, send, recv, *cargo):
    ids = plane_ids()
    step = pl.program_id(0)
    home_start, home_finish = home_cargo(homed_ref, homed_out, *cargo)
    rows = slots.shape[1]
    size = head_ref.shape[1] // (3 * heads)
    scale = size ** (-0.5)
    factor = scale * log2_e

    @pl.when(step == 0)
    def _():
        first = pltpu.make_async_copy(branch_ref, slots.at[0], load)
        first.start()
        for h in range(heads):
            turned[h] = head_ref[:, (3 * h + 1) * size:(3 * h + 2) * size].T
        key_sum[...] = jnp.zeros_like(key_sum)
        value_sum[...] = jnp.zeros_like(value_sum)
        part_sum[...] = jnp.zeros_like(part_sum)
        greet_all(ids[:3], True)
        home_start()
        first.wait()
    gather_step(step, slots, send, recv, ids)
    k = gather_order(step)
    here = pl.ds(pl.multiple_of(ids[3](k) * rows, rows), rows)
    part_sum[...] += row_outer(attended_ref[here, :], slots[k])
    slopes = product_transposed(slots[k], mixing_ref[...]).astype(jnp.bfloat16)
    place = place_ref[:, here]
    allowed = (first_ref[...] <= place) & (place <= last_ref[...])
    for h in range(heads):
        queries = head_ref[here, 3 * h * size:(3 * h + 1) * size]
        keys = head_ref[:, (3 * h + 1) * size:(3 * h + 2) * size]
        values = head_ref[:, (3 * h + 2) * size:(3 * h + 3) * size]
        slope = slopes[:, h * size:(h + 1) * size]
        scores = product_transposed(keys, queries)
        soft = jnp.where(allowed, jnp.exp2(scores * factor - total_ref[h, :1, here]), 0.0)
        weight_slope = product_transposed(values, slope)
        centre = jnp.sum(soft * weight_slope, axis=0, keepdims=True)
        score_slope = (soft * (weight_slope - centre)).astype(jnp.bfloat16)
        value_sum[h] += product(soft.astype(jnp.bfloat16), slope)
        key_sum[h] += product(score_slope, queries)
        query_slope = product(turned[h], score_slope)
        out_ref[here, 3 * h * size:(3 * h + 1) * size] = (query_slope.T * scale).astype(jnp.bfloat16)

    @pl.when(step == 7)
    def _():
        for h in range(heads):
            out_ref[:, (3 * h + 1) * size:(3 * h + 2) * size] = (key_sum[h] * scale).astype(jnp.bfloat16)
            out_ref[:, (3 * h + 2) * size:(3 * h + 3) * size] = value_sum[h].astype(jnp.bfloat16)
        part_ref[...] = part_sum[...].astype(jnp.bfloat16)
        home_finish()

def attend_back(branch_slope, homed, packed, mixing, attended, totals, places, key_last, heads, collective_id):
    rows, columns = packed.shape
    token_rows, width = branch_slope.shape
    size = columns // (3 * heads)
    if not small_plane():
        every = lax.all_gather(branch_slope, PLANE, axis=0, tiled=True)
        slopes = product_transposed(every, mixing).astype(jnp.bfloat16)
        part = row_outer(attended, every).astype(jnp.bfloat16)
        slopes = attention_backward(packed, totals, slopes, places, key_last, heads)
        return (part, slopes, from_plane(homed))
    return pl.pallas_call(functools.partial(attend_back_kernel, heads), grid=(8,), out_shape=[jax.ShapeDtypeStruct(mixing.shape, jnp.bfloat16), jax.ShapeDtypeStruct((rows, columns), jnp.bfloat16), jax.ShapeDtypeStruct(homed.shape, homed.dtype)], in_specs=[ANY] * 2 + [VMEM] * 7, out_specs=[VMEM, VMEM, ANY], scratch_shapes=[pltpu.VMEM((heads, size, rows), jnp.bfloat16), pltpu.VMEM((heads, rows, size), jnp.float32), pltpu.VMEM((heads, rows, size), jnp.float32), pltpu.VMEM(mixing.shape, jnp.float32), pltpu.VMEM((8, token_rows, width), jnp.bfloat16), DMA, DMA((11,)), DMA((11,)), DMA, DMA, DMA], compiler_params=remote_params(collective_id, 62), name='attend_back')(branch_slope, homed, packed, mixing, attended, totals, places[None, :], places[:, None], key_last[:, None])

def add_outer(total, left, right):
    turned = left.T
    for first in range(0, total.shape[1], 256):
        here = pl.ds(first, 256)
        total[:, here] += product(turned, right[:, first:first + 256])

def rep_order(total, narrow, part_ref, sem):
    groups, reps = (lax.axis_size('grp'), lax.axis_size('rep'))
    rows = total.shape[0] // (groups * reps)
    for g in range(groups):
        for r in range(reps):
            come, go = (pl.ds((g * reps + r) * rows, rows), pl.ds((r * groups + g) * rows, rows))
            narrow[come, :] = total[come, :].astype(jnp.bfloat16)
            pltpu.make_async_copy(narrow.at[come], part_ref.at[go], sem.at[g, r]).start()

def rep_order_wait(narrow, part_ref, sem):
    groups, reps = (lax.axis_size('grp'), lax.axis_size('rep'))
    rows = narrow.shape[0] // (groups * reps)
    for g in range(groups):
        for r in range(reps):
            come, go = (pl.ds((g * reps + r) * rows, rows), pl.ds((r * groups + g) * rows, rows))
            pltpu.make_async_copy(narrow.at[come], part_ref.at[go], sem.at[g, r]).wait()

def hidden_kernel(middle_ref, cotangent_ref, expand_ref, offset_ref, every_ref, active_ref, rise_ref, part_ref, slots, cotangents, actives, rises, total, load, send, recv, store, fetch_cotangent, active_store, rise_store, expand, expand_load, narrow, part_store):
    ids = plane_ids()
    step = pl.program_id(0)
    turn = lax.rem(step, 2)

    def fetch(number, side):
        return pltpu.make_async_copy(cotangent_ref.at[ids[3](gather_order(number))], cotangents.at[side], fetch_cotangent.at[side])

    @pl.when(step == 0)
    def _():
        first = pltpu.make_async_copy(middle_ref, slots.at[0], load)
        first.start()
        rows_in = row_loads(expand_ref, expand, expand_load)
        for one in rows_in:
            one.start()
        fetch(0, 0).start()
        total[...] = jnp.zeros_like(total)
        greet(ids[:3])
        first.wait()
        for one in rows_in:
            one.wait()
    gather_step(step, slots, send, recv, ids)
    k = gather_order(step)

    def keep(number):
        return pltpu.make_async_copy(slots.at[number], every_ref.at[ids[3](number)], store.at[number])

    def put(number, side):
        piece = ids[3](number)
        return (pltpu.make_async_copy(actives.at[side], active_ref.at[piece], active_store.at[side]), pltpu.make_async_copy(rises.at[side], rise_ref.at[piece], rise_store.at[side]))
    keep(k).start()

    @pl.when(step >= 2)
    def _():
        for one in put(k, turn):
            one.wait()
    expanded = product(slots[k], expand[...]) + offset_ref[...]
    below = 0.5 * (1.0 + lax.erf(expanded * root_half))
    actives[turn] = (expanded * below).astype(jnp.bfloat16)
    rises[turn] = below + expanded * (jnp.exp(-0.5 * expanded * expanded) * normal_peak)
    for one in put(k, turn):
        one.start()
    fetch(step, turn).wait()

    @pl.when(step < 7)
    def _():
        fetch(step + 1, 1 - turn).start()
    add_outer(total, cotangents[turn], actives[turn])

    @pl.when(step == 7)
    def _():
        rep_order(total, narrow, part_ref, part_store)
        for late in range(2):
            for one in put(k, late):
                one.wait()
        for number in range(8):
            keep(number).wait()
        rep_order_wait(narrow, part_ref, part_store)

def hidden(middle, cotangent_all, expand_slice, offset, collective_id):
    rows, width = middle.shape
    count = lax.axis_size('grp') * lax.axis_size('sub')
    inner = expand_slice.shape[1]
    if not small_plane():
        every = lax.all_gather(middle, PLANE, axis=0, tiled=True)
        expanded = product(every, rep_rows_last(expand_slice)) + offset
        below = 0.5 * (1.0 + lax.erf(expanded * root_half))
        rise = below + expanded * (jnp.exp(-0.5 * expanded * expanded) * normal_peak)
        active = (expanded * below).astype(jnp.bfloat16)
        return (every, active, rise, rep_rows_first(row_outer(cotangent_all, active)))
    every, active, rise, part = pl.pallas_call(hidden_kernel, grid=(8,), out_shape=[jax.ShapeDtypeStruct((8, rows, width), middle.dtype), jax.ShapeDtypeStruct((8, rows, inner), jnp.bfloat16), jax.ShapeDtypeStruct((8, rows, inner), jnp.float32), jax.ShapeDtypeStruct((width, inner), jnp.bfloat16)], in_specs=[ANY, ANY, ANY, VMEM], out_specs=[ANY] * 4, scratch_shapes=[pltpu.VMEM((8, rows, width), middle.dtype), pltpu.VMEM((2, rows, width), jnp.bfloat16), pltpu.VMEM((2, rows, inner), jnp.bfloat16), pltpu.VMEM((2, rows, inner), jnp.float32), pltpu.VMEM((width, inner), jnp.float32), DMA, DMA((11,)), DMA((11,)), DMA((8,)), DMA((2,)), DMA((2,)), DMA((2,)), *row_loads_scratch(expand_slice.shape, expand_slice.dtype), *row_loads_scratch(expand_slice.shape, jnp.bfloat16)], compiler_params=remote_params(collective_id, 60), name='hidden')(middle, cotangent_all.reshape(8, rows, width), expand_slice, offset[None, :])
    return (every.reshape(count * rows, width), active.reshape(count * rows, inner), rise.reshape(count * rows, inner), part)

def hidden_back_kernel(cotangent_ref, middle_ref, rise_ref, shrink_ref, expand_ref, slope_ref, out_ref, part_ref, cotangents, middles, rises, slopes, total, fetches, store, shrink, shrink_load, expand, expand_load, narrow, part_store, *refs):
    ids = plane_ids()
    step = pl.program_id(0)

    def fetch(number, side):
        piece = ids[3](reduce_order(number))
        return [pltpu.make_async_copy(source.at[piece], target.at[side], fetches.at[kind, side]) for kind, (source, target) in enumerate(((cotangent_ref, cotangents), (rise_ref, rises), (middle_ref, middles)))]

    def put(number, side):
        return pltpu.make_async_copy(slopes.at[side], slope_ref.at[ids[3](reduce_order(number))], store.at[side])
    turn = lax.rem(step, 2)

    @pl.when(step == 0)
    def _():
        rows_in = row_loads(shrink_ref, shrink, shrink_load) + row_loads(expand_ref, expand, expand_load)
        for one in rows_in:
            one.start()
        for one in fetch(0, 0):
            one.start()
        total[...] = jnp.zeros_like(total)
        greet(ids[:3])
        for one in rows_in:
            one.wait()
    for one in fetch(step, turn):
        one.wait()

    @pl.when(step < 7)
    def _():
        for one in fetch(step + 1, 1 - turn):
            one.start()

    @pl.when(step >= 2)
    def _():
        put(step, turn).wait()
    slope = product(cotangents[turn], shrink[...]) * rises[turn]
    slopes[turn] = slope.astype(jnp.bfloat16)
    put(step, turn).start()

    def before():
        add_outer(total, middles[turn], slopes[turn])

        @pl.when(step == 7)
        def _():
            rep_order(total, narrow, part_ref, part_store)
    reduce_step(step, product_transposed(slopes[turn], expand[...]), refs, ids, out_ref, before)

    @pl.when(step == 7)
    def _():
        put(6, 0).wait()
        put(7, 1).wait()
        rep_order_wait(narrow, part_ref, part_store)

def hidden_back(cotangent_all, middle_all, rise, shrink_slice, expand_slice, token_rows, collective_id):
    rows, width = cotangent_all.shape
    inner = shrink_slice.shape[1]
    if not small_plane():
        slope = (product(cotangent_all, rep_rows_last(shrink_slice)) * rise).astype(jnp.bfloat16)
        part = product_transposed(slope, rep_rows_last(expand_slice)).astype(jnp.bfloat16)
        normed = lax.psum_scatter(part, PLANE, scatter_dimension=0, tiled=True).astype(jnp.float32)
        return (slope, normed, rep_rows_first(row_outer(middle_all, slope)))
    pieces = (8, token_rows, width)
    slope, normed, part = pl.pallas_call(hidden_back_kernel, grid=(8,), out_shape=[jax.ShapeDtypeStruct((8, token_rows, inner), jnp.bfloat16), jax.ShapeDtypeStruct((token_rows, width), jnp.float32), jax.ShapeDtypeStruct((width, inner), jnp.bfloat16)], in_specs=[ANY] * 5, out_specs=[ANY, VMEM, ANY], scratch_shapes=[pltpu.VMEM((2, token_rows, width), jnp.bfloat16), pltpu.VMEM((2, token_rows, width), jnp.bfloat16), pltpu.VMEM((2, token_rows, inner), jnp.float32), pltpu.VMEM((2, token_rows, inner), jnp.bfloat16), pltpu.VMEM((width, inner), jnp.float32), DMA((3, 2)), DMA((2,)), *row_loads_scratch(shrink_slice.shape, shrink_slice.dtype), *row_loads_scratch(expand_slice.shape, expand_slice.dtype), *row_loads_scratch(expand_slice.shape, jnp.bfloat16), *reduce_scratch(token_rows, width)], compiler_params=remote_params(collective_id, 63), name='hidden_back')(cotangent_all.reshape(pieces), middle_all.reshape(pieces), rise.reshape(8, token_rows, inner), shrink_slice, expand_slice)
    return (slope.reshape(rows, inner), normed, part)

def plane_moves():
    groups, reps, subs = (lax.axis_size(n) for n in EVERY)
    moves = []
    for g in range(groups):
        for r in range(reps):
            turn = (g + r) % groups
            position = turn % 2 * (groups // 2) + turn // 2
            for u in range(subs):
                moves.append(tuple(((a * reps + b) * subs + u for a, b in ((g, r), (position, r), (position, g)))))
    return moves

def to_door(array):
    return lax.ppermute(array, EVERY, [(home, door) for home, door, _ in plane_moves()])

def to_keeper(array):
    return lax.ppermute(array, EVERY, [(door, away) for _, door, away in plane_moves()])

def to_plane_at_once(array):
    return lax.ppermute(array, EVERY, [(home, away) for home, _, away in plane_moves()])

def from_plane(array):
    return lax.ppermute(array, EVERY, [(away, home) for home, _, away in plane_moves()])

def plane_order(places):
    groups = lax.axis_size('grp')
    blocks = jnp.roll(places.reshape(groups, -1), lax.axis_index('rep'), axis=0)
    return blocks.reshape(groups // 2, 2, -1).transpose(1, 0, 2).reshape(-1)

def rep_rows(own):
    return lax.all_gather(own, 'rep', axis=0, tiled=True)

def rep_rows_last(every):
    groups, reps, subs = (lax.axis_size(name) for name in EVERY)
    columns = every.shape[1]
    ordered = every.reshape(reps, groups, subs, -1, columns).transpose(1, 0, 2, 3, 4)
    return ordered.reshape(-1, columns)

def rep_rows_first(gradient):
    groups, reps, subs = (lax.axis_size(name) for name in EVERY)
    columns = gradient.shape[1]
    ordered = gradient.astype(jnp.bfloat16).reshape(groups, reps, subs, -1, columns)
    return ordered.transpose(1, 0, 2, 3, 4).reshape(-1, columns)

def rep_sums(ordered):
    return lax.psum_scatter(ordered, 'rep', scatter_dimension=0, tiled=True)

def sub_turn(block):
    groups, reps, subs = (lax.axis_size(name) for name in EVERY)
    low = reps // subs
    moves = [((g * reps + r) * subs + u, (g * reps + u * low + r % low) * subs + r // low) for g in range(groups) for r in range(reps) for u in range(subs)]
    return lax.ppermute(block, EVERY, moves)

def sub_rows(own):
    rows, width = own.shape
    reps, subs = (lax.axis_size('rep'), lax.axis_size('sub'))
    shares = own.reshape(subs, reps // subs, -1, width)
    if subs != 2:
        every = lax.all_to_all(shares, 'sub', split_axis=0, concat_axis=0, tiled=True)
        return every.transpose(1, 0, 2, 3).reshape(rows, width)
    me = lax.axis_index('sub')
    kept = jnp.where(me == 0, shares[0], shares[1])
    come = lax.ppermute(jnp.where(me == 0, shares[1], shares[0]), 'sub', [(0, 1), (1, 0)])
    first, second = (jnp.where(me == 0, kept, come), jnp.where(me == 0, come, kept))
    return jnp.stack([first, second], axis=1).reshape(rows, width)

def mixing_sums_of(part):
    reps, subs = (lax.axis_size('rep'), lax.axis_size('sub'))
    rows, width = part.shape
    ordered = part.reshape(reps // subs, subs, rows // reps, width).transpose(1, 0, 2, 3)
    return lax.psum_scatter(ordered.reshape(rows, width), 'rep', scatter_dimension=0, tiled=True)

def sub_owned(part, reps):
    rows, width = part.shape
    subs = lax.axis_size('sub')
    shares = part.reshape(reps // subs, subs, -1, width).transpose(1, 0, 2, 3)
    if subs != 2:
        every = lax.all_to_all(shares, 'sub', split_axis=0, concat_axis=0, tiled=True)
        return every.reshape(rows, width)
    me = lax.axis_index('sub')
    kept = jnp.where(me == 0, shares[0], shares[1])
    come = lax.ppermute(jnp.where(me == 0, shares[1], shares[0]), 'sub', [(0, 1), (1, 0)])
    first, second = (jnp.where(me == 0, kept, come), jnp.where(me == 0, come, kept))
    return jnp.concatenate([first, second], axis=0).reshape(rows, width)

def shards(layer_input, entry_gain, entry_shift, joint_weight, query_offset, value_offset, mixing_weight, attention_offset, middle_gain, middle_shift, expand_weight, expand_offset, shrink_weight, shrink_offset, placement, slot_lengths, cotangent):
    token_rows, width = layer_input.shape
    hidden_width = expand_weight.shape[1]
    groups, reps, subs = (lax.axis_size(name) for name in EVERY)
    plane_count = groups * subs
    plane_index = lax.axis_index(PLANE)
    head_size = width // HEADS
    local_heads = HEADS // plane_count
    head_columns = local_heads * head_size
    plane_rows = plane_count * token_rows
    facts = to_plane_at_once(jnp.concatenate([placement, slot_lengths], axis=1))[0]
    mixing_own = rep_rows(mixing_weight)
    moved_input, joint_own, expand_own, shrink_own = opening(layer_input, (joint_weight, expand_weight, shrink_weight), 12)
    joint_own, mixing_own = lax.optimization_barrier((joint_own, mixing_own))
    input_float = moved_input.astype(jnp.float32)
    joint_every = rep_rows(joint_own)
    entry_normal, entry_inverse = norm_terms(input_float)
    entry_normed = (entry_normal * entry_gain + entry_shift).astype(jnp.bfloat16)
    entry_all, = plane_gather(entry_normed, (), 1)
    cotangent, facts, entry_all = lax.optimization_barrier((cotangent, facts, entry_all))
    cotangent = to_door(cotangent)
    places = plane_order(facts[:placement.shape[1]])
    lengths = facts[placement.shape[1]:]
    prompt = places.shape[0] // 2
    key_last = key_bounds(places, lengths, prompt)
    expand_slice = rep_rows(expand_own)
    shrink_slice = rep_rows(shrink_own)
    cotangent = to_keeper(cotangent)
    mixing_slice = sub_rows(mixing_own)
    offsets = jnp.stack([query_offset.reshape(HEADS, head_size), jnp.zeros((HEADS, head_size), jnp.float32), value_offset.reshape(HEADS, head_size)], axis=1).reshape(-1)
    offsets = lax.dynamic_slice_in_dim(offsets, plane_index * 3 * head_columns, 3 * head_columns)
    heads_kept = (product(entry_all, rep_rows_last(joint_every)) + offsets).astype(jnp.bfloat16)
    attended, log_totals, branch = attend(heads_kept, places, key_last, mixing_slice, local_heads, token_rows, 3)
    residual = input_float + (branch + attention_offset)
    middle_normal, middle_inverse = norm_terms(residual)
    middle_normed = (middle_normal * middle_gain + middle_shift).astype(jnp.bfloat16)
    cotangent, middle_normed = lax.optimization_barrier((cotangent, middle_normed))
    cotangent_all, = plane_gather(cotangent, (), 4)
    middle_normed, cotangent_all = lax.optimization_barrier((middle_normed, cotangent_all))
    hidden_local = hidden_width // plane_count
    offset_local = lax.dynamic_slice_in_dim(expand_offset, plane_index * hidden_local, hidden_local)
    middle_all, activated, rise, shrink_part = hidden(middle_normed, cotangent_all, expand_slice, offset_local, 5)
    shrink_sums = rep_sums(shrink_part)
    expanded_slope, normed_slope, expand_part = hidden_back(cotangent_all, middle_all, rise, shrink_slice, expand_slice, token_rows, 6)
    expand_sums = rep_sums(expand_part)
    activated, normed_slope = lax.optimization_barrier((activated, normed_slope))
    shrunk, = product_reduce(activated.reshape(plane_count, token_rows, hidden_local), shrink_slice, None, None, 8)
    own_output = (residual + shrunk + shrink_offset).astype(jnp.bfloat16)
    own_output, normed_slope = lax.optimization_barrier((own_output, normed_slope))
    cotangent_float = cotangent.astype(jnp.float32)
    residual_slope = cotangent_float + norm_back(normed_slope, middle_gain, middle_normal, middle_inverse)
    branch_slope = residual_slope.astype(jnp.bfloat16)
    mixing_part, joint_slope, layer_output = attend_back(branch_slope, own_output, heads_kept, mixing_slice, attended, log_totals, places, key_last, local_heads, 7)
    shrink_sums, joint_slope = lax.optimization_barrier((shrink_sums, joint_slope))
    joint_part = rep_rows_first(row_outer(entry_all, joint_slope))
    joint_part, joint_slope, expand_sums, mixing_part = lax.optimization_barrier((joint_part, joint_slope, expand_sums, mixing_part))
    joint_sums = rep_sums(joint_part)
    mixing_part = sub_owned(mixing_part, reps)
    joint_sums, mixing_part = lax.optimization_barrier((joint_sums, mixing_part))
    mixing_sums = rep_sums(mixing_part)
    entry_slope, expand_rows = product_reduce(joint_slope.reshape(plane_count, token_rows, 3 * head_columns), joint_every, expand_sums, None, 9)
    own_gradient = (residual_slope + norm_back(entry_slope, entry_gain, entry_normal, entry_inverse)).astype(jnp.bfloat16)
    slope_sums = jnp.sum(joint_slope.astype(jnp.float32), axis=0).reshape(local_heads, 3, head_size)

    def placed(piece, whole_size):
        return lax.dynamic_update_slice_in_dim(jnp.zeros((whole_size,), jnp.float32), piece, plane_index * piece.shape[0], 0)
    small = [jnp.sum(entry_slope * entry_normal, axis=0), jnp.sum(entry_slope, axis=0), placed(slope_sums[:, 0].reshape(-1), width), placed(slope_sums[:, 2].reshape(-1), width), jnp.sum(branch_slope.astype(jnp.float32), axis=0), jnp.sum(normed_slope * middle_normal, axis=0), jnp.sum(normed_slope, axis=0), placed(jnp.sum(expanded_slope.astype(jnp.float32), axis=0), hidden_width), jnp.sum(cotangent_float, axis=0)]
    small_own = jnp.concatenate(small).reshape(-1, 128)
    small_all, input_gradient, joint_rows, shrink_rows = closing(small_own, own_gradient, (joint_sums, shrink_sums), 10)
    shrink_gradient = shrink_rows.astype(jnp.float32)
    expand_gradient = expand_rows.astype(jnp.float32)
    joint_gradient = joint_rows.astype(jnp.float32)
    mixing_gradient = mixing_sums.astype(jnp.float32)
    small_all = small_all.reshape(-1)
    small_sums, first = ([], 0)
    for piece in small:
        small_sums.append(small_all[first:first + piece.shape[0]])
        first += piece.shape[0]
    return (layer_output, input_gradient, small_sums[0], small_sums[1], joint_gradient, small_sums[2], small_sums[3], mixing_gradient, small_sums[4], small_sums[5], small_sums[6], expand_gradient, small_sums[7], shrink_gradient, small_sums[8])

def solution(mesh):
    groups, sequence = (mesh.shape['grp'], mesh.shape['seq'])
    subs = sequence // groups
    planes = Mesh(mesh.devices.reshape(groups, sequence // subs, subs), EVERY)
    rows, whole, group_rows = (P(EVERY, None), P(), P('grp', None))
    return jax.shard_map(shards, mesh=planes, in_specs=(rows, whole, whole, rows, whole, whole, rows, whole, whole, whole, rows, whole, rows) + (whole, group_rows, group_rows, rows), out_specs=(rows, rows, whole, whole, rows, whole, whole, rows, whole, whole, whole, rows, whole) + (rows, whole), check_vma=False)
```

```python
import functools
import jax
import jax.numpy as jnp
from jax import lax
from jax.experimental import pallas as pl
from jax.experimental.pallas import tpu as pltpu
from jax.sharding import Mesh, PartitionSpec as P
HEADS = 16
CONT = 256
PLANE = ('grp', 'sub')
EVERY = ('grp', 'rep', 'sub')
MESH = pl.DeviceIdType.MESH
ANY = pl.BlockSpec(memory_space=pl.ANY)
VMEM = pl.BlockSpec(memory_space=pltpu.VMEM)
DMA = pltpu.SemaphoreType.DMA
MIB = 1 << 20
norm_epsilon = 1e-05
masked_score = -1e+30
log2_e = 1.4426950408889634
root_half = 0.7071067811865476
normal_peak = 0.3989422804014327

def norm_terms(values):
    average = jnp.mean(values, axis=-1, keepdims=True)
    centered = values - average
    variance = jnp.mean(centered * centered, axis=-1, keepdims=True)
    inverse = lax.rsqrt(variance + norm_epsilon)
    return (centered * inverse, inverse)

def norm_back(slope, gain, normal, inverse):
    scaled = slope * gain
    return inverse * (scaled - jnp.mean(scaled, axis=-1, keepdims=True) - normal * jnp.mean(scaled * normal, axis=-1, keepdims=True))

def key_bounds(positions, lengths, prompt):
    segment = (positions - prompt) // CONT
    within = positions - prompt - segment * CONT
    slot_ids = jnp.arange(lengths.shape[0], dtype=jnp.int32)
    slot_limit = jnp.sum(jnp.where(segment[:, None] == slot_ids[None, :], lengths[None, :], 0), axis=1)
    last = prompt + (segment + 1) * CONT - 1
    last = jnp.where(within < slot_limit, last, -1)
    return jnp.where(positions < prompt, positions.shape[0], last)

def product(left_matrix, right_matrix):
    return jnp.dot(left_matrix, right_matrix, preferred_element_type=jnp.float32)

def product_transposed(left_matrix, right_matrix):
    return lax.dot_general(left_matrix, right_matrix, (((1,), (1,)), ((), ())), preferred_element_type=jnp.float32)

def row_outer(left_matrix, right_matrix):
    return lax.dot_general(left_matrix, right_matrix, (((0,), (0,)), ((), ())), preferred_element_type=jnp.float32)

def attention_forward(packed, places, key_last, heads):
    rows, columns = packed.shape
    size = columns // (3 * heads)
    block = 256
    factor = size ** (-0.5) * log2_e

    def kernel(q_ref, k_ref, v_ref, place_ref, first_ref, last_ref, out_ref, total_ref):
        scores = product_transposed(q_ref[...], k_ref[...])
        place = place_ref[...]
        allowed = (first_ref[...] <= place) & (place <= last_ref[...])
        scores = jnp.where(allowed, scores * factor, masked_score)
        top = jnp.max(scores, axis=1, keepdims=True)
        soft = jnp.exp2(scores - top)
        total = jnp.sum(soft, axis=1, keepdims=True)
        mixture = product(soft.astype(jnp.bfloat16), v_ref[...])
        out_ref[...] = (mixture / total).astype(jnp.bfloat16)
        log_total = jnp.broadcast_to(top + jnp.log2(total), (block, 128))
        total_ref[0] = log_total.T[:8]
    return pl.pallas_call(kernel, grid=(heads, rows // block), in_specs=[pl.BlockSpec((block, size), lambda h, i: (i, 3 * h)), pl.BlockSpec((rows, size), lambda h, i: (0, 3 * h + 1)), pl.BlockSpec((rows, size), lambda h, i: (0, 3 * h + 2)), pl.BlockSpec((block, 1), lambda h, i: (i, 0)), pl.BlockSpec((1, rows), lambda h, i: (0, 0)), pl.BlockSpec((1, rows), lambda h, i: (0, 0))], out_specs=[pl.BlockSpec((block, size), lambda h, i: (i, h)), pl.BlockSpec((1, 8, block), lambda h, i: (h, 0, i))], out_shape=[jax.ShapeDtypeStruct((rows, heads * size), jnp.bfloat16), jax.ShapeDtypeStruct((heads, 8, rows), jnp.float32)], compiler_params=pltpu.CompilerParams(vmem_limit_bytes=56 * MIB), cost_estimate=pl.CostEstimate(flops=4 * heads * rows * rows * size, bytes_accessed=4 * rows * heads * size * 2, transcendentals=heads * rows * rows), name='attention_forward')(packed, packed, packed, places[:, None], places[None, :], key_last[None, :])

def attention_backward(packed, totals, slopes, places, key_last, heads):
    rows, columns = packed.shape
    size = columns // (3 * heads)
    block = 256
    scale = size ** (-0.5)
    factor = scale * log2_e

    def kernel(q_ref, k_ref, v_ref, slope_ref, total_ref, place_ref, first_ref, last_ref, out_ref, turned_ref, key_sum, value_sum):
        step = pl.program_id(1)

        @pl.when(step == 0)
        def _():
            turned_ref[...] = k_ref[...].T
            key_sum[...] = jnp.zeros_like(key_sum)
            value_sum[...] = jnp.zeros_like(value_sum)
        queries = q_ref[...]
        slope = slope_ref[...]
        scores = product_transposed(k_ref[...], queries)
        place = place_ref[...]
        allowed = (first_ref[...] <= place) & (place <= last_ref[...])
        soft = jnp.where(allowed, jnp.exp2(scores * factor - total_ref[0, :1]), 0.0)
        weight_slope = product_transposed(v_ref[...], slope)
        centre = jnp.sum(soft * weight_slope, axis=0, keepdims=True)
        score_slope = (soft * (weight_slope - centre)).astype(jnp.bfloat16)
        value_sum[...] += product(soft.astype(jnp.bfloat16), slope)
        key_sum[...] += product(score_slope, queries)
        query_slope = product(turned_ref[...], score_slope)
        here = pl.ds(pl.multiple_of(step * block, block), block)
        out_ref[here, :size] = (query_slope.T * scale).astype(jnp.bfloat16)

        @pl.when(step == pl.num_programs(1) - 1)
        def _():
            out_ref[:, size:2 * size] = (key_sum[...] * scale).astype(jnp.bfloat16)
            out_ref[:, 2 * size:] = value_sum[...].astype(jnp.bfloat16)
    return pl.pallas_call(kernel, grid=(heads, rows // block), in_specs=[pl.BlockSpec((block, size), lambda h, i: (i, 3 * h)), pl.BlockSpec((rows, size), lambda h, i: (0, 3 * h + 1)), pl.BlockSpec((rows, size), lambda h, i: (0, 3 * h + 2)), pl.BlockSpec((block, size), lambda h, i: (i, h)), pl.BlockSpec((1, 8, block), lambda h, i: (h, 0, i)), pl.BlockSpec((1, block), lambda h, i: (0, i)), pl.BlockSpec((rows, 1), lambda h, i: (0, 0)), pl.BlockSpec((rows, 1), lambda h, i: (0, 0))], out_specs=pl.BlockSpec((rows, 3 * size), lambda h, i: (0, h)), out_shape=jax.ShapeDtypeStruct((rows, columns), jnp.bfloat16), scratch_shapes=[pltpu.VMEM((size, rows), jnp.bfloat16), pltpu.VMEM((rows, size), jnp.float32), pltpu.VMEM((rows, size), jnp.float32)], compiler_params=pltpu.CompilerParams(vmem_limit_bytes=56 * MIB), cost_estimate=pl.CostEstimate(flops=10 * heads * rows * rows * size, bytes_accessed=8 * rows * heads * size * 2, transcendentals=heads * rows * rows), name='attention_backward')(packed, packed, packed, slopes, totals, places[None, :], places[:, None], key_last[:, None])

def small_plane():
    return (lax.axis_size('grp'), lax.axis_size('sub')) == (4, 2)

def plane_ids():
    g, r, u = (lax.axis_index(n) for n in ('grp', 'rep', 'sub'))
    y, c = (g // 2, g % 2)
    across, up, partner = ((g, r, 1 - u), ((1 - y) * 2 + c, r, u), (y * 2 + 1 - c, r, u))

    def piece(k):
        above, beside, side = (k // 4, k // 2 % 2, k % 2)
        return ((y + above) % 2 * 2 + (c + beside) % 2) * 2 + (u + side) % 2
    return (across, up, partner, piece)

def greet(devices):
    barrier = pltpu.get_barrier_semaphore()
    for device in devices:
        pl.semaphore_signal(barrier, inc=1, device_id=device, device_id_type=MESH)
    pl.semaphore_wait(barrier, len(devices))

def remote(source, target, send, recv, number, device):
    return pltpu.make_async_remote_copy(src_ref=source, dst_ref=target, send_sem=send.at[number], recv_sem=recv.at[number], device_id=device, device_id_type=MESH)

def plane_peers():
    groups, _, subs = (lax.axis_size(n) for n in EVERY)
    g, r, u = (lax.axis_index(n) for n in EVERY)
    count = groups * subs
    place = g * subs + u
    return (place, [(t // subs, r, lax.rem(t, subs)) for t in (lax.rem(place + step, count) for step in range(1, count))])

def owner_cargo(source, target, send, recv, local):
    count = lax.axis_size('grp') * lax.axis_size('sub')
    subs = lax.axis_size('sub')
    rows, width = (target.shape[0], source.shape[1])
    place, peers = plane_peers()

    def block(t):
        return source.at[pl.ds(pl.multiple_of(t * rows, rows), rows), :]
    landing = target.at[:, pl.ds(pl.multiple_of(place * width, width), width)]
    own = pltpu.make_async_copy(block(place), landing, local)
    away = [remote(block(device[0] * subs + device[2]), landing, send, recv, number, device) for number, device in enumerate(peers)]

    def start():
        own.start()
        for one in away:
            one.start()

    def finish():
        own.wait()
        for one in away:
            one.wait_recv()
        for one in away:
            one.wait_send()
    return (start, finish)

def owner_scratch():
    count = lax.axis_size('grp') * lax.axis_size('sub')
    return [DMA((count - 1,)), DMA((count - 1,)), DMA]

def position_of(turn):
    groups = lax.axis_size('grp')
    return lax.rem(turn, 2) * (groups // 2) + turn // 2

def turn_of(position):
    half = lax.axis_size('grp') // 2
    return lax.rem(position, half) * 2 + position // half

def home_devices():
    g, r, u = (lax.axis_index(n) for n in EVERY)
    groups = lax.axis_size('grp')
    rep = lax.rem(turn_of(g) + groups - r, groups)
    return ((r, rep, u), (position_of(lax.rem(g + r, groups)), g, u), (r == g) & (rep == r))

def column_cargo(source, target, send, recv, local):
    subs = lax.axis_size('sub')
    rows, width = (source.shape[0], target.shape[1])
    place, peers = plane_peers()

    def block(t):
        return source.at[:, pl.ds(pl.multiple_of(t * width, width), width)]
    landing = target.at[pl.ds(pl.multiple_of(place * rows, rows), rows), :]
    own = pltpu.make_async_copy(block(place), landing, local)
    away = [remote(block(device[0] * subs + device[2]), landing, send, recv, number, device) for number, device in enumerate(peers)]

    def start():
        own.start()
        for one in away:
            one.start()

    def finish():
        own.wait()
        for one in away:
            one.wait_recv()
        for one in away:
            one.wait_send()
    return (start, finish)

def column_shape(weight):
    count = lax.axis_size('grp') * lax.axis_size('sub')
    return jax.ShapeDtypeStruct((weight.shape[0] * count, weight.shape[1] // count), weight.dtype)

def row_loads(source, target, sem):
    groups, reps = (lax.axis_size('grp'), lax.axis_size('rep'))
    rows = source.shape[0] // (groups * reps)
    return [pltpu.make_async_copy(source.at[pl.ds((r * groups + g) * rows, rows)], target.at[pl.ds((g * reps + r) * rows, rows)], sem.at[g, r]) for g in range(groups) for r in range(reps)]

def row_loads_scratch(shape, dtype):
    return [pltpu.VMEM(shape, dtype), DMA((lax.axis_size('grp'), lax.axis_size('rep')))]

def home_cargo(source, target, send, recv, local):
    goal, _, stays = home_devices()
    kept = pltpu.make_async_copy(source, target, local)
    moved = pltpu.make_async_remote_copy(src_ref=source, dst_ref=target, send_sem=send, recv_sem=recv, device_id=goal, device_id_type=MESH)

    def start():

        @pl.when(stays)
        def _():
            kept.start()

        @pl.when(jnp.logical_not(stays))
        def _():
            moved.start()

    def finish():

        @pl.when(stays)
        def _():
            kept.wait()

        @pl.when(jnp.logical_not(stays))
        def _():
            moved.wait_recv()
            moved.wait_send()
    return (start, finish)

def greet_all(devices, homes):
    barrier = pltpu.get_barrier_semaphore()
    for device in devices:
        pl.semaphore_signal(barrier, inc=1, device_id=device, device_id_type=MESH)
    if not homes:
        pl.semaphore_wait(barrier, len(devices))
        return
    _, origin, stays = home_devices()

    @pl.when(jnp.logical_not(stays))
    def _():
        pl.semaphore_signal(barrier, inc=1, device_id=origin, device_id_type=MESH)
    pl.semaphore_wait(barrier, len(devices) + 1 - stays.astype(jnp.int32))

def gather_kernel(weights, x_ref, *refs):
    sources, out_ref, landings = (refs[:weights], refs[weights], refs[weights + 1:2 * weights + 1])
    slots, load, send, recv, store, *cargo = refs[2 * weights + 1:]
    ids = plane_ids()
    step = pl.program_id(0)
    cargos = [column_cargo(sources[i], landings[i], *cargo[3 * i:3 * i + 3]) for i in range(weights)]

    @pl.when(step == 0)
    def _():
        first = pltpu.make_async_copy(x_ref, slots.at[0], load)
        first.start()
        greet(plane_peers()[1] if weights else ids[:3])
        first.wait()
    gather_step(step, slots, send, recv, ids)

    def keep(number):
        return pltpu.make_async_copy(slots.at[number], out_ref.at[ids[3](number)], store.at[number])
    keep(gather_order(step)).start()
    if weights:

        @pl.when(step == 2)
        def _():
            for start, _ in cargos:
                start()

    @pl.when(step == 7)
    def _():
        for _, finish in cargos:
            finish()
        for number in range(8):
            keep(number).wait()

def plane_gather(x, weights, collective_id):
    rows, width = x.shape
    if not small_plane():
        return [lax.all_gather(x, PLANE, axis=0, tiled=True)] + [exchange(w, False, collective_id + 20 + i) for i, w in enumerate(weights)]
    number = len(weights)
    every, *columns = pl.pallas_call(functools.partial(gather_kernel, number), grid=(8,), out_shape=[jax.ShapeDtypeStruct((8, rows, width), x.dtype)] + [column_shape(w) for w in weights], in_specs=[ANY] * (1 + number), out_specs=[ANY] * (1 + number), scratch_shapes=[pltpu.VMEM((8, rows, width), x.dtype), DMA, DMA((11,)), DMA((11,)), DMA((8,))] + owner_scratch() * number, compiler_params=remote_params(collective_id, 40), name='plane_gather')(x, *weights)
    return [every.reshape(8 * rows, width)] + columns

def reduce_scratch(rows, width):
    wide, narrow = (jnp.float32, jnp.bfloat16)
    return [pltpu.VMEM((4, rows, width), wide), pltpu.VMEM((4, rows, width), narrow), pltpu.VMEM((4, rows, width), narrow), pltpu.VMEM((3, rows, width), narrow), pltpu.VMEM((3, rows, width), narrow), DMA((10,)), DMA((10,))]

def reduce_order(step):
    return 7 - 2 * step + 7 * (step // 4)

def reduce_step(step, piece, refs, ids, out, before=None):
    sums, give, take, leave, come, send, recv = refs
    across, up, partner, _ = ids
    half = sums.shape[1] // 2
    low, high = (pl.ds(0, half), pl.ds(half, half))
    pair = step // 2

    def to_partner(number):
        return remote(give.at[number], take.at[number], send, recv, number, partner)

    def part(number, which, rows, device):
        return remote(leave.at[which, rows], come.at[which, rows], send, recv, number, device)

    def down(value):
        return value.astype(jnp.bfloat16)

    def up_cast(value):
        return value.astype(jnp.float32)

    @pl.when(lax.rem(step, 2) == 0)
    def _():
        give[pair] = down(piece)
        to_partner(pair).start()

    @pl.when(lax.rem(step, 2) == 1)
    def _():
        sums[pair] = piece
    if before is not None:
        before()

    @pl.when(lax.rem(step, 2) == 1)
    def _():
        to_partner(pair).wait_recv()
        sums[pair] += up_cast(take[pair])
    diagonal_across, diagonal_up = (part(4, 2, low, across), part(5, 2, high, up))
    across_low, up_high = (part(6, 0, low, across), part(7, 1, high, up))
    across_high, up_low = (part(8, 0, high, across), part(9, 1, low, up))

    @pl.when(step == 1)
    def _():
        leave[2] = down(sums[0])
        diagonal_across.start()
        diagonal_up.start()

    @pl.when(step == 3)
    def _():
        leave[0, low] = down(sums[1, low])
        across_low.start()

    @pl.when(step == 5)
    def _():
        leave[1, high] = down(sums[2, high])
        up_high.start()

    @pl.when(step == 7)
    def _():
        diagonal_up.wait_recv()
        leave[0, high] = down(sums[1, high] + up_cast(come[2, high]))
        across_high.start()
        diagonal_across.wait_recv()
        leave[1, low] = down(sums[2, low] + up_cast(come[2, low]))
        up_low.start()
        for one in (across_low, up_high, across_high, up_low):
            one.wait_recv()
        out[...] = sums[3] + up_cast(come[0]) + up_cast(come[1])
        for number in range(4):
            to_partner(number).wait_send()
        for one in (diagonal_across, diagonal_up, across_low, up_high, across_high, up_low):
            one.wait_send()

def product_reduce_kernel(owns, homes, slope_ref, weight_ref, *refs):
    ids = plane_ids()
    step = pl.program_id(0)
    refs = list(refs)
    parcels = [refs.pop(0) for _ in range(owns + homes)]
    out_ref = refs.pop(0)
    landings = [refs.pop(0) for _ in range(owns + homes)]
    slopes, load, weight, weight_load, *refs = refs
    tail = refs[7:]
    rows_in = row_loads(weight_ref, weight, weight_load)
    early, late = ([], [])
    if owns:
        late.append(owner_cargo(parcels[0], landings[0], *tail[:3]))
    if homes:
        early.append(home_cargo(parcels[-1], landings[-1], *tail[-3:]))

    def fetch(number):
        return pltpu.make_async_copy(slope_ref.at[ids[3](number)], slopes.at[number], load.at[number])

    @pl.when(step == 0)
    def _():
        for one in rows_in:
            one.start()
        for number in range(8):
            fetch(reduce_order(number)).start()
        greet_all(plane_peers()[1] if owns else ids[:3], homes)
        for start, _ in early:
            start()
        for one in rows_in:
            one.wait()
    k = reduce_order(step)
    fetch(k).wait()
    reduce_step(step, product_transposed(slopes[k], weight[...]), refs[:7], ids, out_ref)
    if owns:

        @pl.when(step == 5)
        def _():
            for start, _ in late:
                start()
    if owns or homes:

        @pl.when(step == 7)
        def _():
            for _, finish in late + early:
                finish()

def remote_params(collective_id, limit):
    return pltpu.CompilerParams(collective_id=collective_id, has_side_effects=True, vmem_limit_bytes=limit * MIB)

def owner_shape(parcel):
    count = lax.axis_size('grp') * lax.axis_size('sub')
    return jax.ShapeDtypeStruct((parcel.shape[0] // count, parcel.shape[1] * count), parcel.dtype)

def product_reduce(slopes, weight, owned, homed, collective_id):
    count, rows, inner = slopes.shape
    width = weight.shape[0]
    owns, homes = (owned is not None, homed is not None)
    if not small_plane():
        part = product_transposed(slopes.reshape(-1, inner), rep_rows_last(weight))
        whole = [lax.psum_scatter(part.astype(jnp.bfloat16), PLANE, scatter_dimension=0, tiled=True).astype(jnp.float32)]
        return whole + ([exchange(owned, True, collective_id)] if owns else []) + ([from_plane(homed)] if homes else [])
    cargo = ([owned] if owns else []) + ([homed] if homes else [])
    shapes = ([owner_shape(owned)] if owns else []) + ([jax.ShapeDtypeStruct(homed.shape, homed.dtype)] if homes else [])
    return pl.pallas_call(functools.partial(product_reduce_kernel, owns, homes), grid=(8,), out_shape=[jax.ShapeDtypeStruct((rows, width), jnp.float32)] + shapes, in_specs=[ANY, ANY] + [ANY] * len(cargo), out_specs=[VMEM] + [ANY] * len(cargo), scratch_shapes=[pltpu.VMEM((8, rows, inner), slopes.dtype), DMA((8,)), *row_loads_scratch(weight.shape, weight.dtype), *reduce_scratch(rows, width)] + (owner_scratch() if owns else []) + ([DMA, DMA, DMA] if homes else []), compiler_params=remote_params(collective_id, 60), name='product_reduce')(slopes, weight, *cargo)

def closing_kernel(number, x_ref, homed_ref, *refs):
    owned_refs, (out_ref, homed_out), owned_outs = (refs[:number], refs[number:number + 2], refs[number + 2:2 * number + 2])
    refs = refs[2 * number + 2:]
    here = {n: lax.axis_index(n) for n in EVERY}
    phases = ('grp', 'sub', 'rep')
    home_start, home_finish = home_cargo(homed_ref, homed_out, *refs[:3])
    owners = [owner_cargo(owned_refs[i], owned_outs[i], *refs[3 + 3 * i:6 + 3 * i]) for i in range(number)]
    refs = refs[3 + 3 * number:]

    def other(name, step):
        size = lax.axis_size(name)
        return tuple((lax.rem(here[n] + step, size) if n == name else here[n] for n in EVERY))
    greet_all(plane_peers()[1] + [other('rep', s) for s in range(1, lax.axis_size('rep'))], True)
    home_start()
    out_ref[...] = x_ref[...]
    for j, name in enumerate(phases):
        slots, send, recv = refs[3 * j:3 * j + 3]
        size = lax.axis_size(name)
        me = here[name]
        slots[me] = out_ref[...]
        copies = []
        for s in range(1, size):
            one = pltpu.make_async_remote_copy(src_ref=out_ref, dst_ref=slots.at[me], send_sem=send.at[s], recv_sem=recv.at[s], device_id=other(name, s), device_id_type=MESH)
            one.start()
            copies.append(one)
        if name == 'rep':
            for start, _ in owners:
                start()
        for one in copies:
            one.wait_recv()
        for one in copies:
            one.wait_send()
        value = slots[0]
        for s in range(1, size):
            value = value + slots[s]
        out_ref[...] = value
    for _, finish in owners:
        finish()
    home_finish()

def closing(x, homed, owned, collective_id):
    scratch = []
    for name in ('grp', 'sub', 'rep'):
        n = lax.axis_size(name)
        scratch += [pltpu.VMEM((n,) + x.shape, x.dtype), DMA((n,)), DMA((n,))]
    number = len(owned)
    return pl.pallas_call(functools.partial(closing_kernel, number), out_shape=[jax.ShapeDtypeStruct(x.shape, x.dtype), jax.ShapeDtypeStruct(homed.shape, homed.dtype)] + [owner_shape(one) for one in owned], in_specs=[VMEM] + [ANY] * (1 + number), out_specs=[VMEM] + [ANY] * (1 + number), scratch_shapes=[DMA, DMA, DMA] + owner_scratch() * number + scratch, compiler_params=pltpu.CompilerParams(collective_id=collective_id, has_side_effects=True), name='closing')(x, homed, *owned)

def exchange_kernel(to_tokens, x_ref, out_ref, send, recv, local):
    groups, reps, subs = (lax.axis_size(n) for n in EVERY)
    g, r, u = (lax.axis_index(n) for n in EVERY)
    count = groups * subs
    place = g * subs + u
    if to_tokens:
        tokens, width = (out_ref.shape[0], x_ref.shape[1])
    else:
        tokens, width = (x_ref.shape[0], out_ref.shape[1])

    def rows(ref, t):
        return ref.at[pl.ds(pl.multiple_of(t * tokens, tokens), tokens), :]

    def columns(ref, t):
        return ref.at[:, pl.ds(pl.multiple_of(t * width, width), width)]
    source, target = (rows, columns) if to_tokens else (columns, rows)
    peers = [lax.rem(place + step, count) for step in range(1, count)]

    def device(t):
        return (t // subs, r, lax.rem(t, subs))
    own = pltpu.make_async_copy(source(x_ref, place), target(out_ref, place), local)
    own.start()
    greet([device(t) for t in peers])
    copies = []
    for step, t in enumerate(peers):
        one = pltpu.make_async_remote_copy(src_ref=source(x_ref, t), dst_ref=target(out_ref, place), send_sem=send.at[step], recv_sem=recv.at[step], device_id=device(t), device_id_type=MESH)
        one.start()
        copies.append(one)
    own.wait()
    for one in copies:
        one.wait_recv()
    for one in copies:
        one.wait_send()

def exchange(x, to_tokens, collective_id):
    count = lax.axis_size('grp') * lax.axis_size('sub')
    shape = (x.shape[0] // count, x.shape[1] * count) if to_tokens else (x.shape[0] * count, x.shape[1] // count)
    return pl.pallas_call(functools.partial(exchange_kernel, to_tokens), out_shape=jax.ShapeDtypeStruct(shape, x.dtype), in_specs=[ANY], out_specs=ANY, scratch_shapes=[DMA((count - 1,)), DMA((count - 1,)), DMA], compiler_params=pltpu.CompilerParams(collective_id=collective_id, has_side_effects=True), name='to_tokens' if to_tokens else 'to_heads')(x)

def opening_kernel(x_ref, *refs):
    weights = (len(refs) - 8) // 2
    sources, (moved_ref, *landings) = (refs[:weights], refs[weights:2 * weights + 1])
    transit, move_send, move_recv, move_local, send, recv, local = refs[2 * weights + 1:]
    groups, _, subs = (lax.axis_size(n) for n in EVERY)
    g, r, u = (lax.axis_index(n) for n in EVERY)
    place, peers = plane_peers()
    relay = position_of(lax.rem(g + r, groups))
    beyond = lax.rem(turn_of(g) + groups - r, groups)

    def block(number, t):
        width = landings[number].shape[1]
        return sources[number].at[:, pl.ds(pl.multiple_of(t * width, width), width)]

    def landing(number):
        rows = sources[number].shape[0]
        return landings[number].at[pl.ds(pl.multiple_of(place * rows, rows), rows), :]

    def hop(number, source, target, device, stays):
        kept = pltpu.make_async_copy(source, target, move_local.at[number])
        moved = remote(source, target, move_send, move_recv, number, device)

        def start():

            @pl.when(stays)
            def _():
                kept.start()

            @pl.when(jnp.logical_not(stays))
            def _():
                moved.start()

        def arrive():

            @pl.when(stays)
            def _():
                kept.wait()

            @pl.when(jnp.logical_not(stays))
            def _():
                moved.wait_recv()

        def leave():

            @pl.when(jnp.logical_not(stays))
            def _():
                moved.wait_send()
        return (start, arrive, leave)
    first = hop(0, x_ref, transit, (relay, r, u), relay == g)
    second = hop(1, transit, moved_ref, (g, beyond, u), beyond == r)
    owns = [pltpu.make_async_copy(block(number, place), landing(number), local.at[number]) for number in range(weights)]
    for one in owns:
        one.start()
    barrier = pltpu.get_barrier_semaphore()
    for device in peers:
        pl.semaphore_signal(barrier, inc=1, device_id=device, device_id_type=MESH)

    @pl.when(beyond != r)
    def _():
        pl.semaphore_signal(barrier, inc=1, device_id=(g, beyond, u), device_id_type=MESH)
    pl.semaphore_wait(barrier, len(peers) + (beyond != r).astype(jnp.int32))
    first[0]()
    copies = []
    for number in range(weights):
        for step, device in enumerate(peers):
            one = pltpu.make_async_remote_copy(src_ref=block(number, device[0] * subs + device[2]), dst_ref=landing(number), send_sem=send.at[number, step], recv_sem=recv.at[number, step], device_id=device, device_id_type=MESH)
            one.start()
            copies.append(one)
    first[1]()
    second[0]()
    for one in owns:
        one.wait()
    for one in copies:
        one.wait_recv()
    for one in copies:
        one.wait_send()
    first[2]()
    second[1]()
    second[2]()

def opening(x, weights, collective_id):
    count = lax.axis_size('grp') * lax.axis_size('sub')
    number = len(weights)
    columns = [jax.ShapeDtypeStruct((w.shape[0] * count, w.shape[1] // count), w.dtype) for w in weights]
    return pl.pallas_call(opening_kernel, out_shape=[jax.ShapeDtypeStruct(x.shape, x.dtype), *columns], in_specs=[VMEM] + [ANY] * number, out_specs=[VMEM] + [ANY] * number, scratch_shapes=[pltpu.VMEM(x.shape, x.dtype), DMA((2,)), DMA((2,)), DMA((2,)), DMA((number, count - 1)), DMA((number, count - 1)), DMA((number,))], compiler_params=pltpu.CompilerParams(collective_id=collective_id, has_side_effects=True), name='opening')(x, *weights)

def attend_kernel(heads, head_ref, place_ref, first_ref, last_ref, mixing_ref, attended_ref, total_ref, out_ref, *refs):
    ids = plane_ids()
    step = pl.program_id(0)

    @pl.when(step == 0)
    def _():
        greet(ids[:3])
    rows = out_ref.shape[0]
    size = attended_ref.shape[1] // heads
    factor = size ** (-0.5) * log2_e
    first_row = pl.multiple_of(ids[3](reduce_order(step)) * rows, rows)
    here = pl.ds(first_row, rows)
    place = place_ref[here, :]
    allowed = (first_ref[...] <= place) & (place <= last_ref[...])
    for h in range(heads):
        q, k, v = (3 * h + j for j in range(3))
        scores = product_transposed(head_ref[here, q * size:(q + 1) * size], head_ref[:, k * size:(k + 1) * size])
        scores = jnp.where(allowed, scores * factor, masked_score)
        top = jnp.max(scores, axis=1, keepdims=True)
        soft = jnp.exp2(scores - top)
        total = jnp.sum(soft, axis=1, keepdims=True)
        mixture = product(soft.astype(jnp.bfloat16), head_ref[:, v * size:(v + 1) * size])
        attended_ref[here, h * size:(h + 1) * size] = (mixture / total).astype(jnp.bfloat16)
        log_total = jnp.broadcast_to(top + jnp.log2(total), (rows, 128))
        total_ref[h, :, here] = log_total.T[:8]
    reduce_step(step, product(attended_ref[here, :], mixing_ref[...]), refs, ids, out_ref)

def attend(packed, places, key_last, mixing, heads, token_rows, collective_id):
    rows = packed.shape[0]
    inner, width = mixing.shape
    if not small_plane():
        attended, totals = attention_forward(packed, places, key_last, heads)
        part = product(attended, mixing).astype(jnp.bfloat16)
        return (attended, totals, lax.psum_scatter(part, PLANE, scatter_dimension=0, tiled=True).astype(jnp.float32))
    return pl.pallas_call(functools.partial(attend_kernel, heads), grid=(8,), out_shape=[jax.ShapeDtypeStruct((rows, inner), jnp.bfloat16), jax.ShapeDtypeStruct((heads, 8, rows), jnp.float32), jax.ShapeDtypeStruct((token_rows, width), jnp.float32)], in_specs=[VMEM] * 5, out_specs=[VMEM] * 3, scratch_shapes=reduce_scratch(token_rows, width), compiler_params=remote_params(collective_id, 60), name='attend')(packed, places[:, None], places[None, :], key_last[None, :], mixing)

def gather_order(step):
    return step + 2 * (step % 2) - 1 + (8 - step) // 8 - step // 7

def gather_step(step, slots, send, recv, ids):
    across, up, partner, _ = ids
    half = slots.shape[1] // 2
    low, high = (pl.ds(0, half), pl.ds(half, half))

    def copy(number, source, target, device):
        return remote(slots.at[source], slots.at[target], send, recv, number, device)
    across_low = copy(0, (0, low), (1, low), across)
    up_high = copy(1, (0, high), (4, high), up)
    across_high = copy(2, (0, high), (1, high), across)
    up_low = copy(3, (0, low), (4, low), up)
    own = copy(4, 0, 2, partner)
    far_low = copy(5, (1, low), (5, low), up)
    far_high = copy(6, (4, high), (5, high), across)
    pass_across = copy(7, 1, 3, partner)
    pass_up = copy(8, 4, 6, partner)
    pass_low = copy(9, (5, low), (7, low), partner)
    pass_high = copy(10, (5, high), (7, high), partner)

    @pl.when(step == 0)
    def _():
        for one in (across_low, up_high, own, across_high, up_low):
            one.start()

    @pl.when(step == 1)
    def _():
        own.wait_recv()

    @pl.when(step == 2)
    def _():
        across_low.wait_recv()
        far_low.start()
        up_high.wait_recv()
        far_high.start()
        across_high.wait_recv()
        pass_across.start()

    @pl.when(step == 3)
    def _():
        up_low.wait_recv()
        pass_up.start()

    @pl.when(step == 4)
    def _():
        pass_across.wait_recv()

    @pl.when(step == 5)
    def _():
        pass_up.wait_recv()

    @pl.when(step == 6)
    def _():
        far_low.wait_recv()
        pass_low.start()
        far_high.wait_recv()
        pass_high.start()

    @pl.when(step == 7)
    def _():
        pass_low.wait_recv()
        pass_high.wait_recv()
        for one in (across_low, up_high, across_high, up_low, own, far_low, far_high, pass_across, pass_up, pass_low, pass_high):
            one.wait_send()

def attend_back_kernel(heads, branch_ref, homed_ref, head_ref, mixing_ref, attended_ref, total_ref, place_ref, first_ref, last_ref, part_ref, out_ref, homed_out, sums_ref, turned, key_sum, value_sum, part_sum, slots, load, send, recv, *cargo):
    ids = plane_ids()
    step = pl.program_id(0)
    home_start, home_finish = home_cargo(homed_ref, homed_out, *cargo)
    rows = slots.shape[1]
    size = head_ref.shape[1] // (3 * heads)
    scale = size ** (-0.5)
    factor = scale * log2_e

    @pl.when(step == 0)
    def _():
        first = pltpu.make_async_copy(branch_ref, slots.at[0], load)
        first.start()
        for h in range(heads):
            turned[h] = head_ref[:, (3 * h + 1) * size:(3 * h + 2) * size].T
        key_sum[...] = jnp.zeros_like(key_sum)
        value_sum[...] = jnp.zeros_like(value_sum)
        part_sum[...] = jnp.zeros_like(part_sum)
        sums_ref[...] = jnp.zeros_like(sums_ref)
        greet_all(ids[:3], True)
        home_start()
        first.wait()
    gather_step(step, slots, send, recv, ids)
    k = gather_order(step)
    here = pl.ds(pl.multiple_of(ids[3](k) * rows, rows), rows)
    part_sum[...] += row_outer(attended_ref[here, :], slots[k])
    slopes = product_transposed(slots[k], mixing_ref[...]).astype(jnp.bfloat16)
    place = place_ref[:, here]
    allowed = (first_ref[...] <= place) & (place <= last_ref[...])
    for h in range(heads):
        queries = head_ref[here, 3 * h * size:(3 * h + 1) * size]
        keys = head_ref[:, (3 * h + 1) * size:(3 * h + 2) * size]
        values = head_ref[:, (3 * h + 2) * size:(3 * h + 3) * size]
        slope = slopes[:, h * size:(h + 1) * size]
        scores = product_transposed(keys, queries)
        soft = jnp.where(allowed, jnp.exp2(scores * factor - total_ref[h, :1, here]), 0.0)
        weight_slope = product_transposed(values, slope)
        centre = jnp.sum(soft * weight_slope, axis=0, keepdims=True)
        score_slope = (soft * (weight_slope - centre)).astype(jnp.bfloat16)
        value_sum[h] += product(soft.astype(jnp.bfloat16), slope)
        key_sum[h] += product(score_slope, queries)
        query_slope = product(turned[h], score_slope)
        query_slope = (query_slope.T * scale).astype(jnp.bfloat16)
        out_ref[here, 3 * h * size:(3 * h + 1) * size] = query_slope
        sums_ref[:, 3 * h * size:(3 * h + 1) * size] += jnp.sum(query_slope.astype(jnp.float32), axis=0, keepdims=True)

    @pl.when(step == 7)
    def _():
        for h in range(heads):
            out_ref[:, (3 * h + 1) * size:(3 * h + 2) * size] = (key_sum[h] * scale).astype(jnp.bfloat16)
            value_slope = value_sum[h].astype(jnp.bfloat16)
            out_ref[:, (3 * h + 2) * size:(3 * h + 3) * size] = value_slope
            sums_ref[:, (3 * h + 2) * size:(3 * h + 3) * size] = jnp.sum(value_slope.astype(jnp.float32), axis=0, keepdims=True)
        part_ref[...] = part_sum[...].astype(jnp.bfloat16)
        home_finish()

def attend_back(branch_slope, homed, packed, mixing, attended, totals, places, key_last, heads, collective_id):
    rows, columns = packed.shape
    token_rows, width = branch_slope.shape
    size = columns // (3 * heads)
    if not small_plane():
        every = lax.all_gather(branch_slope, PLANE, axis=0, tiled=True)
        slopes = product_transposed(every, mixing).astype(jnp.bfloat16)
        part = row_outer(attended, every).astype(jnp.bfloat16)
        slopes = attention_backward(packed, totals, slopes, places, key_last, heads)
        return (part, slopes, from_plane(homed), jnp.sum(slopes.astype(jnp.float32), axis=0, keepdims=True))
    return pl.pallas_call(functools.partial(attend_back_kernel, heads), grid=(8,), out_shape=[jax.ShapeDtypeStruct(mixing.shape, jnp.bfloat16), jax.ShapeDtypeStruct((rows, columns), jnp.bfloat16), jax.ShapeDtypeStruct(homed.shape, homed.dtype), jax.ShapeDtypeStruct((1, columns), jnp.float32)], in_specs=[ANY] * 2 + [VMEM] * 7, out_specs=[VMEM, VMEM, ANY, VMEM], scratch_shapes=[pltpu.VMEM((heads, size, rows), jnp.bfloat16), pltpu.VMEM((heads, rows, size), jnp.float32), pltpu.VMEM((heads, rows, size), jnp.float32), pltpu.VMEM(mixing.shape, jnp.float32), pltpu.VMEM((8, token_rows, width), jnp.bfloat16), DMA, DMA((11,)), DMA((11,)), DMA, DMA, DMA], compiler_params=remote_params(collective_id, 62), name='attend_back')(branch_slope, homed, packed, mixing, attended, totals, places[None, :], places[:, None], key_last[:, None])

def add_outer(total, left, right):
    turned = left.T
    for first in range(0, total.shape[1], 256):
        here = pl.ds(first, 256)
        total[:, here] += product(turned, right[:, first:first + 256])

def rep_order(total, narrow, part_ref, sem):
    groups, reps = (lax.axis_size('grp'), lax.axis_size('rep'))
    rows = total.shape[0] // (groups * reps)
    for g in range(groups):
        for r in range(reps):
            come, go = (pl.ds((g * reps + r) * rows, rows), pl.ds((r * groups + g) * rows, rows))
            narrow[come, :] = total[come, :].astype(jnp.bfloat16)
            pltpu.make_async_copy(narrow.at[come], part_ref.at[go], sem.at[g, r]).start()

def rep_order_wait(narrow, part_ref, sem):
    groups, reps = (lax.axis_size('grp'), lax.axis_size('rep'))
    rows = narrow.shape[0] // (groups * reps)
    for g in range(groups):
        for r in range(reps):
            come, go = (pl.ds((g * reps + r) * rows, rows), pl.ds((r * groups + g) * rows, rows))
            pltpu.make_async_copy(narrow.at[come], part_ref.at[go], sem.at[g, r]).wait()

def hidden_kernel(middle_ref, cotangent_ref, expand_ref, offset_ref, every_ref, active_ref, rise_ref, part_ref, slots, cotangents, actives, rises, total, load, send, recv, store, fetch_cotangent, active_store, rise_store, expand, expand_load, narrow, part_store):
    ids = plane_ids()
    step = pl.program_id(0)
    turn = lax.rem(step, 2)

    def fetch(number, side):
        return pltpu.make_async_copy(cotangent_ref.at[ids[3](gather_order(number))], cotangents.at[side], fetch_cotangent.at[side])

    @pl.when(step == 0)
    def _():
        first = pltpu.make_async_copy(middle_ref, slots.at[0], load)
        first.start()
        rows_in = row_loads(expand_ref, expand, expand_load)
        for one in rows_in:
            one.start()
        fetch(0, 0).start()
        total[...] = jnp.zeros_like(total)
        greet(ids[:3])
        first.wait()
        for one in rows_in:
            one.wait()
    gather_step(step, slots, send, recv, ids)
    k = gather_order(step)

    def keep(number):
        return pltpu.make_async_copy(slots.at[number], every_ref.at[ids[3](number)], store.at[number])

    def put(number, side):
        piece = ids[3](number)
        return (pltpu.make_async_copy(actives.at[side], active_ref.at[piece], active_store.at[side]), pltpu.make_async_copy(rises.at[side], rise_ref.at[piece], rise_store.at[side]))
    keep(k).start()

    @pl.when(step >= 2)
    def _():
        for one in put(k, turn):
            one.wait()
    expanded = product(slots[k], expand[...]) + offset_ref[...]
    below = 0.5 * (1.0 + lax.erf(expanded * root_half))
    actives[turn] = (expanded * below).astype(jnp.bfloat16)
    rises[turn] = below + expanded * (jnp.exp(-0.5 * expanded * expanded) * normal_peak)
    for one in put(k, turn):
        one.start()
    fetch(step, turn).wait()

    @pl.when(step < 7)
    def _():
        fetch(step + 1, 1 - turn).start()
    add_outer(total, cotangents[turn], actives[turn])

    @pl.when(step == 7)
    def _():
        rep_order(total, narrow, part_ref, part_store)
        for late in range(2):
            for one in put(k, late):
                one.wait()
        for number in range(8):
            keep(number).wait()
        rep_order_wait(narrow, part_ref, part_store)

def hidden(middle, cotangent_all, expand_slice, offset, collective_id):
    rows, width = middle.shape
    count = lax.axis_size('grp') * lax.axis_size('sub')
    inner = expand_slice.shape[1]
    if not small_plane():
        every = lax.all_gather(middle, PLANE, axis=0, tiled=True)
        expanded = product(every, rep_rows_last(expand_slice)) + offset
        below = 0.5 * (1.0 + lax.erf(expanded * root_half))
        rise = below + expanded * (jnp.exp(-0.5 * expanded * expanded) * normal_peak)
        active = (expanded * below).astype(jnp.bfloat16)
        return (every, active, rise, rep_rows_first(row_outer(cotangent_all, active)))
    every, active, rise, part = pl.pallas_call(hidden_kernel, grid=(8,), out_shape=[jax.ShapeDtypeStruct((8, rows, width), middle.dtype), jax.ShapeDtypeStruct((8, rows, inner), jnp.bfloat16), jax.ShapeDtypeStruct((8, rows, inner), jnp.float32), jax.ShapeDtypeStruct((width, inner), jnp.bfloat16)], in_specs=[ANY, ANY, ANY, VMEM], out_specs=[ANY] * 4, scratch_shapes=[pltpu.VMEM((8, rows, width), middle.dtype), pltpu.VMEM((2, rows, width), jnp.bfloat16), pltpu.VMEM((2, rows, inner), jnp.bfloat16), pltpu.VMEM((2, rows, inner), jnp.float32), pltpu.VMEM((width, inner), jnp.float32), DMA, DMA((11,)), DMA((11,)), DMA((8,)), DMA((2,)), DMA((2,)), DMA((2,)), *row_loads_scratch(expand_slice.shape, expand_slice.dtype), *row_loads_scratch(expand_slice.shape, jnp.bfloat16)], compiler_params=remote_params(collective_id, 60), name='hidden')(middle, cotangent_all.reshape(8, rows, width), expand_slice, offset[None, :])
    return (every.reshape(count * rows, width), active.reshape(count * rows, inner), rise.reshape(count * rows, inner), part)

def hidden_back_kernel(cotangent_ref, middle_ref, rise_ref, shrink_ref, expand_ref, slope_ref, out_ref, part_ref, sums_ref, cotangents, middles, rises, slopes, total, fetches, store, shrink, shrink_load, expand, expand_load, narrow, part_store, *refs):
    ids = plane_ids()
    step = pl.program_id(0)

    def fetch(number, side):
        piece = ids[3](reduce_order(number))
        return [pltpu.make_async_copy(source.at[piece], target.at[side], fetches.at[kind, side]) for kind, (source, target) in enumerate(((cotangent_ref, cotangents), (rise_ref, rises), (middle_ref, middles)))]

    def put(number, side):
        return pltpu.make_async_copy(slopes.at[side], slope_ref.at[ids[3](reduce_order(number))], store.at[side])
    turn = lax.rem(step, 2)

    @pl.when(step == 0)
    def _():
        rows_in = row_loads(shrink_ref, shrink, shrink_load) + row_loads(expand_ref, expand, expand_load)
        for one in rows_in:
            one.start()
        for one in fetch(0, 0):
            one.start()
        total[...] = jnp.zeros_like(total)
        sums_ref[...] = jnp.zeros_like(sums_ref)
        greet(ids[:3])
        for one in rows_in:
            one.wait()
    for one in fetch(step, turn):
        one.wait()

    @pl.when(step < 7)
    def _():
        for one in fetch(step + 1, 1 - turn):
            one.start()

    @pl.when(step >= 2)
    def _():
        put(step, turn).wait()
    slope = product(cotangents[turn], shrink[...]) * rises[turn]
    slopes[turn] = slope.astype(jnp.bfloat16)
    put(step, turn).start()

    def before():
        add_outer(total, middles[turn], slopes[turn])
        sums_ref[...] += jnp.sum(slopes[turn].astype(jnp.float32), axis=0, keepdims=True)

        @pl.when(step == 7)
        def _():
            rep_order(total, narrow, part_ref, part_store)
    reduce_step(step, product_transposed(slopes[turn], expand[...]), refs, ids, out_ref, before)

    @pl.when(step == 7)
    def _():
        put(6, 0).wait()
        put(7, 1).wait()
        rep_order_wait(narrow, part_ref, part_store)

def hidden_back(cotangent_all, middle_all, rise, shrink_slice, expand_slice, token_rows, collective_id):
    rows, width = cotangent_all.shape
    inner = shrink_slice.shape[1]
    if not small_plane():
        slope = (product(cotangent_all, rep_rows_last(shrink_slice)) * rise).astype(jnp.bfloat16)
        part = product_transposed(slope, rep_rows_last(expand_slice)).astype(jnp.bfloat16)
        normed = lax.psum_scatter(part, PLANE, scatter_dimension=0, tiled=True).astype(jnp.float32)
        sums = jnp.sum(slope.astype(jnp.float32), axis=0)
        return (slope, normed, rep_rows_first(row_outer(middle_all, slope)), sums)
    pieces = (8, token_rows, width)
    slope, normed, part, sums = pl.pallas_call(hidden_back_kernel, grid=(8,), out_shape=[jax.ShapeDtypeStruct((8, token_rows, inner), jnp.bfloat16), jax.ShapeDtypeStruct((token_rows, width), jnp.float32), jax.ShapeDtypeStruct((width, inner), jnp.bfloat16), jax.ShapeDtypeStruct((1, inner), jnp.float32)], in_specs=[ANY] * 5, out_specs=[ANY, VMEM, ANY, VMEM], scratch_shapes=[pltpu.VMEM((2, token_rows, width), jnp.bfloat16), pltpu.VMEM((2, token_rows, width), jnp.bfloat16), pltpu.VMEM((2, token_rows, inner), jnp.float32), pltpu.VMEM((2, token_rows, inner), jnp.bfloat16), pltpu.VMEM((width, inner), jnp.float32), DMA((3, 2)), DMA((2,)), *row_loads_scratch(shrink_slice.shape, shrink_slice.dtype), *row_loads_scratch(expand_slice.shape, expand_slice.dtype), *row_loads_scratch(expand_slice.shape, jnp.bfloat16), *reduce_scratch(token_rows, width)], compiler_params=remote_params(collective_id, 63), name='hidden_back')(cotangent_all.reshape(pieces), middle_all.reshape(pieces), rise.reshape(8, token_rows, inner), shrink_slice, expand_slice)
    return (slope.reshape(rows, inner), normed, part, sums[0])

def plane_moves():
    groups, reps, subs = (lax.axis_size(n) for n in EVERY)
    moves = []
    for g in range(groups):
        for r in range(reps):
            turn = (g + r) % groups
            position = turn % 2 * (groups // 2) + turn // 2
            for u in range(subs):
                moves.append(tuple(((a * reps + b) * subs + u for a, b in ((g, r), (position, r), (position, g)))))
    return moves

def to_door(array):
    return lax.ppermute(array, EVERY, [(home, door) for home, door, _ in plane_moves()])

def to_keeper(array):
    return lax.ppermute(array, EVERY, [(door, away) for _, door, away in plane_moves()])

def to_plane_at_once(array):
    return lax.ppermute(array, EVERY, [(home, away) for home, _, away in plane_moves()])

def from_plane(array):
    return lax.ppermute(array, EVERY, [(away, home) for home, _, away in plane_moves()])

def plane_order(places):
    groups = lax.axis_size('grp')
    blocks = jnp.roll(places.reshape(groups, -1), lax.axis_index('rep'), axis=0)
    return blocks.reshape(groups // 2, 2, -1).transpose(1, 0, 2).reshape(-1)

def rep_rows(own):
    return lax.all_gather(own, 'rep', axis=0, tiled=True)

def rep_rows_last(every):
    groups, reps, subs = (lax.axis_size(name) for name in EVERY)
    columns = every.shape[1]
    ordered = every.reshape(reps, groups, subs, -1, columns).transpose(1, 0, 2, 3, 4)
    return ordered.reshape(-1, columns)

def rep_rows_first(gradient):
    groups, reps, subs = (lax.axis_size(name) for name in EVERY)
    columns = gradient.shape[1]
    ordered = gradient.astype(jnp.bfloat16).reshape(groups, reps, subs, -1, columns)
    return ordered.transpose(1, 0, 2, 3, 4).reshape(-1, columns)

def rep_sums(ordered):
    return lax.psum_scatter(ordered, 'rep', scatter_dimension=0, tiled=True)

def sub_turn(block):
    groups, reps, subs = (lax.axis_size(name) for name in EVERY)
    low = reps // subs
    moves = [((g * reps + r) * subs + u, (g * reps + u * low + r % low) * subs + r // low) for g in range(groups) for r in range(reps) for u in range(subs)]
    return lax.ppermute(block, EVERY, moves)

def sub_rows(own):
    rows, width = own.shape
    reps, subs = (lax.axis_size('rep'), lax.axis_size('sub'))
    shares = own.reshape(subs, reps // subs, -1, width)
    if subs != 2:
        every = lax.all_to_all(shares, 'sub', split_axis=0, concat_axis=0, tiled=True)
        return every.transpose(1, 0, 2, 3).reshape(rows, width)
    me = lax.axis_index('sub')
    kept = jnp.where(me == 0, shares[0], shares[1])
    come = lax.ppermute(jnp.where(me == 0, shares[1], shares[0]), 'sub', [(0, 1), (1, 0)])
    first, second = (jnp.where(me == 0, kept, come), jnp.where(me == 0, come, kept))
    return jnp.stack([first, second], axis=1).reshape(rows, width)

def mixing_sums_of(part):
    reps, subs = (lax.axis_size('rep'), lax.axis_size('sub'))
    rows, width = part.shape
    ordered = part.reshape(reps // subs, subs, rows // reps, width).transpose(1, 0, 2, 3)
    return lax.psum_scatter(ordered.reshape(rows, width), 'rep', scatter_dimension=0, tiled=True)

def sub_owned(part, reps):
    rows, width = part.shape
    subs = lax.axis_size('sub')
    shares = part.reshape(reps // subs, subs, -1, width).transpose(1, 0, 2, 3)
    if subs != 2:
        every = lax.all_to_all(shares, 'sub', split_axis=0, concat_axis=0, tiled=True)
        return every.reshape(rows, width)
    me = lax.axis_index('sub')
    kept = jnp.where(me == 0, shares[0], shares[1])
    come = lax.ppermute(jnp.where(me == 0, shares[1], shares[0]), 'sub', [(0, 1), (1, 0)])
    first, second = (jnp.where(me == 0, kept, come), jnp.where(me == 0, come, kept))
    return jnp.concatenate([first, second], axis=0).reshape(rows, width)

def shards(layer_input, entry_gain, entry_shift, joint_weight, query_offset, value_offset, mixing_weight, attention_offset, middle_gain, middle_shift, expand_weight, expand_offset, shrink_weight, shrink_offset, placement, slot_lengths, cotangent):
    token_rows, width = layer_input.shape
    hidden_width = expand_weight.shape[1]
    groups, reps, subs = (lax.axis_size(name) for name in EVERY)
    plane_count = groups * subs
    plane_index = lax.axis_index(PLANE)
    head_size = width // HEADS
    local_heads = HEADS // plane_count
    head_columns = local_heads * head_size
    plane_rows = plane_count * token_rows
    facts = to_plane_at_once(jnp.concatenate([placement, slot_lengths], axis=1))[0]
    mixing_own = rep_rows(mixing_weight)
    moved_input, joint_own, expand_own = opening(layer_input, (joint_weight, expand_weight), 12)
    joint_own, mixing_own = lax.optimization_barrier((joint_own, mixing_own))
    input_float = moved_input.astype(jnp.float32)
    joint_every = rep_rows(joint_own)
    entry_normal, entry_inverse = norm_terms(input_float)
    entry_normed = (entry_normal * entry_gain + entry_shift).astype(jnp.bfloat16)
    entry_all, shrink_own = plane_gather(entry_normed, (shrink_weight,), 1)
    cotangent, facts, entry_all = lax.optimization_barrier((cotangent, facts, entry_all))
    cotangent = to_door(cotangent)
    places = plane_order(facts[:placement.shape[1]])
    lengths = facts[placement.shape[1]:]
    prompt = places.shape[0] // 2
    key_last = key_bounds(places, lengths, prompt)
    expand_slice = rep_rows(expand_own)
    shrink_slice = rep_rows(shrink_own)
    cotangent = to_keeper(cotangent)
    mixing_slice = sub_rows(mixing_own)
    offsets = jnp.stack([query_offset.reshape(HEADS, head_size), jnp.zeros((HEADS, head_size), jnp.float32), value_offset.reshape(HEADS, head_size)], axis=1).reshape(-1)
    offsets = lax.dynamic_slice_in_dim(offsets, plane_index * 3 * head_columns, 3 * head_columns)
    heads_kept = (product(entry_all, rep_rows_last(joint_every)) + offsets).astype(jnp.bfloat16)
    attended, log_totals, branch = attend(heads_kept, places, key_last, mixing_slice, local_heads, token_rows, 3)
    residual = input_float + (branch + attention_offset)
    middle_normal, middle_inverse = norm_terms(residual)
    middle_normed = (middle_normal * middle_gain + middle_shift).astype(jnp.bfloat16)
    cotangent, middle_normed = lax.optimization_barrier((cotangent, middle_normed))
    cotangent_all, = plane_gather(cotangent, (), 4)
    middle_normed, cotangent_all = lax.optimization_barrier((middle_normed, cotangent_all))
    hidden_local = hidden_width // plane_count
    offset_local = lax.dynamic_slice_in_dim(expand_offset, plane_index * hidden_local, hidden_local)
    middle_all, activated, rise, shrink_part = hidden(middle_normed, cotangent_all, expand_slice, offset_local, 5)
    shrink_sums = rep_sums(shrink_part)
    expanded_slope, normed_slope, expand_part, expanded_sums = hidden_back(cotangent_all, middle_all, rise, shrink_slice, expand_slice, token_rows, 6)
    expand_sums = rep_sums(expand_part)
    activated, normed_slope = lax.optimization_barrier((activated, normed_slope))
    shrunk, = product_reduce(activated.reshape(plane_count, token_rows, hidden_local), shrink_slice, None, None, 8)
    own_output = (residual + shrunk + shrink_offset).astype(jnp.bfloat16)
    own_output, normed_slope = lax.optimization_barrier((own_output, normed_slope))
    cotangent_float = cotangent.astype(jnp.float32)
    residual_slope = cotangent_float + norm_back(normed_slope, middle_gain, middle_normal, middle_inverse)
    branch_slope = residual_slope.astype(jnp.bfloat16)
    mixing_part, joint_slope, layer_output, slope_sums = attend_back(branch_slope, own_output, heads_kept, mixing_slice, attended, log_totals, places, key_last, local_heads, 7)
    shrink_sums, joint_slope = lax.optimization_barrier((shrink_sums, joint_slope))
    joint_part = rep_rows_first(row_outer(entry_all, joint_slope))
    joint_part, joint_slope, expand_sums, mixing_part = lax.optimization_barrier((joint_part, joint_slope, expand_sums, mixing_part))
    joint_sums = rep_sums(joint_part)
    mixing_part = sub_owned(mixing_part, reps)
    joint_sums, mixing_part = lax.optimization_barrier((joint_sums, mixing_part))
    mixing_sums = rep_sums(mixing_part)
    entry_slope, expand_rows = product_reduce(joint_slope.reshape(plane_count, token_rows, 3 * head_columns), joint_every, expand_sums, None, 9)
    own_gradient = (residual_slope + norm_back(entry_slope, entry_gain, entry_normal, entry_inverse)).astype(jnp.bfloat16)
    slope_sums = slope_sums.reshape(local_heads, 3, head_size)

    def placed(piece, whole_size):
        return lax.dynamic_update_slice_in_dim(jnp.zeros((whole_size,), jnp.float32), piece, plane_index * piece.shape[0], 0)
    small = [jnp.sum(entry_slope * entry_normal, axis=0), jnp.sum(entry_slope, axis=0), placed(slope_sums[:, 0].reshape(-1), width), placed(slope_sums[:, 2].reshape(-1), width), jnp.sum(branch_slope.astype(jnp.float32), axis=0), jnp.sum(normed_slope * middle_normal, axis=0), jnp.sum(normed_slope, axis=0), placed(expanded_sums, hidden_width), jnp.sum(cotangent_float, axis=0)]
    small_own = jnp.concatenate(small).reshape(-1, 128)
    small_all, input_gradient, joint_rows, shrink_rows = closing(small_own, own_gradient, (joint_sums, shrink_sums), 10)
    shrink_gradient = shrink_rows.astype(jnp.float32)
    expand_gradient = expand_rows.astype(jnp.float32)
    joint_gradient = joint_rows.astype(jnp.float32)
    mixing_gradient = mixing_sums.astype(jnp.float32)
    small_all = small_all.reshape(-1)
    small_sums, first = ([], 0)
    for piece in small:
        small_sums.append(small_all[first:first + piece.shape[0]])
        first += piece.shape[0]
    return (layer_output, input_gradient, small_sums[0], small_sums[1], joint_gradient, small_sums[2], small_sums[3], mixing_gradient, small_sums[4], small_sums[5], small_sums[6], expand_gradient, small_sums[7], shrink_gradient, small_sums[8])

def solution(mesh):
    groups, sequence = (mesh.shape['grp'], mesh.shape['seq'])
    subs = sequence // groups
    planes = Mesh(mesh.devices.reshape(groups, sequence // subs, subs), EVERY)
    rows, whole, group_rows = (P(EVERY, None), P(), P('grp', None))
    return jax.shard_map(shards, mesh=planes, in_specs=(rows, whole, whole, rows, whole, whole, rows, whole, whole, whole, rows, whole, rows) + (whole, group_rows, group_rows, rows), out_specs=(rows, rows, whole, whole, rows, whole, whole, rows, whole, whole, whole, rows, whole) + (rows, whole), check_vma=False)
```

```python
import functools
import jax
import jax.numpy as jnp
from jax import lax
from jax.experimental import pallas as pl
from jax.experimental.pallas import tpu as pltpu
from jax.sharding import Mesh, PartitionSpec as P
HEADS = 16
CONT = 256
PLANE = ('grp', 'sub')
EVERY = ('grp', 'rep', 'sub')
MESH = pl.DeviceIdType.MESH
ANY = pl.BlockSpec(memory_space=pl.ANY)
VMEM = pl.BlockSpec(memory_space=pltpu.VMEM)
DMA = pltpu.SemaphoreType.DMA
MIB = 1 << 20
norm_epsilon = 1e-05
masked_score = -1e+30
log2_e = 1.4426950408889634
root_half = 0.7071067811865476
normal_peak = 0.3989422804014327

def norm_terms(values):
    average = jnp.mean(values, axis=-1, keepdims=True)
    centered = values - average
    variance = jnp.mean(centered * centered, axis=-1, keepdims=True)
    inverse = lax.rsqrt(variance + norm_epsilon)
    return (centered * inverse, inverse)

def norm_back(slope, gain, normal, inverse):
    scaled = slope * gain
    return inverse * (scaled - jnp.mean(scaled, axis=-1, keepdims=True) - normal * jnp.mean(scaled * normal, axis=-1, keepdims=True))

def key_bounds(positions, lengths, prompt):
    segment = (positions - prompt) // CONT
    within = positions - prompt - segment * CONT
    slot_ids = jnp.arange(lengths.shape[0], dtype=jnp.int32)
    slot_limit = jnp.sum(jnp.where(segment[:, None] == slot_ids[None, :], lengths[None, :], 0), axis=1)
    last = prompt + (segment + 1) * CONT - 1
    last = jnp.where(within < slot_limit, last, -1)
    return jnp.where(positions < prompt, positions.shape[0], last)

def product(left_matrix, right_matrix):
    return jnp.dot(left_matrix, right_matrix, preferred_element_type=jnp.float32)

def product_transposed(left_matrix, right_matrix):
    return lax.dot_general(left_matrix, right_matrix, (((1,), (1,)), ((), ())), preferred_element_type=jnp.float32)

def row_outer(left_matrix, right_matrix):
    return lax.dot_general(left_matrix, right_matrix, (((0,), (0,)), ((), ())), preferred_element_type=jnp.float32)

def attention_forward(packed, places, key_last, heads):
    rows, columns = packed.shape
    size = columns // (3 * heads)
    block = 256
    factor = size ** (-0.5) * log2_e

    def kernel(q_ref, k_ref, v_ref, place_ref, first_ref, last_ref, out_ref, total_ref):
        scores = product_transposed(q_ref[...], k_ref[...])
        place = place_ref[...]
        allowed = (first_ref[...] <= place) & (place <= last_ref[...])
        scores = jnp.where(allowed, scores * factor, masked_score)
        top = jnp.max(scores, axis=1, keepdims=True)
        soft = jnp.exp2(scores - top)
        total = jnp.sum(soft, axis=1, keepdims=True)
        mixture = product(soft.astype(jnp.bfloat16), v_ref[...])
        out_ref[...] = (mixture / total).astype(jnp.bfloat16)
        log_total = jnp.broadcast_to(top + jnp.log2(total), (block, 128))
        total_ref[0] = log_total.T[:8]
    return pl.pallas_call(kernel, grid=(heads, rows // block), in_specs=[pl.BlockSpec((block, size), lambda h, i: (i, 3 * h)), pl.BlockSpec((rows, size), lambda h, i: (0, 3 * h + 1)), pl.BlockSpec((rows, size), lambda h, i: (0, 3 * h + 2)), pl.BlockSpec((block, 1), lambda h, i: (i, 0)), pl.BlockSpec((1, rows), lambda h, i: (0, 0)), pl.BlockSpec((1, rows), lambda h, i: (0, 0))], out_specs=[pl.BlockSpec((block, size), lambda h, i: (i, h)), pl.BlockSpec((1, 8, block), lambda h, i: (h, 0, i))], out_shape=[jax.ShapeDtypeStruct((rows, heads * size), jnp.bfloat16), jax.ShapeDtypeStruct((heads, 8, rows), jnp.float32)], compiler_params=pltpu.CompilerParams(vmem_limit_bytes=56 * MIB), cost_estimate=pl.CostEstimate(flops=4 * heads * rows * rows * size, bytes_accessed=4 * rows * heads * size * 2, transcendentals=heads * rows * rows), name='attention_forward')(packed, packed, packed, places[:, None], places[None, :], key_last[None, :])

def attention_backward(packed, totals, slopes, places, key_last, heads):
    rows, columns = packed.shape
    size = columns // (3 * heads)
    block = 256
    scale = size ** (-0.5)
    factor = scale * log2_e

    def kernel(q_ref, k_ref, v_ref, slope_ref, total_ref, place_ref, first_ref, last_ref, out_ref, turned_ref, key_sum, value_sum):
        step = pl.program_id(1)

        @pl.when(step == 0)
        def _():
            turned_ref[...] = k_ref[...].T
            key_sum[...] = jnp.zeros_like(key_sum)
            value_sum[...] = jnp.zeros_like(value_sum)
        queries = q_ref[...]
        slope = slope_ref[...]
        scores = product_transposed(k_ref[...], queries)
        place = place_ref[...]
        allowed = (first_ref[...] <= place) & (place <= last_ref[...])
        soft = jnp.where(allowed, jnp.exp2(scores * factor - total_ref[0, :1]), 0.0)
        weight_slope = product_transposed(v_ref[...], slope)
        centre = jnp.sum(soft * weight_slope, axis=0, keepdims=True)
        score_slope = (soft * (weight_slope - centre)).astype(jnp.bfloat16)
        value_sum[...] += product(soft.astype(jnp.bfloat16), slope)
        key_sum[...] += product(score_slope, queries)
        query_slope = product(turned_ref[...], score_slope)
        here = pl.ds(pl.multiple_of(step * block, block), block)
        out_ref[here, :size] = (query_slope.T * scale).astype(jnp.bfloat16)

        @pl.when(step == pl.num_programs(1) - 1)
        def _():
            out_ref[:, size:2 * size] = (key_sum[...] * scale).astype(jnp.bfloat16)
            out_ref[:, 2 * size:] = value_sum[...].astype(jnp.bfloat16)
    return pl.pallas_call(kernel, grid=(heads, rows // block), in_specs=[pl.BlockSpec((block, size), lambda h, i: (i, 3 * h)), pl.BlockSpec((rows, size), lambda h, i: (0, 3 * h + 1)), pl.BlockSpec((rows, size), lambda h, i: (0, 3 * h + 2)), pl.BlockSpec((block, size), lambda h, i: (i, h)), pl.BlockSpec((1, 8, block), lambda h, i: (h, 0, i)), pl.BlockSpec((1, block), lambda h, i: (0, i)), pl.BlockSpec((rows, 1), lambda h, i: (0, 0)), pl.BlockSpec((rows, 1), lambda h, i: (0, 0))], out_specs=pl.BlockSpec((rows, 3 * size), lambda h, i: (0, h)), out_shape=jax.ShapeDtypeStruct((rows, columns), jnp.bfloat16), scratch_shapes=[pltpu.VMEM((size, rows), jnp.bfloat16), pltpu.VMEM((rows, size), jnp.float32), pltpu.VMEM((rows, size), jnp.float32)], compiler_params=pltpu.CompilerParams(vmem_limit_bytes=56 * MIB), cost_estimate=pl.CostEstimate(flops=10 * heads * rows * rows * size, bytes_accessed=8 * rows * heads * size * 2, transcendentals=heads * rows * rows), name='attention_backward')(packed, packed, packed, slopes, totals, places[None, :], places[:, None], key_last[:, None])

def small_plane():
    return (lax.axis_size('grp'), lax.axis_size('sub')) == (4, 2)

def plane_ids():
    g, r, u = (lax.axis_index(n) for n in ('grp', 'rep', 'sub'))
    y, c = (g // 2, g % 2)
    across, up, partner = ((g, r, 1 - u), ((1 - y) * 2 + c, r, u), (y * 2 + 1 - c, r, u))

    def piece(k):
        above, beside, side = (k // 4, k // 2 % 2, k % 2)
        return ((y + above) % 2 * 2 + (c + beside) % 2) * 2 + (u + side) % 2
    return (across, up, partner, piece)

def greet(devices):
    barrier = pltpu.get_barrier_semaphore()
    for device in devices:
        pl.semaphore_signal(barrier, inc=1, device_id=device, device_id_type=MESH)
    pl.semaphore_wait(barrier, len(devices))

def remote(source, target, send, recv, number, device):
    return pltpu.make_async_remote_copy(src_ref=source, dst_ref=target, send_sem=send.at[number], recv_sem=recv.at[number], device_id=device, device_id_type=MESH)

def plane_peers():
    groups, _, subs = (lax.axis_size(n) for n in EVERY)
    g, r, u = (lax.axis_index(n) for n in EVERY)
    count = groups * subs
    place = g * subs + u
    return (place, [(t // subs, r, lax.rem(t, subs)) for t in (lax.rem(place + step, count) for step in range(1, count))])

def owner_cargo(source, target, send, recv, local):
    count = lax.axis_size('grp') * lax.axis_size('sub')
    subs = lax.axis_size('sub')
    rows, width = (target.shape[0], source.shape[1])
    place, peers = plane_peers()

    def block(t):
        return source.at[pl.ds(pl.multiple_of(t * rows, rows), rows), :]
    landing = target.at[:, pl.ds(pl.multiple_of(place * width, width), width)]
    own = pltpu.make_async_copy(block(place), landing, local)
    away = [remote(block(device[0] * subs + device[2]), landing, send, recv, number, device) for number, device in enumerate(peers)]

    def start():
        own.start()
        for one in away:
            one.start()

    def finish():
        own.wait()
        for one in away:
            one.wait_recv()
        for one in away:
            one.wait_send()
    return (start, finish)

def owner_scratch():
    count = lax.axis_size('grp') * lax.axis_size('sub')
    return [DMA((count - 1,)), DMA((count - 1,)), DMA]

def position_of(turn):
    groups = lax.axis_size('grp')
    return lax.rem(turn, 2) * (groups // 2) + turn // 2

def turn_of(position):
    half = lax.axis_size('grp') // 2
    return lax.rem(position, half) * 2 + position // half

def home_devices():
    g, r, u = (lax.axis_index(n) for n in EVERY)
    groups = lax.axis_size('grp')
    rep = lax.rem(turn_of(g) + groups - r, groups)
    return ((r, rep, u), (position_of(lax.rem(g + r, groups)), g, u), (r == g) & (rep == r))

def column_cargo(source, target, send, recv, local):
    subs = lax.axis_size('sub')
    rows, width = (source.shape[0], target.shape[1])
    place, peers = plane_peers()

    def block(t):
        return source.at[:, pl.ds(pl.multiple_of(t * width, width), width)]
    landing = target.at[pl.ds(pl.multiple_of(place * rows, rows), rows), :]
    own = pltpu.make_async_copy(block(place), landing, local)
    away = [remote(block(device[0] * subs + device[2]), landing, send, recv, number, device) for number, device in enumerate(peers)]

    def start():
        own.start()
        for one in away:
            one.start()

    def finish():
        own.wait()
        for one in away:
            one.wait_recv()
        for one in away:
            one.wait_send()
    return (start, finish)

def column_shape(weight):
    count = lax.axis_size('grp') * lax.axis_size('sub')
    return jax.ShapeDtypeStruct((weight.shape[0] * count, weight.shape[1] // count), weight.dtype)

def row_loads(source, target, sem):
    groups, reps = (lax.axis_size('grp'), lax.axis_size('rep'))
    rows = source.shape[0] // (groups * reps)
    return [pltpu.make_async_copy(source.at[pl.ds((r * groups + g) * rows, rows)], target.at[pl.ds((g * reps + r) * rows, rows)], sem.at[g, r]) for g in range(groups) for r in range(reps)]

def row_loads_scratch(shape, dtype):
    return [pltpu.VMEM(shape, dtype), DMA((lax.axis_size('grp'), lax.axis_size('rep')))]

def home_cargo(source, target, send, recv, local):
    goal, _, stays = home_devices()
    kept = pltpu.make_async_copy(source, target, local)
    moved = pltpu.make_async_remote_copy(src_ref=source, dst_ref=target, send_sem=send, recv_sem=recv, device_id=goal, device_id_type=MESH)

    def start():

        @pl.when(stays)
        def _():
            kept.start()

        @pl.when(jnp.logical_not(stays))
        def _():
            moved.start()

    def finish():

        @pl.when(stays)
        def _():
            kept.wait()

        @pl.when(jnp.logical_not(stays))
        def _():
            moved.wait_recv()
            moved.wait_send()
    return (start, finish)

def greet_all(devices, homes):
    barrier = pltpu.get_barrier_semaphore()
    for device in devices:
        pl.semaphore_signal(barrier, inc=1, device_id=device, device_id_type=MESH)
    if not homes:
        pl.semaphore_wait(barrier, len(devices))
        return
    _, origin, stays = home_devices()

    @pl.when(jnp.logical_not(stays))
    def _():
        pl.semaphore_signal(barrier, inc=1, device_id=origin, device_id_type=MESH)
    pl.semaphore_wait(barrier, len(devices) + 1 - stays.astype(jnp.int32))

def gather_kernel(weights, x_ref, *refs):
    sources, out_ref, landings = (refs[:weights], refs[weights], refs[weights + 1:2 * weights + 1])
    slots, load, send, recv, store, *cargo = refs[2 * weights + 1:]
    ids = plane_ids()
    step = pl.program_id(0)
    cargos = [column_cargo(sources[i], landings[i], *cargo[3 * i:3 * i + 3]) for i in range(weights)]

    @pl.when(step == 0)
    def _():
        first = pltpu.make_async_copy(x_ref, slots.at[0], load)
        first.start()
        greet(plane_peers()[1] if weights else ids[:3])
        first.wait()
    gather_step(step, slots, send, recv, ids)

    def keep(number):
        return pltpu.make_async_copy(slots.at[number], out_ref.at[ids[3](number)], store.at[number])
    keep(gather_order(step)).start()
    if weights:

        @pl.when(step == 2)
        def _():
            for start, _ in cargos:
                start()

    @pl.when(step == 7)
    def _():
        for _, finish in cargos:
            finish()
        for number in range(8):
            keep(number).wait()

def plane_gather(x, weights, collective_id):
    rows, width = x.shape
    if not small_plane():
        return [lax.all_gather(x, PLANE, axis=0, tiled=True)] + [exchange(w, False, collective_id + 20 + i) for i, w in enumerate(weights)]
    number = len(weights)
    every, *columns = pl.pallas_call(functools.partial(gather_kernel, number), grid=(8,), out_shape=[jax.ShapeDtypeStruct((8, rows, width), x.dtype)] + [column_shape(w) for w in weights], in_specs=[ANY] * (1 + number), out_specs=[ANY] * (1 + number), scratch_shapes=[pltpu.VMEM((8, rows, width), x.dtype), DMA, DMA((11,)), DMA((11,)), DMA((8,))] + owner_scratch() * number, compiler_params=remote_params(collective_id, 40), name='plane_gather')(x, *weights)
    return [every.reshape(8 * rows, width)] + columns

def reduce_scratch(rows, width):
    wide, narrow = (jnp.float32, jnp.bfloat16)
    return [pltpu.VMEM((4, rows, width), wide), pltpu.VMEM((4, rows, width), narrow), pltpu.VMEM((4, rows, width), narrow), pltpu.VMEM((3, rows, width), narrow), pltpu.VMEM((3, rows, width), narrow), DMA((10,)), DMA((10,))]

def reduce_order(step):
    return 7 - 2 * step + 7 * (step // 4)

def reduce_step(step, piece, refs, ids, out, before=None):
    sums, give, take, leave, come, send, recv = refs
    across, up, partner, _ = ids
    half = sums.shape[1] // 2
    low, high = (pl.ds(0, half), pl.ds(half, half))
    pair = step // 2

    def to_partner(number):
        return remote(give.at[number], take.at[number], send, recv, number, partner)

    def part(number, which, rows, device):
        return remote(leave.at[which, rows], come.at[which, rows], send, recv, number, device)

    def down(value):
        return value.astype(jnp.bfloat16)

    def up_cast(value):
        return value.astype(jnp.float32)

    @pl.when(lax.rem(step, 2) == 0)
    def _():
        give[pair] = down(piece)
        to_partner(pair).start()

    @pl.when(lax.rem(step, 2) == 1)
    def _():
        sums[pair] = piece
    if before is not None:
        before()

    @pl.when(lax.rem(step, 2) == 1)
    def _():
        to_partner(pair).wait_recv()
        sums[pair] += up_cast(take[pair])
    diagonal_across, diagonal_up = (part(4, 2, low, across), part(5, 2, high, up))
    across_low, up_high = (part(6, 0, low, across), part(7, 1, high, up))
    across_high, up_low = (part(8, 0, high, across), part(9, 1, low, up))

    @pl.when(step == 1)
    def _():
        leave[2] = down(sums[0])
        diagonal_across.start()
        diagonal_up.start()

    @pl.when(step == 3)
    def _():
        leave[0, low] = down(sums[1, low])
        across_low.start()

    @pl.when(step == 5)
    def _():
        leave[1, high] = down(sums[2, high])
        up_high.start()

    @pl.when(step == 7)
    def _():
        diagonal_up.wait_recv()
        leave[0, high] = down(sums[1, high] + up_cast(come[2, high]))
        across_high.start()
        diagonal_across.wait_recv()
        leave[1, low] = down(sums[2, low] + up_cast(come[2, low]))
        up_low.start()
        for one in (across_low, up_high, across_high, up_low):
            one.wait_recv()
        out[...] = sums[3] + up_cast(come[0]) + up_cast(come[1])
        for number in range(4):
            to_partner(number).wait_send()
        for one in (diagonal_across, diagonal_up, across_low, up_high, across_high, up_low):
            one.wait_send()

def product_reduce_kernel(owns, homes, slope_ref, weight_ref, *refs):
    ids = plane_ids()
    step = pl.program_id(0)
    refs = list(refs)
    parcels = [refs.pop(0) for _ in range(owns + homes)]
    out_ref = refs.pop(0)
    landings = [refs.pop(0) for _ in range(owns + homes)]
    slopes, load, weight, weight_load, *refs = refs
    tail = refs[7:]
    rows_in = row_loads(weight_ref, weight, weight_load)
    early, late = ([], [])
    if owns:
        late.append(owner_cargo(parcels[0], landings[0], *tail[:3]))
    if homes:
        early.append(home_cargo(parcels[-1], landings[-1], *tail[-3:]))

    def fetch(number):
        return pltpu.make_async_copy(slope_ref.at[ids[3](number)], slopes.at[number], load.at[number])

    @pl.when(step == 0)
    def _():
        for one in rows_in:
            one.start()
        for number in range(8):
            fetch(reduce_order(number)).start()
        greet_all(plane_peers()[1] if owns else ids[:3], homes)
        for start, _ in early:
            start()
        for one in rows_in:
            one.wait()
    k = reduce_order(step)
    fetch(k).wait()
    reduce_step(step, product_transposed(slopes[k], weight[...]), refs[:7], ids, out_ref)
    if owns:

        @pl.when(step == 5)
        def _():
            for start, _ in late:
                start()
    if owns or homes:

        @pl.when(step == 7)
        def _():
            for _, finish in late + early:
                finish()

def remote_params(collective_id, limit):
    return pltpu.CompilerParams(collective_id=collective_id, has_side_effects=True, vmem_limit_bytes=limit * MIB)

def owner_shape(parcel):
    count = lax.axis_size('grp') * lax.axis_size('sub')
    return jax.ShapeDtypeStruct((parcel.shape[0] // count, parcel.shape[1] * count), parcel.dtype)

def product_reduce(slopes, weight, owned, homed, collective_id):
    count, rows, inner = slopes.shape
    width = weight.shape[0]
    owns, homes = (owned is not None, homed is not None)
    if not small_plane():
        part = product_transposed(slopes.reshape(-1, inner), rep_rows_last(weight))
        whole = [lax.psum_scatter(part.astype(jnp.bfloat16), PLANE, scatter_dimension=0, tiled=True).astype(jnp.float32)]
        return whole + ([exchange(owned, True, collective_id)] if owns else []) + ([from_plane(homed)] if homes else [])
    cargo = ([owned] if owns else []) + ([homed] if homes else [])
    shapes = ([owner_shape(owned)] if owns else []) + ([jax.ShapeDtypeStruct(homed.shape, homed.dtype)] if homes else [])
    return pl.pallas_call(functools.partial(product_reduce_kernel, owns, homes), grid=(8,), out_shape=[jax.ShapeDtypeStruct((rows, width), jnp.float32)] + shapes, in_specs=[ANY, ANY] + [ANY] * len(cargo), out_specs=[VMEM] + [ANY] * len(cargo), scratch_shapes=[pltpu.VMEM((8, rows, inner), slopes.dtype), DMA((8,)), *row_loads_scratch(weight.shape, weight.dtype), *reduce_scratch(rows, width)] + (owner_scratch() if owns else []) + ([DMA, DMA, DMA] if homes else []), compiler_params=remote_params(collective_id, 60), name='product_reduce')(slopes, weight, *cargo)

def closing_kernel(number, x_ref, homed_ref, *refs):
    owned_refs, (out_ref, homed_out), owned_outs = (refs[:number], refs[number:number + 2], refs[number + 2:2 * number + 2])
    refs = refs[2 * number + 2:]
    here = {n: lax.axis_index(n) for n in EVERY}
    phases = ('grp', 'sub', 'rep')
    home_start, home_finish = home_cargo(homed_ref, homed_out, *refs[:3])
    owners = [owner_cargo(owned_refs[i], owned_outs[i], *refs[3 + 3 * i:6 + 3 * i]) for i in range(number)]
    refs = refs[3 + 3 * number:]

    def other(name, step):
        size = lax.axis_size(name)
        return tuple((lax.rem(here[n] + step, size) if n == name else here[n] for n in EVERY))
    greet_all(plane_peers()[1] + [other('rep', s) for s in range(1, lax.axis_size('rep'))], True)
    home_start()
    out_ref[...] = x_ref[...]
    for j, name in enumerate(phases):
        slots, send, recv = refs[3 * j:3 * j + 3]
        size = lax.axis_size(name)
        me = here[name]
        slots[me] = out_ref[...]
        copies = []
        for s in range(1, size):
            one = pltpu.make_async_remote_copy(src_ref=out_ref, dst_ref=slots.at[me], send_sem=send.at[s], recv_sem=recv.at[s], device_id=other(name, s), device_id_type=MESH)
            one.start()
            copies.append(one)
        if j == 0:
            for start, _ in owners:
                start()
        for one in copies:
            one.wait_recv()
        for one in copies:
            one.wait_send()
        value = slots[0]
        for s in range(1, size):
            value = value + slots[s]
        out_ref[...] = value
    for _, finish in owners:
        finish()
    home_finish()

def closing(x, homed, owned, collective_id):
    scratch = []
    for name in ('grp', 'sub', 'rep'):
        n = lax.axis_size(name)
        scratch += [pltpu.VMEM((n,) + x.shape, x.dtype), DMA((n,)), DMA((n,))]
    number = len(owned)
    return pl.pallas_call(functools.partial(closing_kernel, number), out_shape=[jax.ShapeDtypeStruct(x.shape, x.dtype), jax.ShapeDtypeStruct(homed.shape, homed.dtype)] + [owner_shape(one) for one in owned], in_specs=[VMEM] + [ANY] * (1 + number), out_specs=[VMEM] + [ANY] * (1 + number), scratch_shapes=[DMA, DMA, DMA] + owner_scratch() * number + scratch, compiler_params=pltpu.CompilerParams(collective_id=collective_id, has_side_effects=True), name='closing')(x, homed, *owned)

def exchange_kernel(to_tokens, x_ref, out_ref, send, recv, local):
    groups, reps, subs = (lax.axis_size(n) for n in EVERY)
    g, r, u = (lax.axis_index(n) for n in EVERY)
    count = groups * subs
    place = g * subs + u
    if to_tokens:
        tokens, width = (out_ref.shape[0], x_ref.shape[1])
    else:
        tokens, width = (x_ref.shape[0], out_ref.shape[1])

    def rows(ref, t):
        return ref.at[pl.ds(pl.multiple_of(t * tokens, tokens), tokens), :]

    def columns(ref, t):
        return ref.at[:, pl.ds(pl.multiple_of(t * width, width), width)]
    source, target = (rows, columns) if to_tokens else (columns, rows)
    peers = [lax.rem(place + step, count) for step in range(1, count)]

    def device(t):
        return (t // subs, r, lax.rem(t, subs))
    own = pltpu.make_async_copy(source(x_ref, place), target(out_ref, place), local)
    own.start()
    greet([device(t) for t in peers])
    copies = []
    for step, t in enumerate(peers):
        one = pltpu.make_async_remote_copy(src_ref=source(x_ref, t), dst_ref=target(out_ref, place), send_sem=send.at[step], recv_sem=recv.at[step], device_id=device(t), device_id_type=MESH)
        one.start()
        copies.append(one)
    own.wait()
    for one in copies:
        one.wait_recv()
    for one in copies:
        one.wait_send()

def exchange(x, to_tokens, collective_id):
    count = lax.axis_size('grp') * lax.axis_size('sub')
    shape = (x.shape[0] // count, x.shape[1] * count) if to_tokens else (x.shape[0] * count, x.shape[1] // count)
    return pl.pallas_call(functools.partial(exchange_kernel, to_tokens), out_shape=jax.ShapeDtypeStruct(shape, x.dtype), in_specs=[ANY], out_specs=ANY, scratch_shapes=[DMA((count - 1,)), DMA((count - 1,)), DMA], compiler_params=pltpu.CompilerParams(collective_id=collective_id, has_side_effects=True), name='to_tokens' if to_tokens else 'to_heads')(x)

def opening_kernel(x_ref, *refs):
    weights = (len(refs) - 8) // 2
    sources, (moved_ref, *landings) = (refs[:weights], refs[weights:2 * weights + 1])
    transit, move_send, move_recv, move_local, send, recv, local = refs[2 * weights + 1:]
    groups, _, subs = (lax.axis_size(n) for n in EVERY)
    g, r, u = (lax.axis_index(n) for n in EVERY)
    place, peers = plane_peers()
    relay = position_of(lax.rem(g + r, groups))
    beyond = lax.rem(turn_of(g) + groups - r, groups)

    def block(number, t):
        width = landings[number].shape[1]
        return sources[number].at[:, pl.ds(pl.multiple_of(t * width, width), width)]

    def landing(number):
        rows = sources[number].shape[0]
        return landings[number].at[pl.ds(pl.multiple_of(place * rows, rows), rows), :]

    def hop(number, source, target, device, stays):
        kept = pltpu.make_async_copy(source, target, move_local.at[number])
        moved = remote(source, target, move_send, move_recv, number, device)

        def start():

            @pl.when(stays)
            def _():
                kept.start()

            @pl.when(jnp.logical_not(stays))
            def _():
                moved.start()

        def arrive():

            @pl.when(stays)
            def _():
                kept.wait()

            @pl.when(jnp.logical_not(stays))
            def _():
                moved.wait_recv()

        def leave():

            @pl.when(jnp.logical_not(stays))
            def _():
                moved.wait_send()
        return (start, arrive, leave)
    first = hop(0, x_ref, transit, (relay, r, u), relay == g)
    second = hop(1, transit, moved_ref, (g, beyond, u), beyond == r)
    owns = [pltpu.make_async_copy(block(number, place), landing(number), local.at[number]) for number in range(weights)]
    for one in owns:
        one.start()
    barrier = pltpu.get_barrier_semaphore()
    for device in peers:
        pl.semaphore_signal(barrier, inc=1, device_id=device, device_id_type=MESH)

    @pl.when(beyond != r)
    def _():
        pl.semaphore_signal(barrier, inc=1, device_id=(g, beyond, u), device_id_type=MESH)
    pl.semaphore_wait(barrier, len(peers) + (beyond != r).astype(jnp.int32))
    first[0]()
    copies = []
    for number in range(weights):
        for step, device in enumerate(peers):
            one = pltpu.make_async_remote_copy(src_ref=block(number, device[0] * subs + device[2]), dst_ref=landing(number), send_sem=send.at[number, step], recv_sem=recv.at[number, step], device_id=device, device_id_type=MESH)
            one.start()
            copies.append(one)
    first[1]()
    second[0]()
    for one in owns:
        one.wait()
    for one in copies:
        one.wait_recv()
    for one in copies:
        one.wait_send()
    first[2]()
    second[1]()
    second[2]()

def opening(x, weights, collective_id):
    count = lax.axis_size('grp') * lax.axis_size('sub')
    number = len(weights)
    columns = [jax.ShapeDtypeStruct((w.shape[0] * count, w.shape[1] // count), w.dtype) for w in weights]
    return pl.pallas_call(opening_kernel, out_shape=[jax.ShapeDtypeStruct(x.shape, x.dtype), *columns], in_specs=[VMEM] + [ANY] * number, out_specs=[VMEM] + [ANY] * number, scratch_shapes=[pltpu.VMEM(x.shape, x.dtype), DMA((2,)), DMA((2,)), DMA((2,)), DMA((number, count - 1)), DMA((number, count - 1)), DMA((number,))], compiler_params=pltpu.CompilerParams(collective_id=collective_id, has_side_effects=True), name='opening')(x, *weights)

def attend_kernel(heads, head_ref, place_ref, first_ref, last_ref, mixing_ref, attended_ref, total_ref, out_ref, *refs):
    ids = plane_ids()
    step = pl.program_id(0)

    @pl.when(step == 0)
    def _():
        greet(ids[:3])
    rows = out_ref.shape[0]
    size = attended_ref.shape[1] // heads
    factor = size ** (-0.5) * log2_e
    first_row = pl.multiple_of(ids[3](reduce_order(step)) * rows, rows)
    here = pl.ds(first_row, rows)
    place = place_ref[here, :]
    allowed = (first_ref[...] <= place) & (place <= last_ref[...])
    for h in range(heads):
        q, k, v = (3 * h + j for j in range(3))
        scores = product_transposed(head_ref[here, q * size:(q + 1) * size], head_ref[:, k * size:(k + 1) * size])
        scores = jnp.where(allowed, scores * factor, masked_score)
        top = jnp.max(scores, axis=1, keepdims=True)
        soft = jnp.exp2(scores - top)
        total = jnp.sum(soft, axis=1, keepdims=True)
        mixture = product(soft.astype(jnp.bfloat16), head_ref[:, v * size:(v + 1) * size])
        attended_ref[here, h * size:(h + 1) * size] = (mixture / total).astype(jnp.bfloat16)
        log_total = jnp.broadcast_to(top + jnp.log2(total), (rows, 128))
        total_ref[h, :, here] = log_total.T[:8]
    reduce_step(step, product(attended_ref[here, :], mixing_ref[...]), refs, ids, out_ref)

def attend(packed, places, key_last, mixing, heads, token_rows, collective_id):
    rows = packed.shape[0]
    inner, width = mixing.shape
    if not small_plane():
        attended, totals = attention_forward(packed, places, key_last, heads)
        part = product(attended, mixing).astype(jnp.bfloat16)
        return (attended, totals, lax.psum_scatter(part, PLANE, scatter_dimension=0, tiled=True).astype(jnp.float32))
    return pl.pallas_call(functools.partial(attend_kernel, heads), grid=(8,), out_shape=[jax.ShapeDtypeStruct((rows, inner), jnp.bfloat16), jax.ShapeDtypeStruct((heads, 8, rows), jnp.float32), jax.ShapeDtypeStruct((token_rows, width), jnp.float32)], in_specs=[VMEM] * 5, out_specs=[VMEM] * 3, scratch_shapes=reduce_scratch(token_rows, width), compiler_params=remote_params(collective_id, 60), name='attend')(packed, places[:, None], places[None, :], key_last[None, :], mixing)

def gather_order(step):
    return step + 2 * (step % 2) - 1 + (8 - step) // 8 - step // 7

def gather_step(step, slots, send, recv, ids):
    across, up, partner, _ = ids
    half = slots.shape[1] // 2
    low, high = (pl.ds(0, half), pl.ds(half, half))

    def copy(number, source, target, device):
        return remote(slots.at[source], slots.at[target], send, recv, number, device)
    across_low = copy(0, (0, low), (1, low), across)
    up_high = copy(1, (0, high), (4, high), up)
    across_high = copy(2, (0, high), (1, high), across)
    up_low = copy(3, (0, low), (4, low), up)
    own = copy(4, 0, 2, partner)
    far_low = copy(5, (1, low), (5, low), up)
    far_high = copy(6, (4, high), (5, high), across)
    pass_across = copy(7, 1, 3, partner)
    pass_up = copy(8, 4, 6, partner)
    pass_low = copy(9, (5, low), (7, low), partner)
    pass_high = copy(10, (5, high), (7, high), partner)

    @pl.when(step == 0)
    def _():
        for one in (across_low, up_high, own, across_high, up_low):
            one.start()

    @pl.when(step == 1)
    def _():
        own.wait_recv()

    @pl.when(step == 2)
    def _():
        across_low.wait_recv()
        far_low.start()
        up_high.wait_recv()
        far_high.start()
        across_high.wait_recv()
        pass_across.start()

    @pl.when(step == 3)
    def _():
        up_low.wait_recv()
        pass_up.start()

    @pl.when(step == 4)
    def _():
        pass_across.wait_recv()

    @pl.when(step == 5)
    def _():
        pass_up.wait_recv()

    @pl.when(step == 6)
    def _():
        far_low.wait_recv()
        pass_low.start()
        far_high.wait_recv()
        pass_high.start()

    @pl.when(step == 7)
    def _():
        pass_low.wait_recv()
        pass_high.wait_recv()
        for one in (across_low, up_high, across_high, up_low, own, far_low, far_high, pass_across, pass_up, pass_low, pass_high):
            one.wait_send()

def attend_back_kernel(heads, branch_ref, homed_ref, head_ref, mixing_ref, attended_ref, total_ref, place_ref, first_ref, last_ref, part_ref, out_ref, homed_out, sums_ref, turned, key_sum, value_sum, part_sum, slots, load, send, recv, *cargo):
    ids = plane_ids()
    step = pl.program_id(0)
    home_start, home_finish = home_cargo(homed_ref, homed_out, *cargo)
    rows = slots.shape[1]
    size = head_ref.shape[1] // (3 * heads)
    scale = size ** (-0.5)
    factor = scale * log2_e

    @pl.when(step == 0)
    def _():
        first = pltpu.make_async_copy(branch_ref, slots.at[0], load)
        first.start()
        for h in range(heads):
            turned[h] = head_ref[:, (3 * h + 1) * size:(3 * h + 2) * size].T
        key_sum[...] = jnp.zeros_like(key_sum)
        value_sum[...] = jnp.zeros_like(value_sum)
        part_sum[...] = jnp.zeros_like(part_sum)
        sums_ref[...] = jnp.zeros_like(sums_ref)
        greet_all(ids[:3], True)
        home_start()
        first.wait()
    gather_step(step, slots, send, recv, ids)
    k = gather_order(step)
    here = pl.ds(pl.multiple_of(ids[3](k) * rows, rows), rows)
    part_sum[...] += row_outer(attended_ref[here, :], slots[k])
    slopes = product_transposed(slots[k], mixing_ref[...]).astype(jnp.bfloat16)
    place = place_ref[:, here]
    allowed = (first_ref[...] <= place) & (place <= last_ref[...])
    for h in range(heads):
        queries = head_ref[here, 3 * h * size:(3 * h + 1) * size]
        keys = head_ref[:, (3 * h + 1) * size:(3 * h + 2) * size]
        values = head_ref[:, (3 * h + 2) * size:(3 * h + 3) * size]
        slope = slopes[:, h * size:(h + 1) * size]
        scores = product_transposed(keys, queries)
        soft = jnp.where(allowed, jnp.exp2(scores * factor - total_ref[h, :1, here]), 0.0)
        weight_slope = product_transposed(values, slope)
        centre = jnp.sum(soft * weight_slope, axis=0, keepdims=True)
        score_slope = (soft * (weight_slope - centre)).astype(jnp.bfloat16)
        value_sum[h] += product(soft.astype(jnp.bfloat16), slope)
        key_sum[h] += product(score_slope, queries)
        query_slope = product(turned[h], score_slope)
        query_slope = (query_slope.T * scale).astype(jnp.bfloat16)
        out_ref[here, 3 * h * size:(3 * h + 1) * size] = query_slope
        sums_ref[:, 3 * h * size:(3 * h + 1) * size] += jnp.sum(query_slope.astype(jnp.float32), axis=0, keepdims=True)

    @pl.when(step == 7)
    def _():
        for h in range(heads):
            out_ref[:, (3 * h + 1) * size:(3 * h + 2) * size] = (key_sum[h] * scale).astype(jnp.bfloat16)
            value_slope = value_sum[h].astype(jnp.bfloat16)
            out_ref[:, (3 * h + 2) * size:(3 * h + 3) * size] = value_slope
            sums_ref[:, (3 * h + 2) * size:(3 * h + 3) * size] = jnp.sum(value_slope.astype(jnp.float32), axis=0, keepdims=True)
        part_ref[...] = part_sum[...].astype(jnp.bfloat16)
        home_finish()

def attend_back(branch_slope, homed, packed, mixing, attended, totals, places, key_last, heads, collective_id):
    rows, columns = packed.shape
    token_rows, width = branch_slope.shape
    size = columns // (3 * heads)
    if not small_plane():
        every = lax.all_gather(branch_slope, PLANE, axis=0, tiled=True)
        slopes = product_transposed(every, mixing).astype(jnp.bfloat16)
        part = row_outer(attended, every).astype(jnp.bfloat16)
        slopes = attention_backward(packed, totals, slopes, places, key_last, heads)
        return (part, slopes, from_plane(homed), jnp.sum(slopes.astype(jnp.float32), axis=0, keepdims=True))
    return pl.pallas_call(functools.partial(attend_back_kernel, heads), grid=(8,), out_shape=[jax.ShapeDtypeStruct(mixing.shape, jnp.bfloat16), jax.ShapeDtypeStruct((rows, columns), jnp.bfloat16), jax.ShapeDtypeStruct(homed.shape, homed.dtype), jax.ShapeDtypeStruct((1, columns), jnp.float32)], in_specs=[ANY] * 2 + [VMEM] * 7, out_specs=[VMEM, VMEM, ANY, VMEM], scratch_shapes=[pltpu.VMEM((heads, size, rows), jnp.bfloat16), pltpu.VMEM((heads, rows, size), jnp.float32), pltpu.VMEM((heads, rows, size), jnp.float32), pltpu.VMEM(mixing.shape, jnp.float32), pltpu.VMEM((8, token_rows, width), jnp.bfloat16), DMA, DMA((11,)), DMA((11,)), DMA, DMA, DMA], compiler_params=remote_params(collective_id, 62), name='attend_back')(branch_slope, homed, packed, mixing, attended, totals, places[None, :], places[:, None], key_last[:, None])

def add_outer(total, left, right):
    turned = left.T
    for first in range(0, total.shape[1], 256):
        here = pl.ds(first, 256)
        total[:, here] += product(turned, right[:, first:first + 256])

def rep_order(total, narrow, part_ref, sem):
    groups, reps = (lax.axis_size('grp'), lax.axis_size('rep'))
    rows = total.shape[0] // (groups * reps)
    for g in range(groups):
        for r in range(reps):
            come, go = (pl.ds((g * reps + r) * rows, rows), pl.ds((r * groups + g) * rows, rows))
            narrow[come, :] = total[come, :].astype(jnp.bfloat16)
            pltpu.make_async_copy(narrow.at[come], part_ref.at[go], sem.at[g, r]).start()

def rep_order_wait(narrow, part_ref, sem):
    groups, reps = (lax.axis_size('grp'), lax.axis_size('rep'))
    rows = narrow.shape[0] // (groups * reps)
    for g in range(groups):
        for r in range(reps):
            come, go = (pl.ds((g * reps + r) * rows, rows), pl.ds((r * groups + g) * rows, rows))
            pltpu.make_async_copy(narrow.at[come], part_ref.at[go], sem.at[g, r]).wait()

def hidden_kernel(middle_ref, cotangent_ref, expand_ref, offset_ref, every_ref, active_ref, rise_ref, part_ref, slots, cotangents, actives, rises, total, load, send, recv, store, fetch_cotangent, active_store, rise_store, expand, expand_load, narrow, part_store):
    ids = plane_ids()
    step = pl.program_id(0)
    turn = lax.rem(step, 2)

    def fetch(number, side):
        return pltpu.make_async_copy(cotangent_ref.at[ids[3](gather_order(number))], cotangents.at[side], fetch_cotangent.at[side])

    @pl.when(step == 0)
    def _():
        first = pltpu.make_async_copy(middle_ref, slots.at[0], load)
        first.start()
        rows_in = row_loads(expand_ref, expand, expand_load)
        for one in rows_in:
            one.start()
        fetch(0, 0).start()
        total[...] = jnp.zeros_like(total)
        greet(ids[:3])
        first.wait()
        for one in rows_in:
            one.wait()
    gather_step(step, slots, send, recv, ids)
    k = gather_order(step)

    def keep(number):
        return pltpu.make_async_copy(slots.at[number], every_ref.at[ids[3](number)], store.at[number])

    def put(number, side):
        piece = ids[3](number)
        return (pltpu.make_async_copy(actives.at[side], active_ref.at[piece], active_store.at[side]), pltpu.make_async_copy(rises.at[side], rise_ref.at[piece], rise_store.at[side]))
    keep(k).start()

    @pl.when(step >= 2)
    def _():
        for one in put(k, turn):
            one.wait()
    expanded = product(slots[k], expand[...]) + offset_ref[...]
    below = 0.5 * (1.0 + lax.erf(expanded * root_half))
    actives[turn] = (expanded * below).astype(jnp.bfloat16)
    rises[turn] = below + expanded * (jnp.exp(-0.5 * expanded * expanded) * normal_peak)
    for one in put(k, turn):
        one.start()
    fetch(step, turn).wait()

    @pl.when(step < 7)
    def _():
        fetch(step + 1, 1 - turn).start()
    add_outer(total, cotangents[turn], actives[turn])

    @pl.when(step == 7)
    def _():
        rep_order(total, narrow, part_ref, part_store)
        for late in range(2):
            for one in put(k, late):
                one.wait()
        for number in range(8):
            keep(number).wait()
        rep_order_wait(narrow, part_ref, part_store)

def hidden(middle, cotangent_all, expand_slice, offset, collective_id):
    rows, width = middle.shape
    count = lax.axis_size('grp') * lax.axis_size('sub')
    inner = expand_slice.shape[1]
    if not small_plane():
        every = lax.all_gather(middle, PLANE, axis=0, tiled=True)
        expanded = product(every, rep_rows_last(expand_slice)) + offset
        below = 0.5 * (1.0 + lax.erf(expanded * root_half))
        rise = below + expanded * (jnp.exp(-0.5 * expanded * expanded) * normal_peak)
        active = (expanded * below).astype(jnp.bfloat16)
        return (every, active, rise, rep_rows_first(row_outer(cotangent_all, active)))
    every, active, rise, part = pl.pallas_call(hidden_kernel, grid=(8,), out_shape=[jax.ShapeDtypeStruct((8, rows, width), middle.dtype), jax.ShapeDtypeStruct((8, rows, inner), jnp.bfloat16), jax.ShapeDtypeStruct((8, rows, inner), jnp.float32), jax.ShapeDtypeStruct((width, inner), jnp.bfloat16)], in_specs=[ANY, ANY, ANY, VMEM], out_specs=[ANY] * 4, scratch_shapes=[pltpu.VMEM((8, rows, width), middle.dtype), pltpu.VMEM((2, rows, width), jnp.bfloat16), pltpu.VMEM((2, rows, inner), jnp.bfloat16), pltpu.VMEM((2, rows, inner), jnp.float32), pltpu.VMEM((width, inner), jnp.float32), DMA, DMA((11,)), DMA((11,)), DMA((8,)), DMA((2,)), DMA((2,)), DMA((2,)), *row_loads_scratch(expand_slice.shape, expand_slice.dtype), *row_loads_scratch(expand_slice.shape, jnp.bfloat16)], compiler_params=remote_params(collective_id, 60), name='hidden')(middle, cotangent_all.reshape(8, rows, width), expand_slice, offset[None, :])
    return (every.reshape(count * rows, width), active.reshape(count * rows, inner), rise.reshape(count * rows, inner), part)

def hidden_back_kernel(cotangent_ref, middle_ref, rise_ref, shrink_ref, expand_ref, slope_ref, out_ref, part_ref, sums_ref, cotangents, middles, rises, slopes, total, fetches, store, shrink, shrink_load, expand, expand_load, narrow, part_store, *refs):
    ids = plane_ids()
    step = pl.program_id(0)

    def fetch(number, side):
        piece = ids[3](reduce_order(number))
        return [pltpu.make_async_copy(source.at[piece], target.at[side], fetches.at[kind, side]) for kind, (source, target) in enumerate(((cotangent_ref, cotangents), (rise_ref, rises), (middle_ref, middles)))]

    def put(number, side):
        return pltpu.make_async_copy(slopes.at[side], slope_ref.at[ids[3](reduce_order(number))], store.at[side])
    turn = lax.rem(step, 2)

    @pl.when(step == 0)
    def _():
        rows_in = row_loads(shrink_ref, shrink, shrink_load) + row_loads(expand_ref, expand, expand_load)
        for one in rows_in:
            one.start()
        for one in fetch(0, 0):
            one.start()
        total[...] = jnp.zeros_like(total)
        sums_ref[...] = jnp.zeros_like(sums_ref)
        greet(ids[:3])
        for one in rows_in:
            one.wait()
    for one in fetch(step, turn):
        one.wait()

    @pl.when(step < 7)
    def _():
        for one in fetch(step + 1, 1 - turn):
            one.start()

    @pl.when(step >= 2)
    def _():
        put(step, turn).wait()
    slope = product(cotangents[turn], shrink[...]) * rises[turn]
    slopes[turn] = slope.astype(jnp.bfloat16)
    put(step, turn).start()

    def before():
        add_outer(total, middles[turn], slopes[turn])
        sums_ref[...] += jnp.sum(slopes[turn].astype(jnp.float32), axis=0, keepdims=True)

        @pl.when(step == 7)
        def _():
            rep_order(total, narrow, part_ref, part_store)
    reduce_step(step, product_transposed(slopes[turn], expand[...]), refs, ids, out_ref, before)

    @pl.when(step == 7)
    def _():
        put(6, 0).wait()
        put(7, 1).wait()
        rep_order_wait(narrow, part_ref, part_store)

def hidden_back(cotangent_all, middle_all, rise, shrink_slice, expand_slice, token_rows, collective_id):
    rows, width = cotangent_all.shape
    inner = shrink_slice.shape[1]
    if not small_plane():
        slope = (product(cotangent_all, rep_rows_last(shrink_slice)) * rise).astype(jnp.bfloat16)
        part = product_transposed(slope, rep_rows_last(expand_slice)).astype(jnp.bfloat16)
        normed = lax.psum_scatter(part, PLANE, scatter_dimension=0, tiled=True).astype(jnp.float32)
        sums = jnp.sum(slope.astype(jnp.float32), axis=0)
        return (slope, normed, rep_rows_first(row_outer(middle_all, slope)), sums)
    pieces = (8, token_rows, width)
    slope, normed, part, sums = pl.pallas_call(hidden_back_kernel, grid=(8,), out_shape=[jax.ShapeDtypeStruct((8, token_rows, inner), jnp.bfloat16), jax.ShapeDtypeStruct((token_rows, width), jnp.float32), jax.ShapeDtypeStruct((width, inner), jnp.bfloat16), jax.ShapeDtypeStruct((1, inner), jnp.float32)], in_specs=[ANY] * 5, out_specs=[ANY, VMEM, ANY, VMEM], scratch_shapes=[pltpu.VMEM((2, token_rows, width), jnp.bfloat16), pltpu.VMEM((2, token_rows, width), jnp.bfloat16), pltpu.VMEM((2, token_rows, inner), jnp.float32), pltpu.VMEM((2, token_rows, inner), jnp.bfloat16), pltpu.VMEM((width, inner), jnp.float32), DMA((3, 2)), DMA((2,)), *row_loads_scratch(shrink_slice.shape, shrink_slice.dtype), *row_loads_scratch(expand_slice.shape, expand_slice.dtype), *row_loads_scratch(expand_slice.shape, jnp.bfloat16), *reduce_scratch(token_rows, width)], compiler_params=remote_params(collective_id, 63), name='hidden_back')(cotangent_all.reshape(pieces), middle_all.reshape(pieces), rise.reshape(8, token_rows, inner), shrink_slice, expand_slice)
    return (slope.reshape(rows, inner), normed, part, sums[0])

def plane_moves():
    groups, reps, subs = (lax.axis_size(n) for n in EVERY)
    moves = []
    for g in range(groups):
        for r in range(reps):
            turn = (g + r) % groups
            position = turn % 2 * (groups // 2) + turn // 2
            for u in range(subs):
                moves.append(tuple(((a * reps + b) * subs + u for a, b in ((g, r), (position, r), (position, g)))))
    return moves

def to_door(array):
    return lax.ppermute(array, EVERY, [(home, door) for home, door, _ in plane_moves()])

def to_keeper(array):
    return lax.ppermute(array, EVERY, [(door, away) for _, door, away in plane_moves()])

def to_plane_at_once(array):
    return lax.ppermute(array, EVERY, [(home, away) for home, _, away in plane_moves()])

def from_plane(array):
    return lax.ppermute(array, EVERY, [(away, home) for home, _, away in plane_moves()])

def plane_order(places):
    groups = lax.axis_size('grp')
    blocks = jnp.roll(places.reshape(groups, -1), lax.axis_index('rep'), axis=0)
    return blocks.reshape(groups // 2, 2, -1).transpose(1, 0, 2).reshape(-1)

def rep_rows(own):
    return lax.all_gather(own, 'rep', axis=0, tiled=True)

def rep_rows_last(every):
    groups, reps, subs = (lax.axis_size(name) for name in EVERY)
    columns = every.shape[1]
    ordered = every.reshape(reps, groups, subs, -1, columns).transpose(1, 0, 2, 3, 4)
    return ordered.reshape(-1, columns)

def rep_rows_first(gradient):
    groups, reps, subs = (lax.axis_size(name) for name in EVERY)
    columns = gradient.shape[1]
    ordered = gradient.astype(jnp.bfloat16).reshape(groups, reps, subs, -1, columns)
    return ordered.transpose(1, 0, 2, 3, 4).reshape(-1, columns)

def rep_sums(ordered):
    return lax.psum_scatter(ordered, 'rep', scatter_dimension=0, tiled=True)

def sub_turn(block):
    groups, reps, subs = (lax.axis_size(name) for name in EVERY)
    low = reps // subs
    moves = [((g * reps + r) * subs + u, (g * reps + u * low + r % low) * subs + r // low) for g in range(groups) for r in range(reps) for u in range(subs)]
    return lax.ppermute(block, EVERY, moves)

def sub_rows(own):
    rows, width = own.shape
    reps, subs = (lax.axis_size('rep'), lax.axis_size('sub'))
    shares = own.reshape(subs, reps // subs, -1, width)
    if subs != 2:
        every = lax.all_to_all(shares, 'sub', split_axis=0, concat_axis=0, tiled=True)
        return every.transpose(1, 0, 2, 3).reshape(rows, width)
    me = lax.axis_index('sub')
    kept = jnp.where(me == 0, shares[0], shares[1])
    come = lax.ppermute(jnp.where(me == 0, shares[1], shares[0]), 'sub', [(0, 1), (1, 0)])
    first, second = (jnp.where(me == 0, kept, come), jnp.where(me == 0, come, kept))
    return jnp.stack([first, second], axis=1).reshape(rows, width)

def mixing_sums_of(part):
    reps, subs = (lax.axis_size('rep'), lax.axis_size('sub'))
    rows, width = part.shape
    ordered = part.reshape(reps // subs, subs, rows // reps, width).transpose(1, 0, 2, 3)
    return lax.psum_scatter(ordered.reshape(rows, width), 'rep', scatter_dimension=0, tiled=True)

def sub_owned(part, reps):
    rows, width = part.shape
    subs = lax.axis_size('sub')
    shares = part.reshape(reps // subs, subs, -1, width).transpose(1, 0, 2, 3)
    if subs != 2:
        every = lax.all_to_all(shares, 'sub', split_axis=0, concat_axis=0, tiled=True)
        return every.reshape(rows, width)
    me = lax.axis_index('sub')
    kept = jnp.where(me == 0, shares[0], shares[1])
    come = lax.ppermute(jnp.where(me == 0, shares[1], shares[0]), 'sub', [(0, 1), (1, 0)])
    first, second = (jnp.where(me == 0, kept, come), jnp.where(me == 0, come, kept))
    return jnp.concatenate([first, second], axis=0).reshape(rows, width)

def shards(layer_input, entry_gain, entry_shift, joint_weight, query_offset, value_offset, mixing_weight, attention_offset, middle_gain, middle_shift, expand_weight, expand_offset, shrink_weight, shrink_offset, placement, slot_lengths, cotangent):
    token_rows, width = layer_input.shape
    hidden_width = expand_weight.shape[1]
    groups, reps, subs = (lax.axis_size(name) for name in EVERY)
    plane_count = groups * subs
    plane_index = lax.axis_index(PLANE)
    head_size = width // HEADS
    local_heads = HEADS // plane_count
    head_columns = local_heads * head_size
    plane_rows = plane_count * token_rows
    facts = to_plane_at_once(jnp.concatenate([placement, slot_lengths], axis=1))[0]
    mixing_own = rep_rows(mixing_weight)
    moved_input, joint_own, expand_own = opening(layer_input, (joint_weight, expand_weight), 12)
    joint_own, mixing_own = lax.optimization_barrier((joint_own, mixing_own))
    input_float = moved_input.astype(jnp.float32)
    joint_every = rep_rows(joint_own)
    entry_normal, entry_inverse = norm_terms(input_float)
    entry_normed = (entry_normal * entry_gain + entry_shift).astype(jnp.bfloat16)
    entry_all, shrink_own = plane_gather(entry_normed, (shrink_weight,), 1)
    cotangent, facts, entry_all = lax.optimization_barrier((cotangent, facts, entry_all))
    cotangent = to_door(cotangent)
    places = plane_order(facts[:placement.shape[1]])
    lengths = facts[placement.shape[1]:]
    prompt = places.shape[0] // 2
    key_last = key_bounds(places, lengths, prompt)
    expand_slice = rep_rows(expand_own)
    shrink_slice = rep_rows(shrink_own)
    cotangent = to_keeper(cotangent)
    mixing_slice = sub_rows(mixing_own)
    offsets = jnp.stack([query_offset.reshape(HEADS, head_size), jnp.zeros((HEADS, head_size), jnp.float32), value_offset.reshape(HEADS, head_size)], axis=1).reshape(-1)
    offsets = lax.dynamic_slice_in_dim(offsets, plane_index * 3 * head_columns, 3 * head_columns)
    heads_kept = (product(entry_all, rep_rows_last(joint_every)) + offsets).astype(jnp.bfloat16)
    attended, log_totals, branch = attend(heads_kept, places, key_last, mixing_slice, local_heads, token_rows, 3)
    residual = input_float + (branch + attention_offset)
    middle_normal, middle_inverse = norm_terms(residual)
    middle_normed = (middle_normal * middle_gain + middle_shift).astype(jnp.bfloat16)
    cotangent, middle_normed = lax.optimization_barrier((cotangent, middle_normed))
    cotangent_all, = plane_gather(cotangent, (), 4)
    middle_normed, cotangent_all = lax.optimization_barrier((middle_normed, cotangent_all))
    hidden_local = hidden_width // plane_count
    offset_local = lax.dynamic_slice_in_dim(expand_offset, plane_index * hidden_local, hidden_local)
    middle_all, activated, rise, shrink_part = hidden(middle_normed, cotangent_all, expand_slice, offset_local, 5)
    shrink_sums = rep_sums(shrink_part)
    expanded_slope, normed_slope, expand_part, expanded_sums = hidden_back(cotangent_all, middle_all, rise, shrink_slice, expand_slice, token_rows, 6)
    expand_sums = rep_sums(expand_part)
    activated, normed_slope = lax.optimization_barrier((activated, normed_slope))
    shrunk, = product_reduce(activated.reshape(plane_count, token_rows, hidden_local), shrink_slice, None, None, 8)
    own_output = (residual + shrunk + shrink_offset).astype(jnp.bfloat16)
    own_output, normed_slope = lax.optimization_barrier((own_output, normed_slope))
    cotangent_float = cotangent.astype(jnp.float32)
    residual_slope = cotangent_float + norm_back(normed_slope, middle_gain, middle_normal, middle_inverse)
    branch_slope = residual_slope.astype(jnp.bfloat16)
    mixing_part, joint_slope, layer_output, slope_sums = attend_back(branch_slope, own_output, heads_kept, mixing_slice, attended, log_totals, places, key_last, local_heads, 7)
    shrink_sums, joint_slope = lax.optimization_barrier((shrink_sums, joint_slope))
    joint_part = rep_rows_first(row_outer(entry_all, joint_slope))
    joint_part, joint_slope, expand_sums, mixing_part = lax.optimization_barrier((joint_part, joint_slope, expand_sums, mixing_part))
    joint_sums = rep_sums(joint_part)
    mixing_part = sub_owned(mixing_part, reps)
    joint_sums, mixing_part = lax.optimization_barrier((joint_sums, mixing_part))
    mixing_sums = rep_sums(mixing_part)
    entry_slope, expand_rows = product_reduce(joint_slope.reshape(plane_count, token_rows, 3 * head_columns), joint_every, expand_sums, None, 9)
    own_gradient = (residual_slope + norm_back(entry_slope, entry_gain, entry_normal, entry_inverse)).astype(jnp.bfloat16)
    slope_sums = slope_sums.reshape(local_heads, 3, head_size)

    def placed(piece, whole_size):
        return lax.dynamic_update_slice_in_dim(jnp.zeros((whole_size,), jnp.float32), piece, plane_index * piece.shape[0], 0)
    small = [jnp.sum(entry_slope * entry_normal, axis=0), jnp.sum(entry_slope, axis=0), placed(slope_sums[:, 0].reshape(-1), width), placed(slope_sums[:, 2].reshape(-1), width), jnp.sum(branch_slope.astype(jnp.float32), axis=0), jnp.sum(normed_slope * middle_normal, axis=0), jnp.sum(normed_slope, axis=0), placed(expanded_sums, hidden_width), jnp.sum(cotangent_float, axis=0)]
    small_own = jnp.concatenate(small).reshape(-1, 128)
    small_all, input_gradient, joint_rows, shrink_rows = closing(small_own, own_gradient, (joint_sums, shrink_sums), 10)
    shrink_gradient = shrink_rows.astype(jnp.float32)
    expand_gradient = expand_rows.astype(jnp.float32)
    joint_gradient = joint_rows.astype(jnp.float32)
    mixing_gradient = mixing_sums.astype(jnp.float32)
    small_all = small_all.reshape(-1)
    small_sums, first = ([], 0)
    for piece in small:
        small_sums.append(small_all[first:first + piece.shape[0]])
        first += piece.shape[0]
    return (layer_output, input_gradient, small_sums[0], small_sums[1], joint_gradient, small_sums[2], small_sums[3], mixing_gradient, small_sums[4], small_sums[5], small_sums[6], expand_gradient, small_sums[7], shrink_gradient, small_sums[8])

def solution(mesh):
    groups, sequence = (mesh.shape['grp'], mesh.shape['seq'])
    subs = sequence // groups
    planes = Mesh(mesh.devices.reshape(groups, sequence // subs, subs), EVERY)
    rows, whole, group_rows = (P(EVERY, None), P(), P('grp', None))
    return jax.shard_map(shards, mesh=planes, in_specs=(rows, whole, whole, rows, whole, whole, rows, whole, whole, whole, rows, whole, rows) + (whole, group_rows, group_rows, rows), out_specs=(rows, rows, whole, whole, rows, whole, whole, rows, whole, whole, whole, rows, whole) + (rows, whole), check_vma=False)
```

```python
import functools
import jax
import jax.numpy as jnp
from jax import lax
from jax.experimental import pallas as pl
from jax.experimental.pallas import tpu as pltpu
from jax.sharding import Mesh, PartitionSpec as P
HEADS = 16
CONT = 256
PLANE = ('grp', 'sub')
EVERY = ('grp', 'rep', 'sub')
MESH = pl.DeviceIdType.MESH
ANY = pl.BlockSpec(memory_space=pl.ANY)
VMEM = pl.BlockSpec(memory_space=pltpu.VMEM)
DMA = pltpu.SemaphoreType.DMA
MIB = 1 << 20
norm_epsilon = 1e-05
masked_score = -1e+30
log2_e = 1.4426950408889634
root_half = 0.7071067811865476
normal_peak = 0.3989422804014327

def norm_terms(values):
    average = jnp.mean(values, axis=-1, keepdims=True)
    centered = values - average
    variance = jnp.mean(centered * centered, axis=-1, keepdims=True)
    inverse = lax.rsqrt(variance + norm_epsilon)
    return (centered * inverse, inverse)

def norm_back(slope, gain, normal, inverse):
    scaled = slope * gain
    return inverse * (scaled - jnp.mean(scaled, axis=-1, keepdims=True) - normal * jnp.mean(scaled * normal, axis=-1, keepdims=True))

def key_bounds(positions, lengths, prompt):
    segment = (positions - prompt) // CONT
    within = positions - prompt - segment * CONT
    slot_ids = jnp.arange(lengths.shape[0], dtype=jnp.int32)
    slot_limit = jnp.sum(jnp.where(segment[:, None] == slot_ids[None, :], lengths[None, :], 0), axis=1)
    last = prompt + (segment + 1) * CONT - 1
    last = jnp.where(within < slot_limit, last, -1)
    return jnp.where(positions < prompt, positions.shape[0], last)

def product(left_matrix, right_matrix):
    return jnp.dot(left_matrix, right_matrix, preferred_element_type=jnp.float32)

def product_transposed(left_matrix, right_matrix):
    return lax.dot_general(left_matrix, right_matrix, (((1,), (1,)), ((), ())), preferred_element_type=jnp.float32)

def row_outer(left_matrix, right_matrix):
    return lax.dot_general(left_matrix, right_matrix, (((0,), (0,)), ((), ())), preferred_element_type=jnp.float32)

def attention_forward(packed, places, key_last, heads):
    rows, columns = packed.shape
    size = columns // (3 * heads)
    block = 256
    factor = size ** (-0.5) * log2_e

    def kernel(q_ref, k_ref, v_ref, place_ref, first_ref, last_ref, out_ref, total_ref):
        scores = product_transposed(q_ref[...], k_ref[...])
        place = place_ref[...]
        allowed = (first_ref[...] <= place) & (place <= last_ref[...])
        scores = jnp.where(allowed, scores * factor, masked_score)
        top = jnp.max(scores, axis=1, keepdims=True)
        soft = jnp.exp2(scores - top)
        total = jnp.sum(soft, axis=1, keepdims=True)
        mixture = product(soft.astype(jnp.bfloat16), v_ref[...])
        out_ref[...] = (mixture / total).astype(jnp.bfloat16)
        log_total = jnp.broadcast_to(top + jnp.log2(total), (block, 128))
        total_ref[0] = log_total.T[:8]
    return pl.pallas_call(kernel, grid=(heads, rows // block), in_specs=[pl.BlockSpec((block, size), lambda h, i: (i, 3 * h)), pl.BlockSpec((rows, size), lambda h, i: (0, 3 * h + 1)), pl.BlockSpec((rows, size), lambda h, i: (0, 3 * h + 2)), pl.BlockSpec((block, 1), lambda h, i: (i, 0)), pl.BlockSpec((1, rows), lambda h, i: (0, 0)), pl.BlockSpec((1, rows), lambda h, i: (0, 0))], out_specs=[pl.BlockSpec((block, size), lambda h, i: (i, h)), pl.BlockSpec((1, 8, block), lambda h, i: (h, 0, i))], out_shape=[jax.ShapeDtypeStruct((rows, heads * size), jnp.bfloat16), jax.ShapeDtypeStruct((heads, 8, rows), jnp.float32)], compiler_params=pltpu.CompilerParams(vmem_limit_bytes=56 * MIB), cost_estimate=pl.CostEstimate(flops=4 * heads * rows * rows * size, bytes_accessed=4 * rows * heads * size * 2, transcendentals=heads * rows * rows), name='attention_forward')(packed, packed, packed, places[:, None], places[None, :], key_last[None, :])

def attention_backward(packed, totals, slopes, places, key_last, heads):
    rows, columns = packed.shape
    size = columns // (3 * heads)
    block = 256
    scale = size ** (-0.5)
    factor = scale * log2_e

    def kernel(q_ref, k_ref, v_ref, slope_ref, total_ref, place_ref, first_ref, last_ref, out_ref, turned_ref, key_sum, value_sum):
        step = pl.program_id(1)

        @pl.when(step == 0)
        def _():
            turned_ref[...] = k_ref[...].T
            key_sum[...] = jnp.zeros_like(key_sum)
            value_sum[...] = jnp.zeros_like(value_sum)
        queries = q_ref[...]
        slope = slope_ref[...]
        scores = product_transposed(k_ref[...], queries)
        place = place_ref[...]
        allowed = (first_ref[...] <= place) & (place <= last_ref[...])
        soft = jnp.where(allowed, jnp.exp2(scores * factor - total_ref[0, :1]), 0.0)
        weight_slope = product_transposed(v_ref[...], slope)
        centre = jnp.sum(soft * weight_slope, axis=0, keepdims=True)
        score_slope = (soft * (weight_slope - centre)).astype(jnp.bfloat16)
        value_sum[...] += product(soft.astype(jnp.bfloat16), slope)
        key_sum[...] += product(score_slope, queries)
        query_slope = product(turned_ref[...], score_slope)
        here = pl.ds(pl.multiple_of(step * block, block), block)
        out_ref[here, :size] = (query_slope.T * scale).astype(jnp.bfloat16)

        @pl.when(step == pl.num_programs(1) - 1)
        def _():
            out_ref[:, size:2 * size] = (key_sum[...] * scale).astype(jnp.bfloat16)
            out_ref[:, 2 * size:] = value_sum[...].astype(jnp.bfloat16)
    return pl.pallas_call(kernel, grid=(heads, rows // block), in_specs=[pl.BlockSpec((block, size), lambda h, i: (i, 3 * h)), pl.BlockSpec((rows, size), lambda h, i: (0, 3 * h + 1)), pl.BlockSpec((rows, size), lambda h, i: (0, 3 * h + 2)), pl.BlockSpec((block, size), lambda h, i: (i, h)), pl.BlockSpec((1, 8, block), lambda h, i: (h, 0, i)), pl.BlockSpec((1, block), lambda h, i: (0, i)), pl.BlockSpec((rows, 1), lambda h, i: (0, 0)), pl.BlockSpec((rows, 1), lambda h, i: (0, 0))], out_specs=pl.BlockSpec((rows, 3 * size), lambda h, i: (0, h)), out_shape=jax.ShapeDtypeStruct((rows, columns), jnp.bfloat16), scratch_shapes=[pltpu.VMEM((size, rows), jnp.bfloat16), pltpu.VMEM((rows, size), jnp.float32), pltpu.VMEM((rows, size), jnp.float32)], compiler_params=pltpu.CompilerParams(vmem_limit_bytes=56 * MIB), cost_estimate=pl.CostEstimate(flops=10 * heads * rows * rows * size, bytes_accessed=8 * rows * heads * size * 2, transcendentals=heads * rows * rows), name='attention_backward')(packed, packed, packed, slopes, totals, places[None, :], places[:, None], key_last[:, None])

def small_plane():
    return (lax.axis_size('grp'), lax.axis_size('sub')) == (4, 2)

def plane_ids():
    g, r, u = (lax.axis_index(n) for n in ('grp', 'rep', 'sub'))
    y, c = (g // 2, g % 2)
    across, up, partner = ((g, r, 1 - u), ((1 - y) * 2 + c, r, u), (y * 2 + 1 - c, r, u))

    def piece(k):
        above, beside, side = (k // 4, k // 2 % 2, k % 2)
        return ((y + above) % 2 * 2 + (c + beside) % 2) * 2 + (u + side) % 2
    return (across, up, partner, piece)

def greet(devices):
    barrier = pltpu.get_barrier_semaphore()
    for device in devices:
        pl.semaphore_signal(barrier, inc=1, device_id=device, device_id_type=MESH)
    pl.semaphore_wait(barrier, len(devices))

def remote(source, target, send, recv, number, device):
    return pltpu.make_async_remote_copy(src_ref=source, dst_ref=target, send_sem=send.at[number], recv_sem=recv.at[number], device_id=device, device_id_type=MESH)

def plane_peers():
    groups, _, subs = (lax.axis_size(n) for n in EVERY)
    g, r, u = (lax.axis_index(n) for n in EVERY)
    count = groups * subs
    place = g * subs + u
    return (place, [(t // subs, r, lax.rem(t, subs)) for t in (lax.rem(place + step, count) for step in range(1, count))])

def owner_cargo(source, target, send, recv, local):
    count = lax.axis_size('grp') * lax.axis_size('sub')
    subs = lax.axis_size('sub')
    rows, width = (target.shape[0], source.shape[1])
    place, peers = plane_peers()

    def block(t):
        return source.at[pl.ds(pl.multiple_of(t * rows, rows), rows), :]
    landing = target.at[:, pl.ds(pl.multiple_of(place * width, width), width)]
    own = pltpu.make_async_copy(block(place), landing, local)
    away = [remote(block(device[0] * subs + device[2]), landing, send, recv, number, device) for number, device in enumerate(peers)]

    def start():
        own.start()
        for one in away:
            one.start()

    def finish():
        own.wait()
        for one in away:
            one.wait_recv()
        for one in away:
            one.wait_send()
    return (start, finish)

def owner_scratch():
    count = lax.axis_size('grp') * lax.axis_size('sub')
    return [DMA((count - 1,)), DMA((count - 1,)), DMA]

def position_of(turn):
    groups = lax.axis_size('grp')
    return lax.rem(turn, 2) * (groups // 2) + turn // 2

def turn_of(position):
    half = lax.axis_size('grp') // 2
    return lax.rem(position, half) * 2 + position // half

def home_devices():
    g, r, u = (lax.axis_index(n) for n in EVERY)
    groups = lax.axis_size('grp')
    rep = lax.rem(turn_of(g) + groups - r, groups)
    return ((r, rep, u), (position_of(lax.rem(g + r, groups)), g, u), (r == g) & (rep == r))

def column_cargo(source, target, send, recv, local):
    subs = lax.axis_size('sub')
    rows, width = (source.shape[0], target.shape[1])
    place, peers = plane_peers()

    def block(t):
        return source.at[:, pl.ds(pl.multiple_of(t * width, width), width)]
    landing = target.at[pl.ds(pl.multiple_of(place * rows, rows), rows), :]
    own = pltpu.make_async_copy(block(place), landing, local)
    away = [remote(block(device[0] * subs + device[2]), landing, send, recv, number, device) for number, device in enumerate(peers)]

    def start():
        own.start()
        for one in away:
            one.start()

    def finish():
        own.wait()
        for one in away:
            one.wait_recv()
        for one in away:
            one.wait_send()
    return (start, finish)

def column_shape(weight):
    count = lax.axis_size('grp') * lax.axis_size('sub')
    return jax.ShapeDtypeStruct((weight.shape[0] * count, weight.shape[1] // count), weight.dtype)

def row_loads(source, target, sem):
    groups, reps = (lax.axis_size('grp'), lax.axis_size('rep'))
    rows = source.shape[0] // (groups * reps)
    return [pltpu.make_async_copy(source.at[pl.ds((r * groups + g) * rows, rows)], target.at[pl.ds((g * reps + r) * rows, rows)], sem.at[g, r]) for g in range(groups) for r in range(reps)]

def row_loads_scratch(shape, dtype):
    return [pltpu.VMEM(shape, dtype), DMA((lax.axis_size('grp'), lax.axis_size('rep')))]

def home_cargo(source, target, send, recv, local):
    goal, _, stays = home_devices()
    kept = pltpu.make_async_copy(source, target, local)
    moved = pltpu.make_async_remote_copy(src_ref=source, dst_ref=target, send_sem=send, recv_sem=recv, device_id=goal, device_id_type=MESH)

    def start():

        @pl.when(stays)
        def _():
            kept.start()

        @pl.when(jnp.logical_not(stays))
        def _():
            moved.start()

    def finish():

        @pl.when(stays)
        def _():
            kept.wait()

        @pl.when(jnp.logical_not(stays))
        def _():
            moved.wait_recv()
            moved.wait_send()
    return (start, finish)

def greet_all(devices, homes):
    barrier = pltpu.get_barrier_semaphore()
    for device in devices:
        pl.semaphore_signal(barrier, inc=1, device_id=device, device_id_type=MESH)
    if not homes:
        pl.semaphore_wait(barrier, len(devices))
        return
    _, origin, stays = home_devices()

    @pl.when(jnp.logical_not(stays))
    def _():
        pl.semaphore_signal(barrier, inc=1, device_id=origin, device_id_type=MESH)
    pl.semaphore_wait(barrier, len(devices) + 1 - stays.astype(jnp.int32))

def gather_kernel(weights, x_ref, *refs):
    sources, out_ref, landings = (refs[:weights], refs[weights], refs[weights + 1:2 * weights + 1])
    slots, load, send, recv, store, *cargo = refs[2 * weights + 1:]
    ids = plane_ids()
    step = pl.program_id(0)
    cargos = [column_cargo(sources[i], landings[i], *cargo[3 * i:3 * i + 3]) for i in range(weights)]

    @pl.when(step == 0)
    def _():
        first = pltpu.make_async_copy(x_ref, slots.at[0], load)
        first.start()
        greet(plane_peers()[1] if weights else ids[:3])
        first.wait()
    gather_step(step, slots, send, recv, ids)

    def keep(number):
        return pltpu.make_async_copy(slots.at[number], out_ref.at[ids[3](number)], store.at[number])
    keep(gather_order(step)).start()
    if weights:

        @pl.when(step == 2)
        def _():
            for start, _ in cargos:
                start()

    @pl.when(step == 7)
    def _():
        for _, finish in cargos:
            finish()
        for number in range(8):
            keep(number).wait()

def plane_gather(x, weights, collective_id):
    rows, width = x.shape
    if not small_plane():
        return [lax.all_gather(x, PLANE, axis=0, tiled=True)] + [exchange(w, False, collective_id + 20 + i) for i, w in enumerate(weights)]
    number = len(weights)
    every, *columns = pl.pallas_call(functools.partial(gather_kernel, number), grid=(8,), out_shape=[jax.ShapeDtypeStruct((8, rows, width), x.dtype)] + [column_shape(w) for w in weights], in_specs=[ANY] * (1 + number), out_specs=[ANY] * (1 + number), scratch_shapes=[pltpu.VMEM((8, rows, width), x.dtype), DMA, DMA((11,)), DMA((11,)), DMA((8,))] + owner_scratch() * number, compiler_params=remote_params(collective_id, 40), name='plane_gather')(x, *weights)
    return [every.reshape(8 * rows, width)] + columns

def reduce_scratch(rows, width):
    wide, narrow = (jnp.float32, jnp.bfloat16)
    return [pltpu.VMEM((4, rows, width), wide), pltpu.VMEM((4, rows, width), narrow), pltpu.VMEM((4, rows, width), narrow), pltpu.VMEM((3, rows, width), narrow), pltpu.VMEM((3, rows, width), narrow), DMA((10,)), DMA((10,))]

def reduce_order(step):
    return 7 - 2 * step + 7 * (step // 4)

def reduce_step(step, piece, refs, ids, out, before=None):
    sums, give, take, leave, come, send, recv = refs
    across, up, partner, _ = ids
    half = sums.shape[1] // 2
    low, high = (pl.ds(0, half), pl.ds(half, half))
    pair = step // 2

    def to_partner(number):
        return remote(give.at[number], take.at[number], send, recv, number, partner)

    def part(number, which, rows, device):
        return remote(leave.at[which, rows], come.at[which, rows], send, recv, number, device)

    def down(value):
        return value.astype(jnp.bfloat16)

    def up_cast(value):
        return value.astype(jnp.float32)

    @pl.when(lax.rem(step, 2) == 0)
    def _():
        give[pair] = down(piece)
        to_partner(pair).start()

    @pl.when(lax.rem(step, 2) == 1)
    def _():
        sums[pair] = piece
    if before is not None:
        before()

    @pl.when(lax.rem(step, 2) == 1)
    def _():
        to_partner(pair).wait_recv()
        sums[pair] += up_cast(take[pair])
    diagonal_across, diagonal_up = (part(4, 2, low, across), part(5, 2, high, up))
    across_low, up_high = (part(6, 0, low, across), part(7, 1, high, up))
    across_high, up_low = (part(8, 0, high, across), part(9, 1, low, up))

    @pl.when(step == 1)
    def _():
        leave[2] = down(sums[0])
        diagonal_across.start()
        diagonal_up.start()

    @pl.when(step == 3)
    def _():
        leave[0, low] = down(sums[1, low])
        across_low.start()

    @pl.when(step == 5)
    def _():
        leave[1, high] = down(sums[2, high])
        up_high.start()

    @pl.when(step == 7)
    def _():
        diagonal_up.wait_recv()
        leave[0, high] = down(sums[1, high] + up_cast(come[2, high]))
        across_high.start()
        diagonal_across.wait_recv()
        leave[1, low] = down(sums[2, low] + up_cast(come[2, low]))
        up_low.start()
        for one in (across_low, up_high, across_high, up_low):
            one.wait_recv()
        out[...] = sums[3] + up_cast(come[0]) + up_cast(come[1])
        for number in range(4):
            to_partner(number).wait_send()
        for one in (diagonal_across, diagonal_up, across_low, up_high, across_high, up_low):
            one.wait_send()

def product_reduce_kernel(owns, homes, slope_ref, weight_ref, *refs):
    ids = plane_ids()
    step = pl.program_id(0)
    refs = list(refs)
    parcels = [refs.pop(0) for _ in range(owns + homes)]
    out_ref = refs.pop(0)
    landings = [refs.pop(0) for _ in range(owns + homes)]
    slopes, load, weight, weight_load, *refs = refs
    tail = refs[7:]
    rows_in = row_loads(weight_ref, weight, weight_load)
    early, late = ([], [])
    if owns:
        late.append(owner_cargo(parcels[0], landings[0], *tail[:3]))
    if homes:
        early.append(home_cargo(parcels[-1], landings[-1], *tail[-3:]))

    def fetch(number):
        return pltpu.make_async_copy(slope_ref.at[ids[3](number)], slopes.at[number], load.at[number])

    @pl.when(step == 0)
    def _():
        for one in rows_in:
            one.start()
        for number in range(8):
            fetch(reduce_order(number)).start()
        greet_all(plane_peers()[1] if owns else ids[:3], homes)
        for start, _ in early:
            start()
        for one in rows_in:
            one.wait()
    k = reduce_order(step)
    fetch(k).wait()
    reduce_step(step, product_transposed(slopes[k], weight[...]), refs[:7], ids, out_ref)
    if owns:

        @pl.when(step == 5)
        def _():
            for start, _ in late:
                start()
    if owns or homes:

        @pl.when(step == 7)
        def _():
            for _, finish in late + early:
                finish()

def remote_params(collective_id, limit):
    return pltpu.CompilerParams(collective_id=collective_id, has_side_effects=True, vmem_limit_bytes=limit * MIB)

def owner_shape(parcel):
    count = lax.axis_size('grp') * lax.axis_size('sub')
    return jax.ShapeDtypeStruct((parcel.shape[0] // count, parcel.shape[1] * count), parcel.dtype)

def product_reduce(slopes, weight, owned, homed, collective_id):
    count, rows, inner = slopes.shape
    width = weight.shape[0]
    owns, homes = (owned is not None, homed is not None)
    if not small_plane():
        part = product_transposed(slopes.reshape(-1, inner), rep_rows_last(weight))
        whole = [lax.psum_scatter(part.astype(jnp.bfloat16), PLANE, scatter_dimension=0, tiled=True).astype(jnp.float32)]
        return whole + ([exchange(owned, True, collective_id)] if owns else []) + ([from_plane(homed)] if homes else [])
    cargo = ([owned] if owns else []) + ([homed] if homes else [])
    shapes = ([owner_shape(owned)] if owns else []) + ([jax.ShapeDtypeStruct(homed.shape, homed.dtype)] if homes else [])
    return pl.pallas_call(functools.partial(product_reduce_kernel, owns, homes), grid=(8,), out_shape=[jax.ShapeDtypeStruct((rows, width), jnp.float32)] + shapes, in_specs=[ANY, ANY] + [ANY] * len(cargo), out_specs=[VMEM] + [ANY] * len(cargo), scratch_shapes=[pltpu.VMEM((8, rows, inner), slopes.dtype), DMA((8,)), *row_loads_scratch(weight.shape, weight.dtype), *reduce_scratch(rows, width)] + (owner_scratch() if owns else []) + ([DMA, DMA, DMA] if homes else []), compiler_params=remote_params(collective_id, 60), name='product_reduce')(slopes, weight, *cargo)

def closing_kernel(number, x_ref, homed_ref, *refs):
    owned_refs, (out_ref, homed_out), owned_outs = (refs[:number], refs[number:number + 2], refs[number + 2:2 * number + 2])
    refs = refs[2 * number + 2:]
    here = {n: lax.axis_index(n) for n in EVERY}
    phases = ('rep', 'grp', 'sub')
    home_start, home_finish = home_cargo(homed_ref, homed_out, *refs[:3])
    owners = [owner_cargo(owned_refs[i], owned_outs[i], *refs[3 + 3 * i:6 + 3 * i]) for i in range(number)]
    refs = refs[3 + 3 * number:]

    def other(name, step):
        size = lax.axis_size(name)
        return tuple((lax.rem(here[n] + step, size) if n == name else here[n] for n in EVERY))
    greet_all(plane_peers()[1] + [other('rep', s) for s in range(1, lax.axis_size('rep'))], True)
    out_ref[...] = x_ref[...]
    for j, name in enumerate(phases):
        slots, send, recv = refs[3 * j:3 * j + 3]
        size = lax.axis_size(name)
        me = here[name]
        slots[me] = out_ref[...]
        copies = []
        for s in range(1, size):
            one = pltpu.make_async_remote_copy(src_ref=out_ref, dst_ref=slots.at[me], send_sem=send.at[s], recv_sem=recv.at[s], device_id=other(name, s), device_id_type=MESH)
            one.start()
            copies.append(one)
        if j == 0:
            home_start()
            for start, _ in owners:
                start()
        for one in copies:
            one.wait_recv()
        for one in copies:
            one.wait_send()
        value = slots[0]
        for s in range(1, size):
            value = value + slots[s]
        out_ref[...] = value
    for _, finish in owners:
        finish()
    home_finish()

def closing(x, homed, owned, collective_id):
    scratch = []
    for name in ('rep', 'grp', 'sub'):
        n = lax.axis_size(name)
        scratch += [pltpu.VMEM((n,) + x.shape, x.dtype), DMA((n,)), DMA((n,))]
    number = len(owned)
    return pl.pallas_call(functools.partial(closing_kernel, number), out_shape=[jax.ShapeDtypeStruct(x.shape, x.dtype), jax.ShapeDtypeStruct(homed.shape, homed.dtype)] + [owner_shape(one) for one in owned], in_specs=[VMEM] + [ANY] * (1 + number), out_specs=[VMEM] + [ANY] * (1 + number), scratch_shapes=[DMA, DMA, DMA] + owner_scratch() * number + scratch, compiler_params=pltpu.CompilerParams(collective_id=collective_id, has_side_effects=True), name='closing')(x, homed, *owned)

def exchange_kernel(to_tokens, x_ref, out_ref, send, recv, local):
    groups, reps, subs = (lax.axis_size(n) for n in EVERY)
    g, r, u = (lax.axis_index(n) for n in EVERY)
    count = groups * subs
    place = g * subs + u
    if to_tokens:
        tokens, width = (out_ref.shape[0], x_ref.shape[1])
    else:
        tokens, width = (x_ref.shape[0], out_ref.shape[1])

    def rows(ref, t):
        return ref.at[pl.ds(pl.multiple_of(t * tokens, tokens), tokens), :]

    def columns(ref, t):
        return ref.at[:, pl.ds(pl.multiple_of(t * width, width), width)]
    source, target = (rows, columns) if to_tokens else (columns, rows)
    peers = [lax.rem(place + step, count) for step in range(1, count)]

    def device(t):
        return (t // subs, r, lax.rem(t, subs))
    own = pltpu.make_async_copy(source(x_ref, place), target(out_ref, place), local)
    own.start()
    greet([device(t) for t in peers])
    copies = []
    for step, t in enumerate(peers):
        one = pltpu.make_async_remote_copy(src_ref=source(x_ref, t), dst_ref=target(out_ref, place), send_sem=send.at[step], recv_sem=recv.at[step], device_id=device(t), device_id_type=MESH)
        one.start()
        copies.append(one)
    own.wait()
    for one in copies:
        one.wait_recv()
    for one in copies:
        one.wait_send()

def exchange(x, to_tokens, collective_id):
    count = lax.axis_size('grp') * lax.axis_size('sub')
    shape = (x.shape[0] // count, x.shape[1] * count) if to_tokens else (x.shape[0] * count, x.shape[1] // count)
    return pl.pallas_call(functools.partial(exchange_kernel, to_tokens), out_shape=jax.ShapeDtypeStruct(shape, x.dtype), in_specs=[ANY], out_specs=ANY, scratch_shapes=[DMA((count - 1,)), DMA((count - 1,)), DMA], compiler_params=pltpu.CompilerParams(collective_id=collective_id, has_side_effects=True), name='to_tokens' if to_tokens else 'to_heads')(x)

def opening_kernel(x_ref, *refs):
    weights = (len(refs) - 8) // 2
    sources, (moved_ref, *landings) = (refs[:weights], refs[weights:2 * weights + 1])
    transit, move_send, move_recv, move_local, send, recv, local = refs[2 * weights + 1:]
    groups, _, subs = (lax.axis_size(n) for n in EVERY)
    g, r, u = (lax.axis_index(n) for n in EVERY)
    place, peers = plane_peers()
    relay = position_of(lax.rem(g + r, groups))
    beyond = lax.rem(turn_of(g) + groups - r, groups)

    def block(number, t):
        width = landings[number].shape[1]
        return sources[number].at[:, pl.ds(pl.multiple_of(t * width, width), width)]

    def landing(number):
        rows = sources[number].shape[0]
        return landings[number].at[pl.ds(pl.multiple_of(place * rows, rows), rows), :]

    def hop(number, source, target, device, stays):
        kept = pltpu.make_async_copy(source, target, move_local.at[number])
        moved = remote(source, target, move_send, move_recv, number, device)

        def start():

            @pl.when(stays)
            def _():
                kept.start()

            @pl.when(jnp.logical_not(stays))
            def _():
                moved.start()

        def arrive():

            @pl.when(stays)
            def _():
                kept.wait()

            @pl.when(jnp.logical_not(stays))
            def _():
                moved.wait_recv()

        def leave():

            @pl.when(jnp.logical_not(stays))
            def _():
                moved.wait_send()
        return (start, arrive, leave)
    first = hop(0, x_ref, transit, (relay, r, u), relay == g)
    second = hop(1, transit, moved_ref, (g, beyond, u), beyond == r)
    owns = [pltpu.make_async_copy(block(number, place), landing(number), local.at[number]) for number in range(weights)]
    for one in owns:
        one.start()
    barrier = pltpu.get_barrier_semaphore()
    for device in peers:
        pl.semaphore_signal(barrier, inc=1, device_id=device, device_id_type=MESH)

    @pl.when(beyond != r)
    def _():
        pl.semaphore_signal(barrier, inc=1, device_id=(g, beyond, u), device_id_type=MESH)
    pl.semaphore_wait(barrier, len(peers) + (beyond != r).astype(jnp.int32))
    first[0]()
    copies = []
    for number in range(weights):
        for step, device in enumerate(peers):
            one = pltpu.make_async_remote_copy(src_ref=block(number, device[0] * subs + device[2]), dst_ref=landing(number), send_sem=send.at[number, step], recv_sem=recv.at[number, step], device_id=device, device_id_type=MESH)
            one.start()
            copies.append(one)
    first[1]()
    second[0]()
    for one in owns:
        one.wait()
    for one in copies:
        one.wait_recv()
    for one in copies:
        one.wait_send()
    first[2]()
    second[1]()
    second[2]()

def opening(x, weights, collective_id):
    count = lax.axis_size('grp') * lax.axis_size('sub')
    number = len(weights)
    columns = [jax.ShapeDtypeStruct((w.shape[0] * count, w.shape[1] // count), w.dtype) for w in weights]
    return pl.pallas_call(opening_kernel, out_shape=[jax.ShapeDtypeStruct(x.shape, x.dtype), *columns], in_specs=[VMEM] + [ANY] * number, out_specs=[VMEM] + [ANY] * number, scratch_shapes=[pltpu.VMEM(x.shape, x.dtype), DMA((2,)), DMA((2,)), DMA((2,)), DMA((number, count - 1)), DMA((number, count - 1)), DMA((number,))], compiler_params=pltpu.CompilerParams(collective_id=collective_id, has_side_effects=True), name='opening')(x, *weights)

def attend_kernel(heads, head_ref, place_ref, first_ref, last_ref, mixing_ref, attended_ref, total_ref, out_ref, *refs):
    ids = plane_ids()
    step = pl.program_id(0)

    @pl.when(step == 0)
    def _():
        greet(ids[:3])
    rows = out_ref.shape[0]
    size = attended_ref.shape[1] // heads
    factor = size ** (-0.5) * log2_e
    first_row = pl.multiple_of(ids[3](reduce_order(step)) * rows, rows)
    here = pl.ds(first_row, rows)
    place = place_ref[here, :]
    allowed = (first_ref[...] <= place) & (place <= last_ref[...])
    for h in range(heads):
        q, k, v = (3 * h + j for j in range(3))
        scores = product_transposed(head_ref[here, q * size:(q + 1) * size], head_ref[:, k * size:(k + 1) * size])
        scores = jnp.where(allowed, scores * factor, masked_score)
        top = jnp.max(scores, axis=1, keepdims=True)
        soft = jnp.exp2(scores - top)
        total = jnp.sum(soft, axis=1, keepdims=True)
        mixture = product(soft.astype(jnp.bfloat16), head_ref[:, v * size:(v + 1) * size])
        attended_ref[here, h * size:(h + 1) * size] = (mixture / total).astype(jnp.bfloat16)
        log_total = jnp.broadcast_to(top + jnp.log2(total), (rows, 128))
        total_ref[h, :, here] = log_total.T[:8]
    reduce_step(step, product(attended_ref[here, :], mixing_ref[...]), refs, ids, out_ref)

def attend(packed, places, key_last, mixing, heads, token_rows, collective_id):
    rows = packed.shape[0]
    inner, width = mixing.shape
    if not small_plane():
        attended, totals = attention_forward(packed, places, key_last, heads)
        part = product(attended, mixing).astype(jnp.bfloat16)
        return (attended, totals, lax.psum_scatter(part, PLANE, scatter_dimension=0, tiled=True).astype(jnp.float32))
    return pl.pallas_call(functools.partial(attend_kernel, heads), grid=(8,), out_shape=[jax.ShapeDtypeStruct((rows, inner), jnp.bfloat16), jax.ShapeDtypeStruct((heads, 8, rows), jnp.float32), jax.ShapeDtypeStruct((token_rows, width), jnp.float32)], in_specs=[VMEM] * 5, out_specs=[VMEM] * 3, scratch_shapes=reduce_scratch(token_rows, width), compiler_params=remote_params(collective_id, 60), name='attend')(packed, places[:, None], places[None, :], key_last[None, :], mixing)

def gather_order(step):
    return step + 2 * (step % 2) - 1 + (8 - step) // 8 - step // 7

def gather_step(step, slots, send, recv, ids):
    across, up, partner, _ = ids
    half = slots.shape[1] // 2
    low, high = (pl.ds(0, half), pl.ds(half, half))

    def copy(number, source, target, device):
        return remote(slots.at[source], slots.at[target], send, recv, number, device)
    across_low = copy(0, (0, low), (1, low), across)
    up_high = copy(1, (0, high), (4, high), up)
    across_high = copy(2, (0, high), (1, high), across)
    up_low = copy(3, (0, low), (4, low), up)
    own = copy(4, 0, 2, partner)
    far_low = copy(5, (1, low), (5, low), up)
    far_high = copy(6, (4, high), (5, high), across)
    pass_across = copy(7, 1, 3, partner)
    pass_up = copy(8, 4, 6, partner)
    pass_low = copy(9, (5, low), (7, low), partner)
    pass_high = copy(10, (5, high), (7, high), partner)

    @pl.when(step == 0)
    def _():
        for one in (across_low, up_high, own, across_high, up_low):
            one.start()

    @pl.when(step == 1)
    def _():
        own.wait_recv()

    @pl.when(step == 2)
    def _():
        across_low.wait_recv()
        far_low.start()
        up_high.wait_recv()
        far_high.start()
        across_high.wait_recv()
        pass_across.start()

    @pl.when(step == 3)
    def _():
        up_low.wait_recv()
        pass_up.start()

    @pl.when(step == 4)
    def _():
        pass_across.wait_recv()

    @pl.when(step == 5)
    def _():
        pass_up.wait_recv()

    @pl.when(step == 6)
    def _():
        far_low.wait_recv()
        pass_low.start()
        far_high.wait_recv()
        pass_high.start()

    @pl.when(step == 7)
    def _():
        pass_low.wait_recv()
        pass_high.wait_recv()
        for one in (across_low, up_high, across_high, up_low, own, far_low, far_high, pass_across, pass_up, pass_low, pass_high):
            one.wait_send()

def attend_back_kernel(heads, branch_ref, homed_ref, head_ref, mixing_ref, attended_ref, total_ref, place_ref, first_ref, last_ref, part_ref, out_ref, homed_out, sums_ref, turned, key_sum, value_sum, part_sum, slots, load, send, recv, *cargo):
    ids = plane_ids()
    step = pl.program_id(0)
    home_start, home_finish = home_cargo(homed_ref, homed_out, *cargo)
    rows = slots.shape[1]
    size = head_ref.shape[1] // (3 * heads)
    scale = size ** (-0.5)
    factor = scale * log2_e

    @pl.when(step == 0)
    def _():
        first = pltpu.make_async_copy(branch_ref, slots.at[0], load)
        first.start()
        for h in range(heads):
            turned[h] = head_ref[:, (3 * h + 1) * size:(3 * h + 2) * size].T
        key_sum[...] = jnp.zeros_like(key_sum)
        value_sum[...] = jnp.zeros_like(value_sum)
        part_sum[...] = jnp.zeros_like(part_sum)
        sums_ref[...] = jnp.zeros_like(sums_ref)
        greet_all(ids[:3], True)
        home_start()
        first.wait()
    gather_step(step, slots, send, recv, ids)
    k = gather_order(step)
    here = pl.ds(pl.multiple_of(ids[3](k) * rows, rows), rows)
    part_sum[...] += row_outer(attended_ref[here, :], slots[k])
    slopes = product_transposed(slots[k], mixing_ref[...]).astype(jnp.bfloat16)
    place = place_ref[:, here]
    allowed = (first_ref[...] <= place) & (place <= last_ref[...])
    for h in range(heads):
        queries = head_ref[here, 3 * h * size:(3 * h + 1) * size]
        keys = head_ref[:, (3 * h + 1) * size:(3 * h + 2) * size]
        values = head_ref[:, (3 * h + 2) * size:(3 * h + 3) * size]
        slope = slopes[:, h * size:(h + 1) * size]
        scores = product_transposed(keys, queries)
        soft = jnp.where(allowed, jnp.exp2(scores * factor - total_ref[h, :1, here]), 0.0)
        weight_slope = product_transposed(values, slope)
        centre = jnp.sum(soft * weight_slope, axis=0, keepdims=True)
        score_slope = (soft * (weight_slope - centre)).astype(jnp.bfloat16)
        value_sum[h] += product(soft.astype(jnp.bfloat16), slope)
        key_sum[h] += product(score_slope, queries)
        query_slope = product(turned[h], score_slope)
        query_slope = (query_slope.T * scale).astype(jnp.bfloat16)
        out_ref[here, 3 * h * size:(3 * h + 1) * size] = query_slope
        sums_ref[:, 3 * h * size:(3 * h + 1) * size] += jnp.sum(query_slope.astype(jnp.float32), axis=0, keepdims=True)

    @pl.when(step == 7)
    def _():
        for h in range(heads):
            out_ref[:, (3 * h + 1) * size:(3 * h + 2) * size] = (key_sum[h] * scale).astype(jnp.bfloat16)
            value_slope = value_sum[h].astype(jnp.bfloat16)
            out_ref[:, (3 * h + 2) * size:(3 * h + 3) * size] = value_slope
            sums_ref[:, (3 * h + 2) * size:(3 * h + 3) * size] = jnp.sum(value_slope.astype(jnp.float32), axis=0, keepdims=True)
        part_ref[...] = part_sum[...].astype(jnp.bfloat16)
        home_finish()

def attend_back(branch_slope, homed, packed, mixing, attended, totals, places, key_last, heads, collective_id):
    rows, columns = packed.shape
    token_rows, width = branch_slope.shape
    size = columns // (3 * heads)
    if not small_plane():
        every = lax.all_gather(branch_slope, PLANE, axis=0, tiled=True)
        slopes = product_transposed(every, mixing).astype(jnp.bfloat16)
        part = row_outer(attended, every).astype(jnp.bfloat16)
        slopes = attention_backward(packed, totals, slopes, places, key_last, heads)
        return (part, slopes, from_plane(homed), jnp.sum(slopes.astype(jnp.float32), axis=0, keepdims=True))
    return pl.pallas_call(functools.partial(attend_back_kernel, heads), grid=(8,), out_shape=[jax.ShapeDtypeStruct(mixing.shape, jnp.bfloat16), jax.ShapeDtypeStruct((rows, columns), jnp.bfloat16), jax.ShapeDtypeStruct(homed.shape, homed.dtype), jax.ShapeDtypeStruct((1, columns), jnp.float32)], in_specs=[ANY] * 2 + [VMEM] * 7, out_specs=[VMEM, VMEM, ANY, VMEM], scratch_shapes=[pltpu.VMEM((heads, size, rows), jnp.bfloat16), pltpu.VMEM((heads, rows, size), jnp.float32), pltpu.VMEM((heads, rows, size), jnp.float32), pltpu.VMEM(mixing.shape, jnp.float32), pltpu.VMEM((8, token_rows, width), jnp.bfloat16), DMA, DMA((11,)), DMA((11,)), DMA, DMA, DMA], compiler_params=remote_params(collective_id, 62), name='attend_back')(branch_slope, homed, packed, mixing, attended, totals, places[None, :], places[:, None], key_last[:, None])

def add_outer(total, left, right):
    turned = left.T
    for first in range(0, total.shape[1], 256):
        here = pl.ds(first, 256)
        total[:, here] += product(turned, right[:, first:first + 256])

def rep_order(total, narrow, part_ref, sem):
    groups, reps = (lax.axis_size('grp'), lax.axis_size('rep'))
    rows = total.shape[0] // (groups * reps)
    for g in range(groups):
        for r in range(reps):
            come, go = (pl.ds((g * reps + r) * rows, rows), pl.ds((r * groups + g) * rows, rows))
            narrow[come, :] = total[come, :].astype(jnp.bfloat16)
            pltpu.make_async_copy(narrow.at[come], part_ref.at[go], sem.at[g, r]).start()

def rep_order_wait(narrow, part_ref, sem):
    groups, reps = (lax.axis_size('grp'), lax.axis_size('rep'))
    rows = narrow.shape[0] // (groups * reps)
    for g in range(groups):
        for r in range(reps):
            come, go = (pl.ds((g * reps + r) * rows, rows), pl.ds((r * groups + g) * rows, rows))
            pltpu.make_async_copy(narrow.at[come], part_ref.at[go], sem.at[g, r]).wait()

def hidden_kernel(middle_ref, cotangent_ref, expand_ref, offset_ref, every_ref, active_ref, rise_ref, part_ref, slots, cotangents, actives, rises, total, load, send, recv, store, fetch_cotangent, active_store, rise_store, expand, expand_load, narrow, part_store):
    ids = plane_ids()
    step = pl.program_id(0)
    turn = lax.rem(step, 2)

    def fetch(number, side):
        return pltpu.make_async_copy(cotangent_ref.at[ids[3](gather_order(number))], cotangents.at[side], fetch_cotangent.at[side])

    @pl.when(step == 0)
    def _():
        first = pltpu.make_async_copy(middle_ref, slots.at[0], load)
        first.start()
        rows_in = row_loads(expand_ref, expand, expand_load)
        for one in rows_in:
            one.start()
        fetch(0, 0).start()
        total[...] = jnp.zeros_like(total)
        greet(ids[:3])
        first.wait()
        for one in rows_in:
            one.wait()
    gather_step(step, slots, send, recv, ids)
    k = gather_order(step)

    def keep(number):
        return pltpu.make_async_copy(slots.at[number], every_ref.at[ids[3](number)], store.at[number])

    def put(number, side):
        piece = ids[3](number)
        return (pltpu.make_async_copy(actives.at[side], active_ref.at[piece], active_store.at[side]), pltpu.make_async_copy(rises.at[side], rise_ref.at[piece], rise_store.at[side]))
    keep(k).start()

    @pl.when(step >= 2)
    def _():
        for one in put(k, turn):
            one.wait()
    expanded = product(slots[k], expand[...]) + offset_ref[...]
    below = 0.5 * (1.0 + lax.erf(expanded * root_half))
    actives[turn] = (expanded * below).astype(jnp.bfloat16)
    rises[turn] = below + expanded * (jnp.exp(-0.5 * expanded * expanded) * normal_peak)
    for one in put(k, turn):
        one.start()
    fetch(step, turn).wait()

    @pl.when(step < 7)
    def _():
        fetch(step + 1, 1 - turn).start()
    add_outer(total, cotangents[turn], actives[turn])

    @pl.when(step == 7)
    def _():
        rep_order(total, narrow, part_ref, part_store)
        for late in range(2):
            for one in put(k, late):
                one.wait()
        for number in range(8):
            keep(number).wait()
        rep_order_wait(narrow, part_ref, part_store)

def hidden(middle, cotangent_all, expand_slice, offset, collective_id):
    rows, width = middle.shape
    count = lax.axis_size('grp') * lax.axis_size('sub')
    inner = expand_slice.shape[1]
    if not small_plane():
        every = lax.all_gather(middle, PLANE, axis=0, tiled=True)
        expanded = product(every, rep_rows_last(expand_slice)) + offset
        below = 0.5 * (1.0 + lax.erf(expanded * root_half))
        rise = below + expanded * (jnp.exp(-0.5 * expanded * expanded) * normal_peak)
        active = (expanded * below).astype(jnp.bfloat16)
        return (every, active, rise, rep_rows_first(row_outer(cotangent_all, active)))
    every, active, rise, part = pl.pallas_call(hidden_kernel, grid=(8,), out_shape=[jax.ShapeDtypeStruct((8, rows, width), middle.dtype), jax.ShapeDtypeStruct((8, rows, inner), jnp.bfloat16), jax.ShapeDtypeStruct((8, rows, inner), jnp.float32), jax.ShapeDtypeStruct((width, inner), jnp.bfloat16)], in_specs=[ANY, ANY, ANY, VMEM], out_specs=[ANY] * 4, scratch_shapes=[pltpu.VMEM((8, rows, width), middle.dtype), pltpu.VMEM((2, rows, width), jnp.bfloat16), pltpu.VMEM((2, rows, inner), jnp.bfloat16), pltpu.VMEM((2, rows, inner), jnp.float32), pltpu.VMEM((width, inner), jnp.float32), DMA, DMA((11,)), DMA((11,)), DMA((8,)), DMA((2,)), DMA((2,)), DMA((2,)), *row_loads_scratch(expand_slice.shape, expand_slice.dtype), *row_loads_scratch(expand_slice.shape, jnp.bfloat16)], compiler_params=remote_params(collective_id, 60), name='hidden')(middle, cotangent_all.reshape(8, rows, width), expand_slice, offset[None, :])
    return (every.reshape(count * rows, width), active.reshape(count * rows, inner), rise.reshape(count * rows, inner), part)

def hidden_back_kernel(cotangent_ref, middle_ref, rise_ref, shrink_ref, expand_ref, slope_ref, out_ref, part_ref, sums_ref, cotangents, middles, rises, slopes, total, fetches, store, shrink, shrink_load, expand, expand_load, narrow, part_store, *refs):
    ids = plane_ids()
    step = pl.program_id(0)

    def fetch(number, side):
        piece = ids[3](reduce_order(number))
        return [pltpu.make_async_copy(source.at[piece], target.at[side], fetches.at[kind, side]) for kind, (source, target) in enumerate(((cotangent_ref, cotangents), (rise_ref, rises), (middle_ref, middles)))]

    def put(number, side):
        return pltpu.make_async_copy(slopes.at[side], slope_ref.at[ids[3](reduce_order(number))], store.at[side])
    turn = lax.rem(step, 2)

    @pl.when(step == 0)
    def _():
        rows_in = row_loads(shrink_ref, shrink, shrink_load) + row_loads(expand_ref, expand, expand_load)
        for one in rows_in:
            one.start()
        for one in fetch(0, 0):
            one.start()
        total[...] = jnp.zeros_like(total)
        sums_ref[...] = jnp.zeros_like(sums_ref)
        greet(ids[:3])
        for one in rows_in:
            one.wait()
    for one in fetch(step, turn):
        one.wait()

    @pl.when(step < 7)
    def _():
        for one in fetch(step + 1, 1 - turn):
            one.start()

    @pl.when(step >= 2)
    def _():
        put(step, turn).wait()
    slope = product(cotangents[turn], shrink[...]) * rises[turn]
    slopes[turn] = slope.astype(jnp.bfloat16)
    put(step, turn).start()

    def before():
        add_outer(total, middles[turn], slopes[turn])
        sums_ref[...] += jnp.sum(slopes[turn].astype(jnp.float32), axis=0, keepdims=True)

        @pl.when(step == 7)
        def _():
            rep_order(total, narrow, part_ref, part_store)
    reduce_step(step, product_transposed(slopes[turn], expand[...]), refs, ids, out_ref, before)

    @pl.when(step == 7)
    def _():
        put(6, 0).wait()
        put(7, 1).wait()
        rep_order_wait(narrow, part_ref, part_store)

def hidden_back(cotangent_all, middle_all, rise, shrink_slice, expand_slice, token_rows, collective_id):
    rows, width = cotangent_all.shape
    inner = shrink_slice.shape[1]
    if not small_plane():
        slope = (product(cotangent_all, rep_rows_last(shrink_slice)) * rise).astype(jnp.bfloat16)
        part = product_transposed(slope, rep_rows_last(expand_slice)).astype(jnp.bfloat16)
        normed = lax.psum_scatter(part, PLANE, scatter_dimension=0, tiled=True).astype(jnp.float32)
        sums = jnp.sum(slope.astype(jnp.float32), axis=0)
        return (slope, normed, rep_rows_first(row_outer(middle_all, slope)), sums)
    pieces = (8, token_rows, width)
    slope, normed, part, sums = pl.pallas_call(hidden_back_kernel, grid=(8,), out_shape=[jax.ShapeDtypeStruct((8, token_rows, inner), jnp.bfloat16), jax.ShapeDtypeStruct((token_rows, width), jnp.float32), jax.ShapeDtypeStruct((width, inner), jnp.bfloat16), jax.ShapeDtypeStruct((1, inner), jnp.float32)], in_specs=[ANY] * 5, out_specs=[ANY, VMEM, ANY, VMEM], scratch_shapes=[pltpu.VMEM((2, token_rows, width), jnp.bfloat16), pltpu.VMEM((2, token_rows, width), jnp.bfloat16), pltpu.VMEM((2, token_rows, inner), jnp.float32), pltpu.VMEM((2, token_rows, inner), jnp.bfloat16), pltpu.VMEM((width, inner), jnp.float32), DMA((3, 2)), DMA((2,)), *row_loads_scratch(shrink_slice.shape, shrink_slice.dtype), *row_loads_scratch(expand_slice.shape, expand_slice.dtype), *row_loads_scratch(expand_slice.shape, jnp.bfloat16), *reduce_scratch(token_rows, width)], compiler_params=remote_params(collective_id, 63), name='hidden_back')(cotangent_all.reshape(pieces), middle_all.reshape(pieces), rise.reshape(8, token_rows, inner), shrink_slice, expand_slice)
    return (slope.reshape(rows, inner), normed, part, sums[0])

def plane_moves():
    groups, reps, subs = (lax.axis_size(n) for n in EVERY)
    moves = []
    for g in range(groups):
        for r in range(reps):
            turn = (g + r) % groups
            position = turn % 2 * (groups // 2) + turn // 2
            for u in range(subs):
                moves.append(tuple(((a * reps + b) * subs + u for a, b in ((g, r), (position, r), (position, g)))))
    return moves

def to_door(array):
    return lax.ppermute(array, EVERY, [(home, door) for home, door, _ in plane_moves()])

def to_keeper(array):
    return lax.ppermute(array, EVERY, [(door, away) for _, door, away in plane_moves()])

def to_plane_at_once(array):
    return lax.ppermute(array, EVERY, [(home, away) for home, _, away in plane_moves()])

def from_plane(array):
    return lax.ppermute(array, EVERY, [(away, home) for home, _, away in plane_moves()])

def plane_order(places):
    groups = lax.axis_size('grp')
    blocks = jnp.roll(places.reshape(groups, -1), lax.axis_index('rep'), axis=0)
    return blocks.reshape(groups // 2, 2, -1).transpose(1, 0, 2).reshape(-1)

def rep_rows(own):
    return lax.all_gather(own, 'rep', axis=0, tiled=True)

def rep_rows_last(every):
    groups, reps, subs = (lax.axis_size(name) for name in EVERY)
    columns = every.shape[1]
    ordered = every.reshape(reps, groups, subs, -1, columns).transpose(1, 0, 2, 3, 4)
    return ordered.reshape(-1, columns)

def rep_rows_first(gradient):
    groups, reps, subs = (lax.axis_size(name) for name in EVERY)
    columns = gradient.shape[1]
    ordered = gradient.astype(jnp.bfloat16).reshape(groups, reps, subs, -1, columns)
    return ordered.transpose(1, 0, 2, 3, 4).reshape(-1, columns)

def rep_sums(ordered):
    return lax.psum_scatter(ordered, 'rep', scatter_dimension=0, tiled=True)

def sub_turn(block):
    groups, reps, subs = (lax.axis_size(name) for name in EVERY)
    low = reps // subs
    moves = [((g * reps + r) * subs + u, (g * reps + u * low + r % low) * subs + r // low) for g in range(groups) for r in range(reps) for u in range(subs)]
    return lax.ppermute(block, EVERY, moves)

def sub_rows(own):
    rows, width = own.shape
    reps, subs = (lax.axis_size('rep'), lax.axis_size('sub'))
    shares = own.reshape(subs, reps // subs, -1, width)
    if subs != 2:
        every = lax.all_to_all(shares, 'sub', split_axis=0, concat_axis=0, tiled=True)
        return every.transpose(1, 0, 2, 3).reshape(rows, width)
    me = lax.axis_index('sub')
    kept = jnp.where(me == 0, shares[0], shares[1])
    come = lax.ppermute(jnp.where(me == 0, shares[1], shares[0]), 'sub', [(0, 1), (1, 0)])
    first, second = (jnp.where(me == 0, kept, come), jnp.where(me == 0, come, kept))
    return jnp.stack([first, second], axis=1).reshape(rows, width)

def mixing_sums_of(part):
    reps, subs = (lax.axis_size('rep'), lax.axis_size('sub'))
    rows, width = part.shape
    ordered = part.reshape(reps // subs, subs, rows // reps, width).transpose(1, 0, 2, 3)
    return lax.psum_scatter(ordered.reshape(rows, width), 'rep', scatter_dimension=0, tiled=True)

def sub_owned(part, reps):
    rows, width = part.shape
    subs = lax.axis_size('sub')
    shares = part.reshape(reps // subs, subs, -1, width).transpose(1, 0, 2, 3)
    if subs != 2:
        every = lax.all_to_all(shares, 'sub', split_axis=0, concat_axis=0, tiled=True)
        return every.reshape(rows, width)
    me = lax.axis_index('sub')
    kept = jnp.where(me == 0, shares[0], shares[1])
    come = lax.ppermute(jnp.where(me == 0, shares[1], shares[0]), 'sub', [(0, 1), (1, 0)])
    first, second = (jnp.where(me == 0, kept, come), jnp.where(me == 0, come, kept))
    return jnp.concatenate([first, second], axis=0).reshape(rows, width)

def shards(layer_input, entry_gain, entry_shift, joint_weight, query_offset, value_offset, mixing_weight, attention_offset, middle_gain, middle_shift, expand_weight, expand_offset, shrink_weight, shrink_offset, placement, slot_lengths, cotangent):
    token_rows, width = layer_input.shape
    hidden_width = expand_weight.shape[1]
    groups, reps, subs = (lax.axis_size(name) for name in EVERY)
    plane_count = groups * subs
    plane_index = lax.axis_index(PLANE)
    head_size = width // HEADS
    local_heads = HEADS // plane_count
    head_columns = local_heads * head_size
    plane_rows = plane_count * token_rows
    facts = to_plane_at_once(jnp.concatenate([placement, slot_lengths], axis=1))[0]
    mixing_own = rep_rows(mixing_weight)
    moved_input, joint_own, expand_own = opening(layer_input, (joint_weight, expand_weight), 12)
    joint_own, mixing_own = lax.optimization_barrier((joint_own, mixing_own))
    input_float = moved_input.astype(jnp.float32)
    joint_every = rep_rows(joint_own)
    entry_normal, entry_inverse = norm_terms(input_float)
    entry_normed = (entry_normal * entry_gain + entry_shift).astype(jnp.bfloat16)
    entry_all, shrink_own = plane_gather(entry_normed, (shrink_weight,), 1)
    cotangent, facts, entry_all = lax.optimization_barrier((cotangent, facts, entry_all))
    cotangent = to_door(cotangent)
    places = plane_order(facts[:placement.shape[1]])
    lengths = facts[placement.shape[1]:]
    prompt = places.shape[0] // 2
    key_last = key_bounds(places, lengths, prompt)
    expand_slice = rep_rows(expand_own)
    shrink_slice = rep_rows(shrink_own)
    cotangent = to_keeper(cotangent)
    mixing_slice = sub_rows(mixing_own)
    offsets = jnp.stack([query_offset.reshape(HEADS, head_size), jnp.zeros((HEADS, head_size), jnp.float32), value_offset.reshape(HEADS, head_size)], axis=1).reshape(-1)
    offsets = lax.dynamic_slice_in_dim(offsets, plane_index * 3 * head_columns, 3 * head_columns)
    heads_kept = (product(entry_all, rep_rows_last(joint_every)) + offsets).astype(jnp.bfloat16)
    attended, log_totals, branch = attend(heads_kept, places, key_last, mixing_slice, local_heads, token_rows, 3)
    residual = input_float + (branch + attention_offset)
    middle_normal, middle_inverse = norm_terms(residual)
    middle_normed = (middle_normal * middle_gain + middle_shift).astype(jnp.bfloat16)
    cotangent, middle_normed = lax.optimization_barrier((cotangent, middle_normed))
    cotangent_all, = plane_gather(cotangent, (), 4)
    middle_normed, cotangent_all = lax.optimization_barrier((middle_normed, cotangent_all))
    hidden_local = hidden_width // plane_count
    offset_local = lax.dynamic_slice_in_dim(expand_offset, plane_index * hidden_local, hidden_local)
    middle_all, activated, rise, shrink_part = hidden(middle_normed, cotangent_all, expand_slice, offset_local, 5)
    shrink_sums = rep_sums(shrink_part)
    expanded_slope, normed_slope, expand_part, expanded_sums = hidden_back(cotangent_all, middle_all, rise, shrink_slice, expand_slice, token_rows, 6)
    expand_sums = rep_sums(expand_part)
    activated, normed_slope = lax.optimization_barrier((activated, normed_slope))
    shrunk, = product_reduce(activated.reshape(plane_count, token_rows, hidden_local), shrink_slice, None, None, 8)
    own_output = (residual + shrunk + shrink_offset).astype(jnp.bfloat16)
    own_output, normed_slope = lax.optimization_barrier((own_output, normed_slope))
    cotangent_float = cotangent.astype(jnp.float32)
    residual_slope = cotangent_float + norm_back(normed_slope, middle_gain, middle_normal, middle_inverse)
    branch_slope = residual_slope.astype(jnp.bfloat16)
    mixing_part, joint_slope, layer_output, slope_sums = attend_back(branch_slope, own_output, heads_kept, mixing_slice, attended, log_totals, places, key_last, local_heads, 7)
    shrink_sums, joint_slope = lax.optimization_barrier((shrink_sums, joint_slope))
    joint_part = rep_rows_first(row_outer(entry_all, joint_slope))
    joint_part, joint_slope, expand_sums, mixing_part = lax.optimization_barrier((joint_part, joint_slope, expand_sums, mixing_part))
    joint_sums = rep_sums(joint_part)
    mixing_part = sub_owned(mixing_part, reps)
    joint_sums, mixing_part = lax.optimization_barrier((joint_sums, mixing_part))
    mixing_sums = rep_sums(mixing_part)
    entry_slope, expand_rows = product_reduce(joint_slope.reshape(plane_count, token_rows, 3 * head_columns), joint_every, expand_sums, None, 9)
    own_gradient = (residual_slope + norm_back(entry_slope, entry_gain, entry_normal, entry_inverse)).astype(jnp.bfloat16)
    slope_sums = slope_sums.reshape(local_heads, 3, head_size)

    def placed(piece, whole_size):
        return lax.dynamic_update_slice_in_dim(jnp.zeros((whole_size,), jnp.float32), piece, plane_index * piece.shape[0], 0)
    small = [jnp.sum(entry_slope * entry_normal, axis=0), jnp.sum(entry_slope, axis=0), placed(slope_sums[:, 0].reshape(-1), width), placed(slope_sums[:, 2].reshape(-1), width), jnp.sum(branch_slope.astype(jnp.float32), axis=0), jnp.sum(normed_slope * middle_normal, axis=0), jnp.sum(normed_slope, axis=0), placed(expanded_sums, hidden_width), jnp.sum(cotangent_float, axis=0)]
    small_own = jnp.concatenate(small).reshape(-1, 128)
    small_all, input_gradient, joint_rows, shrink_rows = closing(small_own, own_gradient, (joint_sums, shrink_sums), 10)
    shrink_gradient = shrink_rows.astype(jnp.float32)
    expand_gradient = expand_rows.astype(jnp.float32)
    joint_gradient = joint_rows.astype(jnp.float32)
    mixing_gradient = mixing_sums.astype(jnp.float32)
    small_all = small_all.reshape(-1)
    small_sums, first = ([], 0)
    for piece in small:
        small_sums.append(small_all[first:first + piece.shape[0]])
        first += piece.shape[0]
    return (layer_output, input_gradient, small_sums[0], small_sums[1], joint_gradient, small_sums[2], small_sums[3], mixing_gradient, small_sums[4], small_sums[5], small_sums[6], expand_gradient, small_sums[7], shrink_gradient, small_sums[8])

def solution(mesh):
    groups, sequence = (mesh.shape['grp'], mesh.shape['seq'])
    subs = sequence // groups
    planes = Mesh(mesh.devices.reshape(groups, sequence // subs, subs), EVERY)
    rows, whole, group_rows = (P(EVERY, None), P(), P('grp', None))
    return jax.shard_map(shards, mesh=planes, in_specs=(rows, whole, whole, rows, whole, whole, rows, whole, whole, whole, rows, whole, rows) + (whole, group_rows, group_rows, rows), out_specs=(rows, rows, whole, whole, rows, whole, whole, rows, whole, whole, whole, rows, whole) + (rows, whole), check_vma=False)
```
